32 devices in a mesh: row: 8 (over z, core), col: 4 (over y, x).
Axes of the slice: x: 2, y: 2, z: 4, core: 2. Of those that a mesh axis runs over, the one named last changes fastest.
Arguments:
- attn_out: bfloat16 [6, 512, 2048], P(None, 'col', 'row'), may hold values from -0.625 to 0.625
- out_cotangent: bfloat16 [6, 512, 2048], P(None, 'row', 'col'), may hold values from -6 to 6
- frozen: bfloat16 [6, 2048, 2048], P(None, 'row', 'col'), may hold values from -0.5 to 0.5
- adapt_in: bfloat16 [6, 32, 2048], P(None, None, 'row'), may hold values from -0.125 to 0.125
- adapt_out: bfloat16 [6, 32, 2048], P(None, None, 'col'), may hold values from -1 to 1
- magnitude: float32 [6, 2048], P(None, 'col'), may hold values from 0.1 to 1.9
Outputs:
- input_grad: bfloat16 [6, 512, 2048], P(None, 'col', 'row')
- adapt_in_grad: float32 [6, 32, 2048], P(None, None, 'row')
- adapt_out_grad: float32 [6, 32, 2048], P(None, None, 'col')
- magnitude_grad: float32 [6, 2048], P(None, 'col')
The draws below stay inside these ranges and needn't reach their ends.
All inputs are finite; a program needn't handle non-finite values.
Results may differ from the reference program's by a relative error of at most 0.0065.
Values may be sent and summed in bfloat16 or wider, within the bound.
A program may use at most 64 MiB of HBM per device.

```python
import jax
import jax.numpy as jnp
from jax import lax

WIDTH = 2048
IN_WIDTH = 2048
RANK = 32
LAYERS = 6
TOKENS = 512


def steps_of(key, extent, shards, smallest, top_value):
    def one(dim, shards_of):
        steps = jax.random.uniform(jax.random.fold_in(jax.random.fold_in(key, 6), dim), (shards_of,), jnp.float32, smallest / len(shards), top_value / len(shards))
        return jnp.repeat(jnp.exp(steps), extent[dim] // shards_of).reshape((-1,) + (1,) * (len(extent) - dim - 1))

    level = one(*shards[0])
    for cut in shards[1:]:
        level = level * one(*cut)
    return level


def gaussian(rng, extent, spread, reach, split=(), kind=jnp.bfloat16):
    level = steps_of(rng, extent, split, -0.22, 0.18) if split else 1.0
    entries = jax.random.normal(rng, extent, jnp.float32) * spread * level
    return jnp.minimum(jnp.maximum(entries, -reach), reach).astype(kind)


def setup_inputs(seed: int = 0) -> dict:
    key_list = jax.random.split(jax.random.key(seed), 7)
    attn_out = gaussian(key_list[0], (LAYERS, TOKENS, IN_WIDTH), (TOKENS ** -0.5), 0.625, ((1, 4), (2, 8)))
    out_cotangent = gaussian(key_list[1], (LAYERS, TOKENS, WIDTH), 1.0, 6.0, ((1, 8), (2, 4)))
    frozen = gaussian(key_list[2], (LAYERS, IN_WIDTH, WIDTH), (IN_WIDTH // 16) ** -0.5, 0.5, ((1, 8), (2, 4)))
    adapt_in = gaussian(key_list[3], (LAYERS, RANK, IN_WIDTH), IN_WIDTH ** -0.5, 0.125, ((2, 8),))
    adapt_out = gaussian(key_list[4], (LAYERS, RANK, WIDTH), RANK ** -0.5, 1.0, ((2, 4),))
    magnitude = jnp.clip(1.0 + 0.18 * jax.random.normal(key_list[5], (LAYERS, WIDTH), jnp.float32), 0.1, 1.9)
    return {"attn_out": attn_out, "out_cotangent": out_cotangent, "frozen": frozen, "adapt_in": adapt_in, "adapt_out": adapt_out, "magnitude": magnitude}


precise = lax.Precision.HIGHEST

def one_layer(acts, grads, frozen, adapt_in, adapt_out, magnitude):
    merged = frozen.astype(jnp.float32) + lax.dot_general(adapt_in, adapt_out, (((0,), (0,)), ((), ())), preferred_element_type=jnp.float32)
    squares = lax.optimization_barrier(jnp.sum(merged * merged, axis=0))
    norms = jnp.sqrt(squares + 0.25)
    outer = lax.dot_general(acts, grads, (((0,), (0,)), ((), ())), preferred_element_type=jnp.float32)
    dots = lax.optimization_barrier(jnp.sum(merged * outer, axis=0))
    scales = magnitude / norms
    correct = -magnitude * dots / (norms * norms * norms)
    magnitude_grad = dots / norms
    delta = outer * scales + merged * correct
    in_grad = lax.dot_general(adapt_out.astype(jnp.float32), delta, (((1,), (1,)), ((), ())), precision=precise)
    out_grad = jnp.dot(adapt_in.astype(jnp.float32), delta, precision=precise)
    scaled = (grads * scales).astype(jnp.bfloat16)
    weight_low = merged.astype(jnp.bfloat16)
    input_grad = lax.dot_general(scaled, weight_low, (((1,), (1,)), ((), ())), preferred_element_type=jnp.float32).astype(jnp.bfloat16)
    return (input_grad, in_grad, out_grad, magnitude_grad)

def reference(attn_out, out_cotangent, frozen, adapt_in, adapt_out, magnitude):
    results = [one_layer(attn_out[layer_at], out_cotangent[layer_at], frozen[layer_at], adapt_in[layer_at], adapt_out[layer_at], magnitude[layer_at]) for layer_at in range(LAYERS)]
    return (jnp.stack([item[0] for item in results]), jnp.stack([item[1] for item in results]), jnp.stack([item[2] for item in results]), jnp.stack([item[3] for item in results]))
```

```python
import functools

import jax
import jax.numpy as jnp
from jax import lax
from jax.experimental import pallas as pl
from jax.experimental.pallas import tpu as pltpu
from jax.sharding import PartitionSpec as P

MESH = pl.DeviceIdType.MESH
F32 = jnp.float32
BF16 = jnp.bfloat16


def mm(a, b, dims):
    return lax.dot_general(a, b, (dims, ((), ())), preferred_element_type=F32)


def kernel(
    R, C,
    acts_hbm, grads_hbm, frozen_hbm, ain_hbm, aout_hbm, mag_hbm,
    ig_hbm, ing_hbm, oug_hbm, mgrad_hbm,
    acts, grads, frozen, ain, aout, mag,
    ig, ing, oug, mgrad, load, save,
    G, A, merged, wlow, prod, own, rs_send, rs_recv,
    sq, dt, im_send, im_sib, im_acc, im_recv, io_send, io_sib, io_acc, io_recv, og, q, q_recv,
    scl, cor, mag3, send, g_in, g_fw, a_in, rs_in, sq_in, dt_in, im_in, io_in, io_fw, og_in, og_fw, q_in,
):
    pairs = ((grads_hbm, grads), (acts_hbm, acts), (frozen_hbm, frozen),
             (ain_hbm, ain), (aout_hbm, aout), (mag_hbm, mag))
    loads = [pltpu.make_async_copy(a, b, load.at[i]) for i, (a, b) in enumerate(pairs)]
    for copy in loads:
        copy.start()
    pairs = ((mgrad, mgrad_hbm), (ig, ig_hbm), (ing, ing_hbm), (oug, oug_hbm))
    saves = [pltpu.make_async_copy(a, b, save.at[i]) for i, (a, b) in enumerate(pairs)]
    L, TR, W = grads.shape
    TC, KI = acts.shape[1:]
    RANK = ain.shape[1]
    k = RANK // R
    Z = R // 2
    ahead = min(4, L)
    r, c = lax.axis_index("row"), lax.axis_index("col")
    z, core = r // 2, lax.rem(r, 2)
    sib = 2 * z + 1 - core

    def row_to(d):
        return lax.rem(r + d, R)

    def row_from(d):
        return lax.rem(r + R - d, R)

    def col_to(d):
        return lax.rem(c + d, C)

    def z_to(d):
        return 2 * lax.rem(z + d, Z) + core

    def z_from(d):
        return 2 * lax.rem(z + Z - d, Z) + core

    def rows(at, size):
        return pl.ds(pl.multiple_of(at * size, size), size)

    def rcopy(src, dst, cat, recv, **dev):
        return pltpu.make_async_remote_copy(
            src_ref=src, dst_ref=dst, send_sem=send.at[cat], recv_sem=recv,
            device_id=dev, device_id_type=MESH,
        )

    barrier = pltpu.get_barrier_semaphore()
    for d in range(1, R):
        pl.semaphore_signal(barrier, inc=1, device_id={"row": row_to(d)}, device_id_type=MESH)
    for d in range(1, C):
        pl.semaphore_signal(barrier, inc=1, device_id={"col": col_to(d)}, device_id_type=MESH)
    pl.semaphore_wait(barrier, R + C - 2)

    def g_block(l, at, which):
        return G.at[l, rows(2 * at + which, TR)]

    def g_own(l, step):
        if step == 0:
            return rcopy(grads.at[l], g_block(l, z, core), 2, g_fw.at[l, z], row=sib)
        return rcopy(grads.at[l], g_block(l, z, core), 0, g_in.at[l, z], row=r + 2 * step)

    def g_pass(l, at, step):
        block = g_block(l, at, core)
        if step == 0:
            return rcopy(block, block, 2, g_fw.at[l, at], row=sib)
        return rcopy(block, block, 0, g_in.at[l, at], row=r + 2 * step)

    def g_own_each(l, act):
        act(g_own(l, 0))

        @pl.when(z < Z - 1)
        def _():
            act(g_own(l, 1))

        @pl.when(z > 0)
        def _():
            act(g_own(l, -1))

    def g_relay(l, d, act, arrive):
        for step in (1, -1):
            at = z - step * d

            @pl.when(jnp.logical_and(at >= 0, at < Z))
            def _():
                if arrive:
                    rcopy(grads.at[l], g_block(l, at, core), 0, g_in.at[l, at], row=r).wait_recv()

                @pl.when(jnp.logical_and(z + step >= 0, z + step < Z))
                def _():
                    act(g_pass(l, at, step))

                act(g_pass(l, at, 0))

    def a_copy(l, d):
        return rcopy(acts.at[l], A.at[l, rows(c, TC)], 1, a_in.at[l, d], col=col_to(d))

    def rs_copy(l, d):
        return rcopy(rs_send.at[d, l], rs_recv.at[d, l], 3, rs_in.at[l, d], col=col_to(d))

    def sq_copy(d):
        return rcopy(sq.at[r], sq.at[r], 4, sq_in.at[d], row=row_to(d))

    def dt_copy(l, d):
        return rcopy(dt.at[r, l], dt.at[r, l], 5, dt_in.at[l, d], row=row_to(d))

    def at_z(d):
        return lax.rem(z + d, Z)

    def im_copy(d):
        if d == 0:
            return rcopy(im_send.at[1 - core], im_sib, 6, im_in.at[0], row=sib)
        return rcopy(im_acc.at[at_z(d)], im_recv.at[z], 7, im_in.at[d], row=z_to(d))

    def io_fw_copy(l):
        return rcopy(io_send.at[1 - core, l], io_sib.at[l], 8, io_fw.at[l], row=sib)

    def io_copy(l, d):
        return rcopy(io_acc.at[at_z(d), l], io_recv.at[z, l], 9, io_in.at[l, d], row=z_to(d))

    def og_copy(d):
        return rcopy(og.at[r], og.at[r], 11, og_in.at[d], row=sib if d == 0 else z_to(d))

    def og_fw_copy(d):
        return rcopy(og.at[z_from(d)], og.at[z_from(d)], 12, og_fw.at[d], row=sib)

    def q_copy(d):
        return rcopy(q, q_recv.at[d], 10, q_in.at[d], col=col_to(d))

    loads[0].wait()
    loads[1].wait()

    @pl.loop(0, L)
    def _(l):
        @pl.when(l < ahead)
        def _():
            g_own_each(l, lambda copy: copy.start())

        for d in range(1, C):
            a_copy(l, d).start()

    for copy in loads[2:]:
        copy.wait()

    @pl.loop(0, L)
    def _(l):
        G[l, rows(r, TR)] = grads[l]
        A[l, rows(c, TC)] = acts[l]
        m = frozen[l].astype(F32) + mm(ain[l], aout[l], ((0,), (0,)))
        merged[l] = m
        low = m.astype(BF16)
        wlow[l] = low
        sq[r, l] = jnp.sum(m * m, axis=0, keepdims=True)
        inner = mm(ain[l], low, ((1,), (0,)))
        for s in range(R):
            im_send[s % 2, s // 2, l] = inner[s * k:(s + 1) * k]

    for d in range(1, R):
        sq_copy(d).start()
    im_copy(0).start()
    for l in range(L):
        mag3[l] = mag[l:l + 1]
    if ahead < L:
        g_own_each(ahead, lambda copy: copy.start())

    def scales_ready():
        for d in range(1, R):
            rcopy(sq.at[r], sq.at[row_from(d)], 4, sq_in.at[d], row=r).wait_recv()
        total = sq[0]
        for s in range(1, R):
            total = total + sq[s]
        norms = jnp.sqrt(total + 0.25)
        cor[...] = norms
        scl[...] = mag3[...] / norms

    def pass_on(l):
        rcopy(io_sib.at[l], io_sib.at[l], 8, io_fw.at[l], row=sib).wait_recv()
        for s in range(Z):
            io_acc[s, l] = io_send[core, l, s] + io_sib[l, s]
        for d in range(1, Z):
            io_copy(l, d).start()
        io_recv[z, l] = io_acc[z, l]

    def compute(l):
        for at in range(Z):
            rcopy(grads.at[l], g_block(l, at, 1 - core), 2, g_fw.at[l, at], row=r).wait_recv()
        scale = scl[l]
        g = G[l]
        scaled = (g.astype(F32) * scale).astype(BF16)
        prod[...] = mm(scaled, wlow[l], ((1,), (1,)))
        for d in range(1, C):
            rs_send[d, l] = prod[rows(col_to(d), TC)].astype(BF16)
            rs_copy(l, d).start()
        own[l] = prod[rows(c, TC)]
        for d in range(1, C):
            src = lax.rem(c + C - d, C)
            rcopy(acts.at[l], A.at[l, rows(src, TC)], 1, a_in.at[l, d], col=c).wait_recv()
        outer = mm(A[l], g, ((0,), (0,)))
        dt[r, l] = jnp.sum(merged[l] * outer, axis=0, keepdims=True)
        for d in range(1, R):
            dt_copy(l, d).start()
        inner = mm(ain[l], outer.astype(BF16), ((1,), (0,)))
        for s in range(R):
            io_send[s % 2, l, s // 2] = inner[s * k:(s + 1) * k]
        io_fw_copy(l).start()

        @pl.when(l > 0)
        def _():
            pass_on(l - 1)

        ing[l] = mm(aout[l], (outer * scale).astype(BF16), ((1,), (1,)))

    @pl.loop(0, L + Z - 1)
    def _(at):
        @pl.when(at + ahead + 1 < L)
        def _():
            g_own_each(at + ahead + 1, lambda copy: copy.start())

        for d in range(1, Z):
            l = at - (d - 1)

            @pl.when(jnp.logical_and(l >= 0, l < L))
            def _():
                g_relay(l, d, lambda copy: copy.start(), True)

        @pl.when(at == L + Z - 3)
        def _():
            im_copy(0).wait_recv()
            im_acc[...] = im_send[core] + im_sib[...]
            for d in range(1, Z):
                im_copy(d).start()
            im_recv[z] = im_acc[z]

        @pl.when(at == Z - 1)
        def _():
            scales_ready()

        @pl.when(at >= Z - 1)
        def _():
            compute(at - (Z - 1))

    pass_on(L - 1)

    @pl.loop(0, L)
    def _(l):
        for d in range(1, R):
            rcopy(dt.at[r, l], dt.at[row_from(d), l], 5, dt_in.at[l, d], row=r).wait_recv()

    dots = dt[0]
    for s in range(1, R):
        dots = dots + dt[s]
    norms = cor[...]
    ratio = dots / norms
    for l in range(L):
        mgrad[l:l + 1] = ratio[l]
    saves[0].start()
    cor[...] = -mag3[...] * dots / (norms * norms * norms)

    @pl.loop(0, L)
    def _(l):
        adjusted = (merged[l] * cor[l]).astype(BF16)
        part = ing[l] + mm(aout[l], adjusted, ((1,), (1,)))
        ing[l] = part
        q[l] = part.astype(BF16)

    for d in range(1, C):
        q_copy(d).start()
    for d in range(1, Z):
        src = lax.rem(z + Z - d, Z)
        rcopy(im_recv.at[z], im_recv.at[src], 7, im_in.at[d], row=r).wait_recv()

    @pl.loop(0, L)
    def _(l):
        for d in range(1, Z):
            src = lax.rem(z + Z - d, Z)
            rcopy(io_recv.at[z, l], io_recv.at[src, l], 9, io_in.at[l, d], row=r).wait_recv()
        summed, side = io_recv[0, l], im_recv[0, l]
        for s in range(1, Z):
            summed = summed + io_recv[s, l]
            side = side + im_recv[s, l]
        og[r, l] = summed * scl[l] + side * cor[l]

    for d in range(Z):
        og_copy(d).start()

    @pl.loop(0, L)
    def _(l):
        result = own[l]
        for d in range(1, C):
            rcopy(rs_send.at[d, l], rs_recv.at[d, l], 3, rs_in.at[l, d], col=c).wait_recv()
            result = result + rs_recv[d, l].astype(F32)
        ig[l] = result.astype(BF16)

    saves[1].start()

    for d in range(1, C):
        rcopy(q, q_recv.at[d], 10, q_in.at[d], col=c).wait_recv()

    @pl.loop(0, L)
    def _(l):
        result = ing[l]
        for d in range(1, C):
            result = result + q_recv[d, l].astype(F32)
        ing[l] = result

    saves[2].start()

    for d in range(1, Z):
        rcopy(og.at[r], og.at[z_from(d)], 11, og_in.at[d], row=r).wait_recv()
        og_fw_copy(d).start()
    rcopy(og.at[r], og.at[sib], 11, og_in.at[0], row=r).wait_recv()
    for d in range(1, Z):
        from_sib = 2 * lax.rem(z + Z - d, Z) + 1 - core
        rcopy(og.at[r], og.at[from_sib], 12, og_fw.at[d], row=r).wait_recv()

    @pl.loop(0, L)
    def _(l):
        for s in range(R):
            oug[l, s * k:(s + 1) * k] = og[s, l]

    saves[3].start()

    @pl.loop(0, L)
    def _(l):
        g_own_each(l, lambda copy: copy.wait_send())
        for d in range(1, Z):
            g_relay(l, d, lambda copy: copy.wait_send(), False)
        for d in range(1, C):
            a_copy(l, d).wait_send()
            rs_copy(l, d).wait_send()

    @pl.loop(0, L)
    def _(l):
        for d in range(1, R):
            dt_copy(l, d).wait_send()
        io_fw_copy(l).wait_send()
        for d in range(1, Z):
            io_copy(l, d).wait_send()

    for d in range(1, R):
        sq_copy(d).wait_send()
    for d in range(Z):
        im_copy(d).wait_send()
        og_copy(d).wait_send()
    for d in range(1, Z):
        og_fw_copy(d).wait_send()
    for d in range(1, C):
        q_copy(d).wait_send()
    for copy in saves:
        copy.wait()


def finish(ig, ing, oug, mgrad, ig_out, ing_out, oug_out, mgrad_out, sem):
    pairs = ((ig, ig_out), (ing, ing_out), (oug, oug_out), (mgrad, mgrad_out))
    copies = [pltpu.make_async_copy(a, b, sem.at[i]) for i, (a, b) in enumerate(pairs)]
    for copy in copies:
        copy.start()
    for copy in copies:
        copy.wait()


def body(R, C, acts, grads, frozen, ain, aout, mag):
    L, TR, W = grads.shape
    TC, KI = acts.shape[1:]
    RANK = ain.shape[1]
    k, T, Z = RANK // R, TR * R, R // 2
    V = pltpu.VMEM
    dma = pltpu.SemaphoreType.DMA
    vm = pl.BlockSpec(memory_space=pltpu.VMEM)
    hbm = pl.BlockSpec(memory_space=pltpu.HBM)
    ig, ing, oug, mgrad = pl.pallas_call(
        functools.partial(kernel, R, C),
        out_shape=(
            V((L, TC, KI), BF16),
            V((L, RANK, KI), F32),
            V((L, RANK, W), F32),
            V((L, W), F32),
        ),
        in_specs=[hbm] * 6,
        out_specs=(vm,) * 4,
        scratch_shapes=[
            V(acts.shape, BF16), V(grads.shape, BF16), V(frozen.shape, BF16),
            V(ain.shape, BF16), V(aout.shape, BF16), V(mag.shape, F32),
            V((L, TC, KI), BF16), V((L, RANK, KI), F32), V((L, RANK, W), F32), V((L, W), F32),
            dma((6,)), dma((4,)),
            V((L, T, W), BF16), V((L, T, KI), BF16), V((L, KI, W), F32), V((L, KI, W), BF16),
            V((T, KI), F32), V((L, TC, KI), F32), V((C, L, TC, KI), BF16), V((C, L, TC, KI), BF16),
            V((R, L, 1, W), F32), V((R, L, 1, W), F32),
            V((2, Z, L, k, W), F32), V((Z, L, k, W), F32), V((Z, L, k, W), F32), V((Z, L, k, W), F32),
            V((2, L, Z, k, W), F32), V((L, Z, k, W), F32), V((Z, L, k, W), F32), V((Z, L, k, W), F32),
            V((R, L, k, W), F32), V((L, RANK, KI), BF16), V((C, L, RANK, KI), BF16),
            V((L, 1, W), F32), V((L, 1, W), F32), V((L, 1, W), F32),
            dma((13,)), dma((L, Z)), dma((L, Z)), dma((L, C)), dma((L, C)),
            dma((R,)), dma((L, R)), dma((Z,)), dma((L, Z)), dma((L,)), dma((Z,)), dma((Z,)), dma((C,)),
        ],
        compiler_params=pltpu.CompilerParams(
            collective_id=0, has_side_effects=True, vmem_limit_bytes=60 * 1024 * 1024
        ),
    )(acts, grads, frozen, ain, aout, mag)
    return pl.pallas_call(
        finish,
        out_shape=tuple(jax.ShapeDtypeStruct(x.shape, x.dtype) for x in (ig, ing, oug, mgrad)),
        in_specs=[vm] * 4,
        out_specs=(hbm,) * 4,
        scratch_shapes=[dma((4,))],
        compiler_params=pltpu.CompilerParams(vmem_limit_bytes=1024 * 1024),
    )(ig, ing, oug, mgrad)


def solution(mesh):
    return jax.shard_map(
        functools.partial(body, mesh.shape["row"], mesh.shape["col"]),
        mesh=mesh,
        in_specs=(
            P(None, "col", "row"),
            P(None, "row", "col"),
            P(None, "row", "col"),
            P(None, None, "row"),
            P(None, None, "col"),
            P(None, "col"),
        ),
        out_specs=(
            P(None, "col", "row"),
            P(None, None, "row"),
            P(None, None, "col"),
            P(None, "col"),
        ),
        check_vma=False,
    )
```

```python
import functools

import jax
import jax.numpy as jnp
from jax import lax
from jax.experimental import pallas as pl
from jax.experimental.pallas import tpu as pltpu
from jax.sharding import PartitionSpec as P

MESH = pl.DeviceIdType.MESH
F32 = jnp.float32
BF16 = jnp.bfloat16


def mm(a, b, dims):
    return lax.dot_general(a, b, (dims, ((), ())), preferred_element_type=F32)


NAMES = (
    "acts", "grads", "frozen", "ain", "aout", "mag", "load", "G", "A", "merged", "ws", "asc", "sqm", "sq_sib",
    "sq_z", "sq_tot", "norms", "scl", "cor", "mag3", "mg3", "prod_buf", "qs", "q_sib", "q_all", "Qg", "Qc", "ims",
    "im_sib", "im_all", "im_fin", "dt", "q", "q_recv", "q1_r", "q2_s", "q2_r", "own", "hold", "rs1_s", "rs1_r",
    "rs2_s", "rs2_r", "send", "g_in", "g_fw", "a_in", "rs1_in", "rs2_in", "sq_in", "dt_in", "root_in", "out_in",
    "col_in", "sib_in", "q_in", "q1_in", "q2_in",
)


def scratch(R, C, L, TR, W, TC, KI, RANK):
    Z, T, H, KH = R // 2, TR * R, L // 2, KI // 2
    V, dma = pltpu.VMEM, pltpu.SemaphoreType.DMA
    wide = (2, L, 2, TC, KH) if C == 4 else (C, L, TC, KI)
    slim = (2, L, TC, KH) if C == 4 else (1, 1, 8, 128)
    col = (L, 4) if C == 4 else (L, C)
    pair = (L, 2, RANK, KH) if C == 4 else (L, 1, RANK, KI)
    return dict(
        acts=V((L, TC, KI), BF16), grads=V((L, TR, W), BF16), frozen=V((L, KI, W), BF16),
        ain=V((L, RANK, KI), BF16), aout=V((L, RANK, W), BF16), mag=V((L, W), F32), load=dma((6,)),
        G=V((L, T, W), BF16), A=V((L, T, KI), BF16), merged=V((L, KI, W), F32), ws=V((L, KI, W), BF16),
        asc=V((L, RANK, W), BF16),
        sqm=V((L, 1, W), F32), sq_sib=V((H, 1, W), F32), sq_z=V((Z, H, 1, W), F32), sq_tot=V((2, H, 1, W), F32),
        norms=V((L, 1, W), F32), scl=V((L, 1, W), F32), cor=V((L, 1, W), F32), mag3=V((L, 1, W), F32),
        mg3=V((L, 1, W), F32),
        prod_buf=V((T, KI), F32), qs=V((2, H, RANK, TC), F32), q_sib=V((H, RANK, TC), F32), q_all=V((Z, H, RANK, TC), F32),
        Qg=V((2, C, H, RANK, TC), BF16), Qc=V((L, RANK, T), BF16),
        ims=V((2, H, RANK, W), F32), im_sib=V((H, RANK, W), F32), im_all=V((Z, H, RANK, W), BF16),
        im_fin=V((2, H, RANK, W), BF16),
        dt=V((R, L, 1, W), F32), q=V(pair, BF16), q_recv=V((C,) + pair, BF16),
        q1_r=V(pair, BF16), q2_s=V(pair, BF16), q2_r=V(pair, BF16),
        own=V((L, TC, KI), F32), hold=V(slim, F32), rs1_s=V(wide, BF16), rs1_r=V(wide, BF16),
        rs2_s=V(slim, BF16), rs2_r=V(slim, BF16),
        send=dma((16,)), g_in=dma((L, Z)), g_fw=dma((L, Z)), a_in=dma(col), rs1_in=dma(col), rs2_in=dma((L, 2)),
        sq_in=dma((Z,)), dt_in=dma((L, R)), root_in=dma((2, Z)), out_in=dma((2,)), col_in=dma((C,)),
        sib_in=dma((6,)), q_in=dma((L, C)), q1_in=dma((L, 2)), q2_in=dma((L, 2)),
    )


def kernel(R, C, *refs):
    acts_hbm, grads_hbm, frozen_hbm, ain_hbm, aout_hbm, mag_hbm, ig, ing, oug, mgrad = refs[:10]
    (acts, grads, frozen, ain, aout, mag, load, G, A, merged, ws, asc, sqm, sq_sib, sq_z, sq_tot, norms, scl, cor,
     mag3, mg3, prod_buf, qs, q_sib, q_all, Qg, Qc, ims, im_sib, im_all, im_fin, dt, q, q_recv, q1_r, q2_s, q2_r,
     own, hold, rs1_s, rs1_r, rs2_s, rs2_r, send, g_in, g_fw, a_in, rs1_in, rs2_in, sq_in, dt_in, root_in, out_in, col_in,
     sib_in, q_in, q1_in, q2_in) = refs[10:]
    pairs = ((grads_hbm, grads), (acts_hbm, acts), (frozen_hbm, frozen),
             (ain_hbm, ain), (aout_hbm, aout), (mag_hbm, mag))
    loads = [pltpu.make_async_copy(a, b, load.at[i]) for i, (a, b) in enumerate(pairs)]
    for copy in loads:
        copy.start()
    L, TR, W = grads.shape
    TC, KI = acts.shape[1:]
    Z, H, KH = R // 2, L // 2, KI // 2
    ahead = min(3, L)
    last = L + Z - 3
    r, c = lax.axis_index("row"), lax.axis_index("col")
    z, core = r // 2, lax.rem(r, 2)
    sib = 2 * z + 1 - core
    square = C == 4
    xn, yn = c + 1 - 2 * lax.rem(c, 2), lax.rem(c + 2, 4)
    dg = 3 - c
    root = Z // 2 - 1 + core
    middle = jnp.logical_and(z > 0, z < Z - 1)
    halves = 2 if square else 1
    KS = KI // halves

    def row_to(d):
        return lax.rem(r + d, R)

    def row_from(d):
        return lax.rem(r + R - d, R)

    def col_to(d):
        return lax.rem(c + d, C)

    def col_from(d):
        return lax.rem(c + C - d, C)

    def z_to(d):
        return 2 * lax.rem(z + d, Z) + core

    def z_from(d):
        return lax.rem(z + Z - d, Z)

    def rows(at, size):
        return pl.ds(pl.multiple_of(at * size, size), size)

    def rcopy(src, dst, cat, recv, **dev):
        return pltpu.make_async_remote_copy(
            src_ref=src, dst_ref=dst, send_sem=send.at[cat], recv_sem=recv,
            device_id=dev, device_id_type=MESH,
        )

    def arrived(ref, recv):
        rcopy(ref, ref, 0, recv, row=r).wait_recv()

    barrier = pltpu.get_barrier_semaphore()
    for d in range(1, R):
        pl.semaphore_signal(barrier, inc=1, device_id={"row": row_to(d)}, device_id_type=MESH)
    for d in range(1, C):
        pl.semaphore_signal(barrier, inc=1, device_id={"col": col_to(d)}, device_id_type=MESH)
    pl.semaphore_wait(barrier, R + C - 2)

    def g_block(l, at, which):
        return G.at[l, rows(2 * at + which, TR)]

    def g_own(l, step):
        if step == 0:
            return rcopy(grads.at[l], g_block(l, z, core), 1, g_fw.at[l, z], row=sib)
        return rcopy(grads.at[l], g_block(l, z, core), 0, g_in.at[l, z], row=r + 2 * step)

    def g_pass(l, at, step):
        block = g_block(l, at, core)
        if step == 0:
            return rcopy(block, block, 1, g_fw.at[l, at], row=sib)
        return rcopy(block, block, 0, g_in.at[l, at], row=r + 2 * step)

    def g_own_each(l, act):
        @pl.when(z < Z - 1)
        def _():
            act(g_own(l, 1))

        @pl.when(z > 0)
        def _():
            act(g_own(l, -1))

        act(g_own(l, 0))

    def g_relay(l, d, act, arrive):
        for step in (1, -1):
            at = z - step * d

            @pl.when(jnp.logical_and(at >= 0, at < Z))
            def _():
                if arrive:
                    arrived(g_block(l, at, core), g_in.at[l, at])

                @pl.when(jnp.logical_and(z + step >= 0, z + step < Z))
                def _():
                    act(g_pass(l, at, step))

                act(g_pass(l, at, 0))

    def a_copies(l):
        mine = A.at[l, rows(c, TC)]
        if square:
            return [rcopy(acts.at[l], mine, 2, a_in.at[l, 0], col=xn), rcopy(acts.at[l], mine, 2, a_in.at[l, 1], col=yn)]
        return [rcopy(acts.at[l], mine, 2, a_in.at[l, d], col=col_to(d)) for d in range(1, C)]

    def a_half(l, of, part):
        size = TC // 2
        return A.at[l, rows(2 * of + part, size)]

    def a_passes(l):
        first, second = a_half(l, xn, 0), a_half(l, yn, 1)
        return [rcopy(first, first, 3, a_in.at[l, 2], col=yn), rcopy(second, second, 3, a_in.at[l, 3], col=xn)]

    def a_relay(l):
        arrived(A.at[l, rows(xn, TC)], a_in.at[l, 0])
        arrived(A.at[l, rows(yn, TC)], a_in.at[l, 1])
        for copy in a_passes(l):
            copy.start()

    def a_ready(l):
        if square:
            arrived(a_half(l, dg, 0), a_in.at[l, 2])
            arrived(a_half(l, dg, 1), a_in.at[l, 3])
        else:
            for d in range(1, C):
                arrived(A.at[l, rows(col_from(d), TC)], a_in.at[l, d])

    def rs1_copies(l):
        if square:
            return [rcopy(rs1_s.at[i, l], rs1_r.at[i, l], 4, rs1_in.at[l, i], col=to) for i, to in enumerate((xn, yn))]
        return [rcopy(rs1_s.at[d, l], rs1_r.at[d, l], 4, rs1_in.at[l, d], col=col_to(d)) for d in range(1, C)]

    def rs2_copies(l):
        return [rcopy(rs2_s.at[i, l], rs2_r.at[i, l], 5, rs2_in.at[l, i], col=to) for i, to in enumerate((yn, xn))]

    def rs_first(l, prod):
        if square:
            for i, near in enumerate((xn, yn)):
                rs1_s[i, l, 0] = prod[rows(near, TC), cols(i)].astype(BF16)
                rs1_s[i, l, 1] = prod[rows(dg, TC), cols(i)].astype(BF16)
                hold[i, l] = prod[rows((yn, xn)[i], TC), cols(i)]
        else:
            for d in range(1, C):
                rs1_s[d, l] = prod[rows(col_to(d), TC)].astype(BF16)
        own[l] = prod[rows(c, TC)]
        for copy in rs1_copies(l):
            copy.start()

    def rs_second(l):
        if square:
            for i in range(2):
                arrived(rs1_r.at[i, l], rs1_in.at[l, i])
                rs2_s[i, l] = (hold[i, l] + rs1_r[i, l, 1].astype(F32)).astype(BF16)
            for copy in rs2_copies(l):
                copy.start()

    def rs_finish(l):
        if square:
            for i in range(2):
                arrived(rs2_r.at[i, l], rs2_in.at[l, i])
                total = own[l, :, cols(i)] + rs1_r[i, l, 0].astype(F32) + rs2_r[i, l].astype(F32)
                ig[l, :, cols(i)] = total.astype(BF16)
        else:
            total = own[l]
            for d in range(1, C):
                arrived(rs1_r.at[d, l], rs1_in.at[l, d])
                total = total + rs1_r[d, l].astype(F32)
            ig[l] = total.astype(BF16)

    def sq_copy(d):
        return rcopy(sq_z.at[z], sq_z.at[z], 6, sq_in.at[d], row=z_to(d))

    to_sib = [
        rcopy(sqm.at[pl.ds((1 - core) * H, H)], sq_sib, 7, sib_in.at[0], row=sib),
        rcopy(sq_tot.at[core], sq_tot.at[core], 7, sib_in.at[1], row=sib),
        rcopy(qs.at[1 - core], q_sib, 7, sib_in.at[2], row=sib),
        rcopy(ims.at[1 - core], im_sib, 7, sib_in.at[3], row=sib),
        rcopy(Qg.at[core], Qg.at[core], 7, sib_in.at[4], row=sib),
        rcopy(im_fin.at[core], im_fin.at[core], 7, sib_in.at[5], row=sib),
    ]

    def root_copies():
        return [rcopy(q_all.at[z], q_all.at[z], 8, root_in.at[0, z], row=2 * root + core),
                rcopy(im_all.at[z], im_all.at[z], 9, root_in.at[1, z], row=2 * root + core)]

    def out_ref(i):
        return Qg.at[core, c] if i == 0 else im_fin.at[core]

    def out_copies(i):
        ref = out_ref(i)
        return [rcopy(ref, ref, 10 + i, out_in.at[i], row=z_to(d)) for d in range(1, Z)]

    def gather_copies():
        mine = Qg.at[core, c]
        return [rcopy(mine, mine, 12, col_in.at[d], col=col_to(d)) for d in range(1, C)]

    def start(copy):
        copy.start()

    def to_root():
        arrived(q_sib, sib_in.at[2])
        arrived(im_sib, sib_in.at[3])
        q_all[z] = qs[core] + q_sib[...]
        im_all[z] = (ims[core] + im_sib[...]).astype(BF16)

        @pl.when(z != root)
        def _():
            for copy in root_copies():
                copy.start()

    def at_root():
        for d in range(1, Z):
            arrived(q_all.at[z_from(d)], root_in.at[0, z_from(d)])
            arrived(im_all.at[z_from(d)], root_in.at[1, z_from(d)])
        q_sum, im_sum = q_all[0], im_all[0].astype(F32)
        for s in range(1, Z):
            q_sum = q_sum + q_all[s]
            im_sum = im_sum + im_all[s].astype(F32)
        Qg[core, c] = q_sum.astype(BF16)
        im_fin[core] = im_sum.astype(BF16)
        for copy in out_copies(0) + gather_copies():
            copy.start()

    def q_arrived():
        arrived(out_ref(0), out_in.at[0])
        for copy in gather_copies():
            copy.start()

    def dt_copy(l, d):
        return rcopy(dt.at[r, l], dt.at[r, l], 13, dt_in.at[l, d], row=row_to(d))

    def q_copies(l):
        return [rcopy(q.at[l], q_recv.at[d, l], 14, q_in.at[l, d], col=col_to(d)) for d in range(1, C)]

    def q1_copies(l):
        return [rcopy(q.at[l, i], q1_r.at[l, i], 15, q1_in.at[l, i], col=to) for i, to in enumerate((xn, yn))]

    def q2_copies(l):
        return [rcopy(q2_s.at[l, i], q2_r.at[l, i], 15, q2_in.at[l, i], col=to) for i, to in enumerate((yn, xn))]

    def cols(i):
        return slice(i * KS, (i + 1) * KS)

    loads[0].wait()
    loads[1].wait()

    @pl.loop(0, ahead)
    def _(l):
        g_own_each(l, start)

    @pl.loop(0, L)
    def _(l):
        for copy in a_copies(l):
            copy.start()

    for copy in loads[2:]:
        copy.wait()

    @pl.loop(0, L)
    def _(l):
        m = frozen[l].astype(F32) + mm(ain[l], aout[l], ((0,), (0,)))
        merged[l] = m
        sqm[l] = jnp.sum(m * m, axis=0, keepdims=True)

    to_sib[0].start()

    @pl.loop(0, L)
    def _(l):
        G[l, rows(r, TR)] = grads[l]
        A[l, rows(c, TC)] = acts[l]
        half, at = l // H, lax.rem(l, H)
        ims[half, at] = mm(ain[l], merged[l].astype(BF16), ((1,), (0,)))
        qs[half, at] = mm(ain[l], acts[l], ((1,), (1,)))

    to_sib[2].start()
    to_sib[3].start()
    for l in range(L):
        mag3[l] = mag[l:l + 1]

    def squares_out():
        arrived(sq_sib, sib_in.at[0])
        sq_z[z] = sqm[pl.ds(core * H, H)] + sq_sib[...]
        for d in range(1, Z):
            sq_copy(d).start()

    def squares_sum():
        for d in range(1, Z):
            arrived(sq_z.at[z_from(d)], sq_in.at[d])
        total = sq_z[0]
        for s in range(1, Z):
            total = total + sq_z[s]
        sq_tot[core] = total
        to_sib[1].start()

    def scales():
        arrived(sq_tot.at[1 - core], sib_in.at[1])

        @pl.loop(0, L)
        def _(l):
            n = jnp.sqrt(sq_tot[l // H, lax.rem(l, H)] + 0.25)
            s = mag3[l] / n
            norms[l] = n
            scl[l] = s
            ws[l] = (merged[l] * s).astype(BF16)
            asc[l] = (aout[l].astype(F32) * s).astype(BF16)

    def compute(l):
        for at in range(Z):
            arrived(g_block(l, at, 1 - core), g_fw.at[l, at])
        a_ready(l)
        g = G[l]
        outer = mm(A[l], g, ((0,), (0,)))
        dt[r, l] = jnp.sum(merged[l] * outer, axis=0, keepdims=True)
        for d in range(1, R):
            dt_copy(l, d).start()
        low = outer.astype(BF16)
        prod_buf[...] = mm(g, ws[l], ((1,), (1,)))
        rs_first(l, prod_buf)
        ing[l] = mm(asc[l], low, ((1,), (1,)))

        @pl.when(l > 1)
        def _():
            rs_second(l - 2)

    def correct(l, direct):
        for d in range(1, R):
            arrived(dt.at[row_from(d), l], dt_in.at[l, d])
        dots = dt[0, l]
        for s in range(1, R):
            dots = dots + dt[s, l]
        n = norms[l]
        mg3[l] = dots / n
        factor = -mag3[l] * dots / (n * n * n)
        cor[l] = factor
        adjusted = (merged[l] * factor).astype(BF16)
        part = ing[l] + mm(aout[l], adjusted, ((1,), (1,)))
        ing[l] = part
        for i in range(halves):
            q[l, i] = part[:, cols(i)].astype(BF16)
        for copy in q_copies(l) if direct else q1_copies(l):
            copy.start()

    def q_second(l):
        for i in range(2):
            arrived(q1_r.at[l, i], q1_in.at[l, i])
            total = ing[l, :, cols(i)] + q1_r[l, i].astype(F32)
            ing[l, :, cols(i)] = total
            q2_s[l, i] = total.astype(BF16)
        for copy in q2_copies(l):
            copy.start()

    def relays(at):
        @pl.when(at + ahead < L)
        def _():
            g_own_each(at + ahead, start)

        for d in range(1, Z):
            l = at - (d - 1)

            @pl.when(jnp.logical_and(l >= 0, l < L))
            def _():
                g_relay(l, d, start, True)

    squares_out()
    lead = 1

    @pl.when(middle)
    def _():
        for at in range(lead):
            relays(at)

    shift = jnp.where(middle, lead, 0)

    @pl.loop(0, last + 1)
    def _(at):
        relays(at + shift)

        if square:
            for l in (2 * at - 1, 2 * at):
                @pl.when(jnp.logical_and(l >= 0, l < L))
                def _():
                    a_relay(l)

        @pl.when(at == 1)
        def _():
            to_root()

        @pl.when(jnp.logical_and(at == min(last - 2, Z), z == root))
        def _():
            at_root()

        @pl.when(jnp.logical_and(at == last, z != root))
        def _():
            q_arrived()

        @pl.when(jnp.logical_and(at == last - 1, z == root))
        def _():
            for copy in out_copies(1):
                copy.start()
            to_sib[5].start()

        @pl.when(at == Z - 2)
        def _():
            squares_sum()
            scales()

        @pl.when(at >= Z - 2)
        def _():
            compute(at - (Z - 2))

        if square:
            @pl.when(jnp.logical_and(jnp.logical_not(middle), at - Z - 1 >= 0))
            def _():
                correct(at - Z - 1, False)

    rs_second(L - 2)

    @pl.loop(jnp.where(middle, 0, jnp.maximum(last - Z, 0)) if square else 0, L - 2)
    def _(l):
        correct(l, not square)

    for d in range(1, C):
        arrived(Qg.at[core, col_from(d)], col_in.at[d])
    to_sib[4].start()

    @pl.when(z != root)
    def _():
        arrived(out_ref(1), out_in.at[1])
        to_sib[5].start()

    correct(L - 2, not square)

    arrived(Qg.at[1 - core], sib_in.at[4])

    @pl.loop(0, L)
    def _(l):
        half, at = l // H, lax.rem(l, H)
        for s in range(C):
            Qc[l, :, s * TC:(s + 1) * TC] = Qg[half, s, at]
        oug[l] = mm(Qc[l], G[l], ((1,), (0,))) * scl[l]

    rs_second(L - 1)

    if square:
        @pl.loop(0, L - 1)
        def _(l):
            q_second(l)

    correct(L - 1, True)
    for l in range(L):
        mgrad[l:l + 1] = mg3[l]

    arrived(im_fin.at[1 - core], sib_in.at[5])

    @pl.loop(0, L)
    def _(l):
        oug[l] += im_fin[l // H, lax.rem(l, H)].astype(F32) * cor[l]

    @pl.loop(0, L)
    def _(l):
        rs_finish(l)

    if square:
        @pl.loop(0, L - 1)
        def _(l):
            for i in range(2):
                arrived(q2_r.at[l, i], q2_in.at[l, i])
                ing[l, :, cols(i)] += q2_r[l, i].astype(F32)

    @pl.loop(L - 1 if square else 0, L)
    def _(l):
        for i in range(halves):
            total = ing[l, :, cols(i)]
            for d in range(1, C):
                if i == 0:
                    arrived(q_recv.at[d, l], q_in.at[l, d])
                total = total + q_recv[d, l, i].astype(F32)
            ing[l, :, cols(i)] = total

    def done(copy):
        copy.wait_send()

    @pl.loop(0, L)
    def _(l):
        g_own_each(l, done)
        for d in range(1, Z):
            g_relay(l, d, done, False)
        sent = a_copies(l) + rs1_copies(l) + [dt_copy(l, d) for d in range(1, R)]
        if square:
            sent += a_passes(l) + rs2_copies(l)
        for copy in sent:
            copy.wait_send()

    @pl.loop(0, L - 1)
    def _(l):
        for copy in q1_copies(l) + q2_copies(l) if square else q_copies(l):
            copy.wait_send()

    for copy in to_sib + [sq_copy(d) for d in range(1, Z)] + gather_copies() + q_copies(L - 1):
        copy.wait_send()

    @pl.when(z == root)
    def _():
        for copy in out_copies(0) + out_copies(1):
            copy.wait_send()

    @pl.when(z != root)
    def _():
        for copy in root_copies():
            copy.wait_send()


def finish(ig, ing, oug, mgrad, ig_out, ing_out, oug_out, mgrad_out, sem):
    pairs = ((ig, ig_out), (ing, ing_out), (oug, oug_out), (mgrad, mgrad_out))
    copies = [pltpu.make_async_copy(a, b, sem.at[i]) for i, (a, b) in enumerate(pairs)]
    for copy in copies:
        copy.start()
    for copy in copies:
        copy.wait()


def body(R, C, acts, grads, frozen, ain, aout, mag):
    L, TR, W = grads.shape
    TC, KI = acts.shape[1:]
    RANK = ain.shape[1]
    V = pltpu.VMEM
    vm = pl.BlockSpec(memory_space=pltpu.VMEM)
    hbm = pl.BlockSpec(memory_space=pltpu.HBM)
    buffers = scratch(R, C, L, TR, W, TC, KI, RANK)
    ig, ing, oug, mgrad = pl.pallas_call(
        functools.partial(kernel, R, C),
        out_shape=(V((L, TC, KI), BF16), V((L, RANK, KI), F32), V((L, RANK, W), F32), V((L, W), F32)),
        in_specs=[hbm] * 6,
        out_specs=(vm,) * 4,
        scratch_shapes=[buffers[name] for name in NAMES],
        compiler_params=pltpu.CompilerParams(
            collective_id=0, has_side_effects=True, vmem_limit_bytes=60 * 1024 * 1024
        ),
    )(acts, grads, frozen, ain, aout, mag)
    return pl.pallas_call(
        finish,
        out_shape=tuple(jax.ShapeDtypeStruct(x.shape, x.dtype) for x in (ig, ing, oug, mgrad)),
        in_specs=[vm] * 4,
        out_specs=(hbm,) * 4,
        scratch_shapes=[pltpu.SemaphoreType.DMA((4,))],
        compiler_params=pltpu.CompilerParams(vmem_limit_bytes=1024 * 1024),
    )(ig, ing, oug, mgrad)


def solution(mesh):
    return jax.shard_map(
        functools.partial(body, mesh.shape["row"], mesh.shape["col"]),
        mesh=mesh,
        in_specs=(
            P(None, "col", "row"),
            P(None, "row", "col"),
            P(None, "row", "col"),
            P(None, None, "row"),
            P(None, None, "col"),
            P(None, "col"),
        ),
        out_specs=(
            P(None, "col", "row"),
            P(None, None, "row"),
            P(None, None, "col"),
            P(None, "col"),
        ),
        check_vma=False,
    )
```

```python
import functools

import jax
import jax.numpy as jnp
from jax import lax
from jax.experimental import pallas as pl
from jax.experimental.pallas import tpu as pltpu
from jax.sharding import PartitionSpec as P

MESH = pl.DeviceIdType.MESH
F32 = jnp.float32
BF16 = jnp.bfloat16


def mm(a, b, dims):
    return lax.dot_general(a, b, (dims, ((), ())), preferred_element_type=F32)


NAMES = (
    "acts", "grads", "frozen", "ain", "aout", "mag", "load", "G", "A", "merged", "ws", "asc", "sqm", "sq_sib", "sq_z",
    "sq_tot", "norms", "scl", "cor", "mag3", "mg3", "prod_buf", "qs", "q_sib", "q_all", "Qg", "Qc", "ims", "im_sib",
    "im_all", "im_fin", "dt_part", "dt_sib", "dt_z", "dt_tot", "dt_all", "q", "q_recv", "q1_r", "q2_s", "q2_r", "own",
    "hold", "rs1_s", "rs1_r", "rs2_s", "rs2_r", "send", "g_in", "g_fw", "a_in", "rs1_in", "rs2_in", "sq_in", "dt_in",
    "dt_last", "root_in", "out_in", "col_in", "sib_in", "news", "q_in", "q1_in", "q2_in",
)


def scratch(R, C, L, TR, W, TC, KI, RANK):
    Z, T, H, KH = R // 2, TR * R, L // 2, KI // 2
    V, dma = pltpu.VMEM, pltpu.SemaphoreType.DMA
    wide = (2, L, 2, TC, KH) if C == 4 else (C, L, TC, KI)
    slim = (2, L, TC, KH) if C == 4 else (1, 1, 8, 128)
    pair = (L, 2, RANK, KH) if C == 4 else (L, 1, RANK, KI)
    return dict(
        acts=V((L, TC, KI), BF16), grads=V((L, TR, W), BF16), frozen=V((L, KI, W), BF16),
        ain=V((L, RANK, KI), BF16), aout=V((L, RANK, W), BF16), mag=V((L, W), F32), load=dma((6,)),
        G=V((L, T, W), BF16), A=V((L, T, KI), BF16), merged=V((L, KI, W), F32), ws=V((L, KI, W), BF16),
        asc=V((L, RANK, W), BF16),
        sqm=V((L, 1, W), F32), sq_sib=V((H, 1, W), F32), sq_z=V((Z, H, 1, W), F32), sq_tot=V((2, H, 1, W), F32),
        norms=V((L, 1, W), F32), scl=V((L, 1, W), F32), cor=V((L, 1, W), F32), mag3=V((L, 1, W), F32),
        mg3=V((L, 1, W), F32),
        prod_buf=V((T, KI), F32), qs=V((2, H, RANK, TC), F32), q_sib=V((H, RANK, TC), F32), q_all=V((Z, H, RANK, TC), F32),
        Qg=V((2, C, H, RANK, TC), BF16), Qc=V((L, RANK, T), BF16),
        ims=V((2, H, RANK, W), F32), im_sib=V((H, RANK, W), F32), im_all=V((Z, H, RANK, W), BF16),
        im_fin=V((2, H, RANK, W), BF16),
        dt_part=V((L, 1, W), F32), dt_sib=V((L, 1, W), F32), dt_z=V((L, Z, 1, W), F32),
        dt_tot=V((L, 1, W), F32), dt_all=V((2, R, 1, W), F32), q=V(pair, BF16), q_recv=V((C,) + pair, BF16),
        q1_r=V(pair, BF16), q2_s=V(pair, BF16), q2_r=V(pair, BF16),
        own=V((L, TC, KI), F32), hold=V(slim, F32), rs1_s=V(wide, BF16), rs1_r=V(wide, BF16),
        rs2_s=V(slim, BF16), rs2_r=V(slim, BF16),
        send=dma((1,)), g_in=dma((L, Z - 1)), g_fw=dma((L,)), a_in=dma((L, 2)), rs1_in=dma((L,)), rs2_in=dma((1,)),
        sq_in=dma((1,)), dt_in=dma((3, L - 2)), dt_last=dma((2,)), root_in=dma((2,)), out_in=dma((2,)), col_in=dma((1,)),
        sib_in=dma((6,)), news=pltpu.SemaphoreType.REGULAR((2, max(Z - 2, 1))), q_in=dma((1,) if C == 4 else (L,)), q1_in=dma((L - 1,)), q2_in=dma((1,)),
    )


def kernel(R, C, *refs):
    acts_hbm, grads_hbm, frozen_hbm, ain_hbm, aout_hbm, mag_hbm, ig, ing, oug, mgrad = refs[:10]
    (acts, grads, frozen, ain, aout, mag, load, G, A, merged, ws, asc, sqm, sq_sib, sq_z, sq_tot, norms, scl, cor,
     mag3, mg3, prod_buf, qs, q_sib, q_all, Qg, Qc, ims, im_sib, im_all, im_fin, dt_part, dt_sib, dt_z, dt_tot,
     dt_all, q, q_recv, q1_r, q2_s, q2_r, own, hold, rs1_s, rs1_r, rs2_s, rs2_r, send, g_in, g_fw, a_in, rs1_in,
     rs2_in, sq_in, dt_in, dt_last, root_in, out_in, col_in, sib_in, news, q_in, q1_in, q2_in) = refs[10:]
    pairs = ((grads_hbm, grads), (acts_hbm, acts), (frozen_hbm, frozen),
             (ain_hbm, ain), (aout_hbm, aout), (mag_hbm, mag))
    loads = [pltpu.make_async_copy(a, b, load.at[i]) for i, (a, b) in enumerate(pairs)]
    for copy in loads:
        copy.start()
    L, TR, W = grads.shape
    TC, KI = acts.shape[1:]
    Z, H, KH = R // 2, L // 2, KI // 2
    ahead = min(3, L)
    last = L + Z - 3
    r, c = lax.axis_index("row"), lax.axis_index("col")
    z, core = r // 2, lax.rem(r, 2)
    sib = 2 * z + 1 - core
    square = C == 4
    xn, yn = c + 1 - 2 * lax.rem(c, 2), lax.rem(c + 2, 4)
    dg = 3 - c
    root = Z // 2 - 1 + core
    middle = jnp.logical_and(z > 0, z < Z - 1)
    halves = 2 if square else 1
    KS = KI // halves

    def row_to(d):
        return lax.rem(r + d, R)

    def row_from(d):
        return lax.rem(r + R - d, R)

    def col_to(d):
        return lax.rem(c + d, C)

    def col_from(d):
        return lax.rem(c + C - d, C)

    def z_to(d):
        return 2 * lax.rem(z + d, Z) + core

    def z_from(d):
        return lax.rem(z + Z - d, Z)

    def rows(at, size):
        return pl.ds(pl.multiple_of(at * size, size), size)

    def rcopy(src, dst, recv, **dev):
        return pltpu.make_async_remote_copy(
            src_ref=src, dst_ref=dst, send_sem=send.at[0], recv_sem=recv,
            device_id=dev, device_id_type=MESH,
        )

    def arrived(ref, recv):
        rcopy(ref, ref, recv, row=r).wait_recv()

    barrier = pltpu.get_barrier_semaphore()

    def greet(**dev):
        pl.semaphore_signal(barrier, inc=1, device_id=dev, device_id_type=MESH)

    greet(row=sib)
    for step in (1, -1):
        @pl.when(jnp.logical_and(z + step >= 0, z + step < Z))
        def _():
            greet(row=r + 2 * step)

    near = [xn, yn] if square else [col_to(d) for d in range(1, C)]
    for to in near:
        greet(col=to)
    pl.semaphore_wait(barrier, len(near) + jnp.where(middle, 3, 2))

    def tell(hops):
        for i, step in enumerate((1, -1)):
            of = z - step * (hops - 1)

            @pl.when((z + step >= 0) & (z + step < Z) & (of >= 0) & (of < Z))
            def _():
                pl.semaphore_signal(
                    news.at[i, hops - 2], inc=1, device_id={"row": r + 2 * step}, device_id_type=MESH
                )

    def hear(hops):
        for i, step in enumerate((1, -1)):
            of = z - step * hops

            @pl.when((of >= 0) & (of < Z))
            def _():
                pl.semaphore_wait(news.at[i, hops - 2], 1)

    def g_block(l, at, which):
        return G.at[l, rows(2 * at + which, TR)]

    def g_sem(l, at, to):
        return g_in.at[l, at - jnp.where(at > to, 1, 0)]

    def g_own(l, step):
        if step == 0:
            return rcopy(grads.at[l], g_block(l, z, core), g_fw.at[l], row=sib)
        return rcopy(grads.at[l], g_block(l, z, core), g_sem(l, z, z + step), row=r + 2 * step)

    def g_pass(l, at, step):
        block = g_block(l, at, core)
        if step == 0:
            return rcopy(block, block, g_fw.at[l], row=sib)
        return rcopy(block, block, g_sem(l, at, z + step), row=r + 2 * step)

    def g_own_each(l, act):
        @pl.when(z < Z - 1)
        def _():
            act(g_own(l, 1))

        @pl.when(z > 0)
        def _():
            act(g_own(l, -1))

        act(g_own(l, 0))

    def g_relay(l, d, act, arrive):
        for step in (1, -1):
            at = z - step * d

            @pl.when(jnp.logical_and(at >= 0, at < Z))
            def _():
                if arrive:
                    arrived(g_block(l, at, core), g_sem(l, at, z))

                @pl.when(jnp.logical_and(z + step >= 0, z + step < Z))
                def _():
                    act(g_pass(l, at, step))

                act(g_pass(l, at, 0))

    def a_copies(l):
        mine = A.at[l, rows(c, TC)]
        if square:
            return [rcopy(acts.at[l], mine, a_in.at[l, 0], col=xn), rcopy(acts.at[l], mine, a_in.at[l, 0], col=yn)]
        return [rcopy(acts.at[l], mine, a_in.at[l, 0], col=col_to(d)) for d in range(1, C)]

    def a_half(l, of, part):
        size = TC // 2
        return A.at[l, rows(2 * of + part, size)]

    def a_passes(l):
        first, second = a_half(l, xn, 0), a_half(l, yn, 1)
        return [rcopy(first, first, a_in.at[l, 1], col=yn), rcopy(second, second, a_in.at[l, 1], col=xn)]

    def a_relay(l):
        arrived(A.at[l, pl.ds(0, 2 * TC)], a_in.at[l, 0])
        for copy in a_passes(l):
            copy.start()

    def a_ready(l):
        if square:
            arrived(A.at[l, rows(dg, TC)], a_in.at[l, 1])
        else:
            arrived(A.at[l, pl.ds(0, (C - 1) * TC)], a_in.at[l, 0])

    def rs1_copies(l):
        if square:
            return [rcopy(rs1_s.at[i, l], rs1_r.at[i, l], rs1_in.at[l], col=to) for i, to in enumerate((xn, yn))]
        return [rcopy(rs1_s.at[d, l], rs1_r.at[d, l], rs1_in.at[l], col=col_to(d)) for d in range(1, C)]

    def rs2_copies(l):
        return [rcopy(rs2_s.at[i, l], rs2_r.at[i, l], rs2_in.at[0], col=to) for i, to in enumerate((yn, xn))]

    def rs_first(l, prod):
        if square:
            for i, near in enumerate((xn, yn)):
                rs1_s[i, l, 0] = prod[rows(near, TC), cols(i)].astype(BF16)
                rs1_s[i, l, 1] = prod[rows(dg, TC), cols(i)].astype(BF16)
                hold[i, l] = prod[rows((yn, xn)[i], TC), cols(i)]
        else:
            for d in range(1, C):
                rs1_s[d, l] = prod[rows(col_to(d), TC)].astype(BF16)
        own[l] = prod[rows(c, TC)]
        for copy in rs1_copies(l):
            copy.start()

    def rs_second(l):
        if square:
            arrived(rs1_r.at[:, l], rs1_in.at[l])
            for i in range(2):
                rs2_s[i, l] = (hold[i, l] + rs1_r[i, l, 1].astype(F32)).astype(BF16)
            for copy in rs2_copies(l):
                copy.start()

    def rs_finish(l):
        if square:
            for i in range(2):
                total = own[l, :, cols(i)] + rs1_r[i, l, 0].astype(F32) + rs2_r[i, l].astype(F32)
                ig[l, :, cols(i)] = total.astype(BF16)
        else:
            total = own[l]
            arrived(rs1_r.at[pl.ds(1, C - 1), l], rs1_in.at[l])
            for d in range(1, C):
                total = total + rs1_r[d, l].astype(F32)
            ig[l] = total.astype(BF16)

    def sq_copies():
        return [rcopy(sq_z.at[z], sq_z.at[z], sq_in.at[0], row=z_to(d)) for d in range(1, Z)]

    to_sib = [
        rcopy(sqm.at[pl.ds((1 - core) * H, H)], sq_sib, sib_in.at[0], row=sib),
        rcopy(sq_tot.at[core], sq_tot.at[core], sib_in.at[1], row=sib),
        rcopy(qs.at[1 - core], q_sib, sib_in.at[2], row=sib),
        rcopy(ims.at[1 - core], im_sib, sib_in.at[3], row=sib),
        rcopy(Qg.at[core], Qg.at[core], sib_in.at[4], row=sib),
        rcopy(im_fin.at[core], im_fin.at[core], sib_in.at[5], row=sib),
    ]

    def root_copies():
        return [rcopy(q_all.at[z], q_all.at[z], root_in.at[0], row=2 * root + core),
                rcopy(im_all.at[z], im_all.at[z], root_in.at[1], row=2 * root + core)]

    def out_ref(i):
        return Qg.at[core, c] if i == 0 else im_fin.at[core]

    def out_copies(i):
        ref = out_ref(i)
        return [rcopy(ref, ref, out_in.at[i], row=z_to(d)) for d in range(1, Z)]

    def gather_copies():
        mine = Qg.at[core, c]
        return [rcopy(mine, mine, col_in.at[0], col=col_to(d)) for d in range(1, C)]

    def start(copy):
        copy.start()

    def to_root():
        arrived(q_sib, sib_in.at[2])
        arrived(im_sib, sib_in.at[3])
        q_all[z] = qs[core] + q_sib[...]
        im_all[z] = (ims[core] + im_sib[...]).astype(BF16)

        @pl.when(z != root)
        def _():
            for copy in root_copies():
                copy.start()

    def at_root():
        arrived(q_all.at[pl.ds(0, Z - 1)], root_in.at[0])
        arrived(im_all.at[pl.ds(0, Z - 1)], root_in.at[1])
        q_sum, im_sum = q_all[0], im_all[0].astype(F32)
        for s in range(1, Z):
            q_sum = q_sum + q_all[s]
            im_sum = im_sum + im_all[s].astype(F32)
        Qg[core, c] = q_sum.astype(BF16)
        im_fin[core] = im_sum.astype(BF16)
        for copy in out_copies(0) + gather_copies():
            copy.start()

    def q_arrived():
        arrived(out_ref(0), out_in.at[0])
        for copy in gather_copies():
            copy.start()

    def dt_all_copies(l):
        mine = dt_all.at[l - (L - 2), r]
        return [rcopy(mine, mine, dt_last.at[l - (L - 2)], row=row_to(d)) for d in range(1, R)]

    def dt_sib_copy(l):
        return rcopy(dt_part.at[l], dt_sib.at[l], dt_in.at[0, l], row=sib)

    def dt_z_copies(l):
        return [rcopy(dt_z.at[l, z], dt_z.at[l, z], dt_in.at[1, l], row=z_to(d)) for d in range(1, Z)]

    def dt_tot_copy(l):
        return rcopy(dt_tot.at[l], dt_tot.at[l], dt_in.at[2, l], row=sib)

    def in_charge(l):
        return lax.rem(l, 2) == core

    def dots_out(l, part):
        @pl.when(l < L - 2)
        def _():
            dt_part[l] = part

            @pl.when(jnp.logical_not(in_charge(l)))
            def _():
                dt_sib_copy(l).start()

        @pl.when(l >= L - 2)
        def _():
            dt_all[l - (L - 2), r] = part
            for copy in dt_all_copies(l):
                copy.start()

    def dots_chip(l):
        @pl.when(in_charge(l))
        def _():
            arrived(dt_sib.at[l], dt_in.at[0, l])
            dt_z[l, z] = dt_part[l] + dt_sib[l]
            for copy in dt_z_copies(l):
                copy.start()

    def dots_sum(l):
        @pl.when(in_charge(l))
        def _():
            arrived(dt_z.at[l, pl.ds(0, Z - 1)], dt_in.at[1, l])
            total = dt_z[l, 0]
            for s in range(1, Z):
                total = total + dt_z[l, s]
            dt_tot[l] = total
            dt_tot_copy(l).start()

    def q_copies(l):
        return [rcopy(q.at[l], q_recv.at[d, l], q_in.at[0 if square else l], col=col_to(d)) for d in range(1, C)]

    def q1_copies(l):
        return [rcopy(q.at[l, i], q1_r.at[l, i], q1_in.at[l], col=to) for i, to in enumerate((xn, yn))]

    def q2_copies(l):
        return [rcopy(q2_s.at[l, i], q2_r.at[l, i], q2_in.at[0], col=to) for i, to in enumerate((yn, xn))]

    def cols(i):
        return slice(i * KS, (i + 1) * KS)

    loads[0].wait()
    loads[1].wait()

    @pl.loop(0, ahead)
    def _(l):
        g_own_each(l, start)

    @pl.loop(0, L)
    def _(l):
        for copy in a_copies(l):
            copy.start()

    if Z > 2:
        tell(2)
    for copy in loads[2:]:
        copy.wait()

    @pl.loop(0, L)
    def _(l):
        m = frozen[l].astype(F32) + mm(ain[l], aout[l], ((0,), (0,)))
        merged[l] = m
        sqm[l] = jnp.sum(m * m, axis=0, keepdims=True)

    to_sib[0].start()
    for hops in range(2, Z):
        hear(hops)
        if hops < Z - 1:
            tell(hops + 1)

    @pl.loop(0, L)
    def _(l):
        G[l, rows(r, TR)] = grads[l]
        A[l, rows(c, TC)] = acts[l]
        half, at = l // H, lax.rem(l, H)
        ims[half, at] = mm(ain[l], merged[l].astype(BF16), ((1,), (0,)))
        qs[half, at] = mm(ain[l], acts[l], ((1,), (1,)))

    to_sib[2].start()
    to_sib[3].start()
    for l in range(L):
        mag3[l] = mag[l:l + 1]

    def squares_out():
        arrived(sq_sib, sib_in.at[0])
        sq_z[z] = sqm[pl.ds(core * H, H)] + sq_sib[...]
        for copy in sq_copies():
            copy.start()

    def squares_sum():
        arrived(sq_z.at[pl.ds(0, Z - 1)], sq_in.at[0])
        total = sq_z[0]
        for s in range(1, Z):
            total = total + sq_z[s]
        sq_tot[core] = total
        to_sib[1].start()

    def scales():
        arrived(sq_tot.at[1 - core], sib_in.at[1])

        @pl.loop(0, L)
        def _(l):
            n = jnp.sqrt(sq_tot[l // H, lax.rem(l, H)] + 0.25)
            s = mag3[l] / n
            norms[l] = n
            scl[l] = s
            ws[l] = (merged[l] * s).astype(BF16)
            asc[l] = (aout[l].astype(F32) * s).astype(BF16)

    def compute(l):
        @pl.when(jnp.logical_and(l >= 1, l < L - 1))
        def _():
            dots_chip(l - 1)

        arrived(G.at[l, pl.ds(0, Z * TR)], g_fw.at[l])
        a_ready(l)
        g = G[l]
        outer = mm(A[l], g, ((0,), (0,)))
        dots_out(l, jnp.sum(merged[l] * outer, axis=0, keepdims=True))
        low = outer.astype(BF16)
        prod_buf[...] = mm(g, ws[l], ((1,), (1,)))
        rs_first(l, prod_buf)
        ing[l] = mm(asc[l], low, ((1,), (1,)))

        @pl.when(l > 1)
        def _():
            rs_second(l - 2)

    def correct(l, direct):
        if isinstance(l, int) and l >= L - 2:
            every = dt_all.at[l - (L - 2)]
            arrived(every.at[pl.ds(0, R - 1)], dt_last.at[l - (L - 2)])
            dots = every[0]
            for s in range(1, R):
                dots = dots + every[s]
        else:
            @pl.when(jnp.logical_not(in_charge(l)))
            def _():
                arrived(dt_tot.at[l], dt_in.at[2, l])

            dots = dt_tot[l]
        n = norms[l]
        mg3[l] = dots / n
        factor = -mag3[l] * dots / (n * n * n)
        cor[l] = factor
        adjusted = (merged[l] * factor).astype(BF16)
        part = ing[l] + mm(aout[l], adjusted, ((1,), (1,)))
        ing[l] = part
        for i in range(halves):
            q[l, i] = part[:, cols(i)].astype(BF16)
        for copy in q_copies(l) if direct else q1_copies(l):
            copy.start()

    def q_second(l):
        arrived(q1_r.at[l], q1_in.at[l])
        for i in range(2):
            total = ing[l, :, cols(i)] + q1_r[l, i].astype(F32)
            ing[l, :, cols(i)] = total
            q2_s[l, i] = total.astype(BF16)
        for copy in q2_copies(l):
            copy.start()

    def relays(at):
        @pl.when(at + ahead < L)
        def _():
            g_own_each(at + ahead, start)

        for d in range(1, Z):
            l = at - (d - 1)

            @pl.when(jnp.logical_and(l >= 0, l < L))
            def _():
                g_relay(l, d, start, True)

    squares_out()
    lead = 1

    @pl.when(middle)
    def _():
        for at in range(lead):
            relays(at)

    @pl.loop(0, last + 1)
    def _(at):
        relays(at + jnp.where(middle, lead, at // last))

        @pl.when(jnp.logical_and(jnp.logical_not(middle), at == last - 1))
        def _():
            relays(last)

        if square:
            for l in (2 * at - 1, 2 * at):
                @pl.when(jnp.logical_and(l >= 0, l < L))
                def _():
                    a_relay(l)

        @pl.when(at == Z - 2)
        def _():
            to_root()

        @pl.when(jnp.logical_and(at == last - 2, z == root))
        def _():
            at_root()

        @pl.when(jnp.logical_and(at == last, z != root))
        def _():
            q_arrived()

        @pl.when(at == Z - 2)
        def _():
            squares_sum()
            scales()

        @pl.when(at >= Z - 2)
        def _():
            compute(at - (Z - 2))

        for lag, act in ((2, dots_sum), (3, lambda l: correct(l, not square))):
            @pl.when(jnp.logical_and(jnp.logical_not(middle), at - (Z - 2) - lag >= 0))
            def _():
                act(at - (Z - 2) - lag)

    @pl.when(z == root)
    def _():
        for copy in out_copies(1):
            copy.start()
        to_sib[5].start()

    @pl.loop(jnp.where(middle, 0, L - 2), L - 2)
    def _(l):
        dots_sum(l)

    @pl.loop(jnp.where(middle, 0, max(L - 3, 0)), L - 2)
    def _(l):
        correct(l, not square)

    correct(L - 2, not square)

    rs_second(L - 2)

    arrived(Qg.at[core, pl.ds(0, C - 1)], col_in.at[0])
    to_sib[4].start()

    correct(L - 1, True)

    rs_second(L - 1)

    if square:
        @pl.loop(0, L - 1)
        def _(l):
            q_second(l)

    @pl.when(z != root)
    def _():
        arrived(out_ref(1), out_in.at[1])
        to_sib[5].start()

    for l in range(L):
        mgrad[l:l + 1] = mg3[l]

    arrived(Qg.at[1 - core], sib_in.at[4])

    arrived(im_fin.at[1 - core], sib_in.at[5])

    @pl.loop(0, L)
    def _(l):
        half, at = l // H, lax.rem(l, H)
        for s in range(C):
            Qc[l, :, s * TC:(s + 1) * TC] = Qg[half, s, at]
        low = mm(Qc[l], G[l], ((1,), (0,))) * scl[l]
        oug[l] = low + im_fin[half, at].astype(F32) * cor[l]

    def done(copy):
        copy.wait_send()

    @pl.loop(0, L)
    def _(l):
        g_own_each(l, done)
        for d in range(1, Z):
            g_relay(l, d, done, False)
        for copy in a_copies(l) + rs1_copies(l):
            copy.wait_send()
        if square:
            for copy in a_passes(l):
                copy.wait_send()

    @pl.loop(0, L - 2)
    def _(l):
        @pl.when(in_charge(l))
        def _():
            for copy in dt_z_copies(l) + [dt_tot_copy(l)]:
                copy.wait_send()

        @pl.when(jnp.logical_not(in_charge(l)))
        def _():
            dt_sib_copy(l).wait_send()

    for copy in sq_copies() + to_sib + gather_copies() + dt_all_copies(L - 2) + dt_all_copies(L - 1):
        copy.wait_send()

    @pl.when(z == root)
    def _():
        for copy in out_copies(0) + out_copies(1):
            copy.wait_send()

    @pl.when(z != root)
    def _():
        for copy in root_copies():
            copy.wait_send()

    if square:
        arrived(rs2_r, rs2_in.at[0])

    @pl.loop(0, L)
    def _(l):
        rs_finish(l)

    arrived(q_recv.at[pl.ds(1, C - 1), L - 1], q_in.at[0 if square else L - 1])
    for i in range(halves):
        total = ing[L - 1, :, cols(i)]
        for d in range(1, C):
            total = total + q_recv[d, L - 1, i].astype(F32)
        ing[L - 1, :, cols(i)] = total

    if square:
        arrived(q2_r.at[pl.ds(0, L - 1)], q2_in.at[0])

    @pl.loop(0, L - 1)
    def _(l):
        if not square:
            arrived(q_recv.at[pl.ds(1, C - 1), l], q_in.at[0 if square else l])
        for i in range(halves):
            total = ing[l, :, cols(i)]
            if square:
                total = total + q2_r[l, i].astype(F32)
            else:
                for d in range(1, C):
                    total = total + q_recv[d, l, i].astype(F32)
            ing[l, :, cols(i)] = total

    @pl.loop(0, L)
    def _(l):
        if square:
            for copy in rs2_copies(l):
                copy.wait_send()

    @pl.loop(0, L - 1)
    def _(l):
        for copy in q1_copies(l) + q2_copies(l) if square else q_copies(l):
            copy.wait_send()

    for copy in q_copies(L - 1):
        copy.wait_send()


def finish(ig, ing, oug, mgrad, ig_out, ing_out, oug_out, mgrad_out, sem):
    pairs = ((ig, ig_out), (ing, ing_out), (oug, oug_out), (mgrad, mgrad_out))
    copies = [pltpu.make_async_copy(a, b, sem.at[i]) for i, (a, b) in enumerate(pairs)]
    for copy in copies:
        copy.start()
    for copy in copies:
        copy.wait()


def body(R, C, acts, grads, frozen, ain, aout, mag):
    L, TR, W = grads.shape
    TC, KI = acts.shape[1:]
    RANK = ain.shape[1]
    V = pltpu.VMEM
    vm = pl.BlockSpec(memory_space=pltpu.VMEM)
    hbm = pl.BlockSpec(memory_space=pltpu.HBM)
    buffers = scratch(R, C, L, TR, W, TC, KI, RANK)
    ig, ing, oug, mgrad = pl.pallas_call(
        functools.partial(kernel, R, C),
        out_shape=(V((L, TC, KI), BF16), V((L, RANK, KI), F32), V((L, RANK, W), F32), V((L, W), F32)),
        in_specs=[hbm] * 6,
        out_specs=(vm,) * 4,
        scratch_shapes=[buffers[name] for name in NAMES],
        compiler_params=pltpu.CompilerParams(
            collective_id=0, has_side_effects=True, vmem_limit_bytes=60 * 1024 * 1024
        ),
    )(acts, grads, frozen, ain, aout, mag)
    return pl.pallas_call(
        finish,
        out_shape=tuple(jax.ShapeDtypeStruct(x.shape, x.dtype) for x in (ig, ing, oug, mgrad)),
        in_specs=[vm] * 4,
        out_specs=(hbm,) * 4,
        scratch_shapes=[pltpu.SemaphoreType.DMA((4,))],
        compiler_params=pltpu.CompilerParams(vmem_limit_bytes=1024 * 1024),
    )(ig, ing, oug, mgrad)


def solution(mesh):
    return jax.shard_map(
        functools.partial(body, mesh.shape["row"], mesh.shape["col"]),
        mesh=mesh,
        in_specs=(
            P(None, "col", "row"),
            P(None, "row", "col"),
            P(None, "row", "col"),
            P(None, None, "row"),
            P(None, None, "col"),
            P(None, "col"),
        ),
        out_specs=(
            P(None, "col", "row"),
            P(None, None, "row"),
            P(None, None, "col"),
            P(None, "col"),
        ),
        check_vma=False,
    )
```

```python
import functools

import jax
import jax.numpy as jnp
from jax import lax
from jax.experimental import pallas as pl
from jax.experimental.pallas import tpu as pltpu
from jax.sharding import PartitionSpec as P

MESH = pl.DeviceIdType.MESH
F32 = jnp.float32
BF16 = jnp.bfloat16


def mm(a, b, dims):
    return lax.dot_general(a, b, (dims, ((), ())), preferred_element_type=F32)


NAMES = (
    "acts", "grads", "frozen", "ain", "aout", "mag", "load", "G", "A", "merged", "ws", "asc", "sqm", "sq_sib", "sq_z",
    "sq_tot", "norms", "scl", "cor", "mag3", "mg3", "prod_buf", "qs", "q_sib", "q_all", "Qg", "Qc", "ims", "im_sib",
    "im_all", "im_fin", "dt_own", "dt_tot", "dt_all", "q", "q_recv", "q1_r", "q2_s", "q2_r", "own",
    "hold", "rs1_s", "rs1_r", "rs2_s", "rs2_r", "send", "g_in", "g_fw", "a_in", "rs1_in", "rs2_in", "sq_in", "dt_in",
    "dt_last", "root_in", "out_in", "col_in", "sib_in", "news", "q_in", "q1_in", "q2_in",
)


def scratch(R, C, L, TR, W, TC, KI, RANK):
    Z, T, H, KH = R // 2, TR * R, L // 2, KI // 2
    V, dma = pltpu.VMEM, pltpu.SemaphoreType.DMA
    wide = (2, L, 2, TC, KH) if C == 4 else (C, L, TC, KI)
    slim = (2, L, TC, KH) if C == 4 else (1, 1, 8, 128)
    pair = (L, 2, RANK, KH) if C == 4 else (L, 1, RANK, KI)
    return dict(
        acts=V((L, TC, KI), BF16), grads=V((L, TR, W), BF16), frozen=V((L, KI, W), BF16),
        ain=V((L, RANK, KI), BF16), aout=V((L, RANK, W), BF16), mag=V((L, W), F32), load=dma((6,)),
        G=V((L, T, W), BF16), A=V((L, T, KI), BF16), merged=V((L, KI, W), F32), ws=V((L, KI, W), BF16),
        asc=V((L, RANK, W), BF16),
        sqm=V((L, 1, W), F32), sq_sib=V((H, 1, W), F32), sq_z=V((Z, H, 1, W), F32), sq_tot=V((2, H, 1, W), F32),
        norms=V((L, 1, W), F32), scl=V((L, 1, W), F32), cor=V((L, 1, W), F32), mag3=V((L, 1, W), F32),
        mg3=V((L, 1, W), F32),
        prod_buf=V((T, KI), F32), qs=V((2, H, RANK, TC), F32), q_sib=V((H, RANK, TC), F32), q_all=V((Z, H, RANK, TC), F32),
        Qg=V((2, C, H, RANK, TC), BF16), Qc=V((L, RANK, T), BF16),
        ims=V((2, H, RANK, W), F32), im_sib=V((H, RANK, W), F32), im_all=V((Z, H, RANK, W), BF16),
        im_fin=V((2, H, RANK, W), BF16),
        dt_own=V((L, R, 1, W), F32),
        dt_tot=V((L, 1, W), F32), dt_all=V((2, R, 1, W), F32), q=V(pair, BF16), q_recv=V((C,) + pair, BF16),
        q1_r=V(pair, BF16), q2_s=V(pair, BF16), q2_r=V(pair, BF16),
        own=V((L, TC, KI), F32), hold=V(slim, F32), rs1_s=V(wide, BF16), rs1_r=V(wide, BF16),
        rs2_s=V(slim, BF16), rs2_r=V(slim, BF16),
        send=dma((1,)), g_in=dma((L, Z - 1)), g_fw=dma((L,)), a_in=dma((L, 2)), rs1_in=dma((L,)), rs2_in=dma((1,)),
        sq_in=dma((1,)), dt_in=dma((2, L - 2)), dt_last=dma((2,)), root_in=dma((2,)), out_in=dma((2,)), col_in=dma((1,)),
        sib_in=dma((6,)), news=pltpu.SemaphoreType.REGULAR((2, max(Z - 2, 1))), q_in=dma((L,)), q1_in=dma((L - 2,)), q2_in=dma((1,)),
    )


def kernel(R, C, *refs):
    acts_hbm, grads_hbm, frozen_hbm, ain_hbm, aout_hbm, mag_hbm, ig, ing, oug, mgrad = refs[:10]
    (acts, grads, frozen, ain, aout, mag, load, G, A, merged, ws, asc, sqm, sq_sib, sq_z, sq_tot, norms, scl, cor,
     mag3, mg3, prod_buf, qs, q_sib, q_all, Qg, Qc, ims, im_sib, im_all, im_fin, dt_own, dt_tot,
     dt_all, q, q_recv, q1_r, q2_s, q2_r, own, hold, rs1_s, rs1_r, rs2_s, rs2_r, send, g_in, g_fw, a_in, rs1_in,
     rs2_in, sq_in, dt_in, dt_last, root_in, out_in, col_in, sib_in, news, q_in, q1_in, q2_in) = refs[10:]
    pairs = ((grads_hbm, grads), (acts_hbm, acts), (frozen_hbm, frozen),
             (ain_hbm, ain), (aout_hbm, aout), (mag_hbm, mag))
    loads = [pltpu.make_async_copy(a, b, load.at[i]) for i, (a, b) in enumerate(pairs)]
    for copy in loads:
        copy.start()
    L, TR, W = grads.shape
    TC, KI = acts.shape[1:]
    Z, H, KH = R // 2, L // 2, KI // 2
    ahead = min(3, L)
    last = L + Z - 3
    r, c = lax.axis_index("row"), lax.axis_index("col")
    z, core = r // 2, lax.rem(r, 2)
    sib = 2 * z + 1 - core
    square = C == 4
    xn, yn = c + 1 - 2 * lax.rem(c, 2), lax.rem(c + 2, 4)
    dg = 3 - c
    root = Z // 2 - 1 + core
    middle = jnp.logical_and(z > 0, z < Z - 1)
    ends = jnp.logical_not(middle)
    halves = 2 if square else 1
    KS = KI // halves

    def row_to(d):
        return lax.rem(r + d, R)

    def row_from(d):
        return lax.rem(r + R - d, R)

    def col_to(d):
        return lax.rem(c + d, C)

    def col_from(d):
        return lax.rem(c + C - d, C)

    def z_to(d):
        return 2 * lax.rem(z + d, Z) + core

    def z_from(d):
        return lax.rem(z + Z - d, Z)

    def rows(at, size):
        return pl.ds(pl.multiple_of(at * size, size), size)

    def rcopy(src, dst, recv, **dev):
        return pltpu.make_async_remote_copy(
            src_ref=src, dst_ref=dst, send_sem=send.at[0], recv_sem=recv,
            device_id=dev, device_id_type=MESH,
        )

    def arrived(ref, recv):
        rcopy(ref, ref, recv, row=r).wait_recv()

    barrier = pltpu.get_barrier_semaphore()

    def greet(**dev):
        pl.semaphore_signal(barrier, inc=1, device_id=dev, device_id_type=MESH)

    greet(row=sib)
    for step in (1, -1):
        @pl.when(jnp.logical_and(z + step >= 0, z + step < Z))
        def _():
            greet(row=r + 2 * step)

    near = [xn, yn] if square else [col_to(d) for d in range(1, C)]
    for to in near:
        greet(col=to)
    pl.semaphore_wait(barrier, len(near) + jnp.where(middle, 3, 2))

    def tell(hops):
        for i, step in enumerate((1, -1)):
            of = z - step * (hops - 1)

            @pl.when((z + step >= 0) & (z + step < Z) & (of >= 0) & (of < Z))
            def _():
                pl.semaphore_signal(
                    news.at[i, hops - 2], inc=1, device_id={"row": r + 2 * step}, device_id_type=MESH
                )

    def hear(hops):
        for i, step in enumerate((1, -1)):
            of = z - step * hops

            @pl.when((of >= 0) & (of < Z))
            def _():
                pl.semaphore_wait(news.at[i, hops - 2], 1)

    def g_block(l, at, which):
        return G.at[l, rows(2 * at + which, TR)]

    def g_sem(l, at, to):
        return g_in.at[l, at - jnp.where(at > to, 1, 0)]

    def g_own(l, step):
        if step == 0:
            return rcopy(grads.at[l], g_block(l, z, core), g_fw.at[l], row=sib)
        return rcopy(grads.at[l], g_block(l, z, core), g_sem(l, z, z + step), row=r + 2 * step)

    def g_pass(l, at, step):
        block = g_block(l, at, core)
        if isinstance(step, int) and step == 0:
            return rcopy(block, block, g_fw.at[l], row=sib)
        return rcopy(block, block, g_sem(l, at, z + step), row=r + 2 * step)

    def g_own_each(l, act):
        @pl.when(z < Z - 1)
        def _():
            act(g_own(l, 1))

        @pl.when(z > 0)
        def _():
            act(g_own(l, -1))

        act(g_own(l, 0))

    def g_relay(l, d, step, act, arrive):
        at = z - step * d

        @pl.when(jnp.logical_and(at >= 0, at < Z))
        def _():
            if arrive:
                arrived(g_block(l, at, core), g_sem(l, at, z))

            @pl.when(jnp.logical_and(z + step >= 0, z + step < Z))
            def _():
                act(g_pass(l, at, step))

            act(g_pass(l, at, 0))

    def a_copies(l):
        mine = A.at[l, rows(c, TC)]
        if square:
            return [rcopy(acts.at[l], mine, a_in.at[l, 0], col=xn), rcopy(acts.at[l], mine, a_in.at[l, 0], col=yn)]
        return [rcopy(acts.at[l], mine, a_in.at[l, 0], col=col_to(d)) for d in range(1, C)]

    def a_half(l, of, part):
        size = TC // 2
        return A.at[l, rows(2 * of + part, size)]

    def a_passes(l):
        first, second = a_half(l, xn, 0), a_half(l, yn, 1)
        return [rcopy(first, first, a_in.at[l, 1], col=yn), rcopy(second, second, a_in.at[l, 1], col=xn)]

    def a_relay(l):
        arrived(A.at[l, pl.ds(0, 2 * TC)], a_in.at[l, 0])
        for copy in a_passes(l):
            copy.start()

    def a_ready(l):
        if square:
            arrived(A.at[l, rows(dg, TC)], a_in.at[l, 1])
        else:
            arrived(A.at[l, pl.ds(0, (C - 1) * TC)], a_in.at[l, 0])

    def rs1_copies(l):
        if square:
            return [rcopy(rs1_s.at[i, l], rs1_r.at[i, l], rs1_in.at[l], col=to) for i, to in enumerate((xn, yn))]
        return [rcopy(rs1_s.at[d, l], rs1_r.at[d, l], rs1_in.at[l], col=col_to(d)) for d in range(1, C)]

    def rs2_copies(l):
        return [rcopy(rs2_s.at[i, l], rs2_r.at[i, l], rs2_in.at[0], col=to) for i, to in enumerate((yn, xn))]

    def rs_first(l, prod):
        if square:
            for i, near in enumerate((xn, yn)):
                rs1_s[i, l, 0] = prod[rows(near, TC), cols(i)].astype(BF16)
                rs1_s[i, l, 1] = prod[rows(dg, TC), cols(i)].astype(BF16)
                hold[i, l] = prod[rows((yn, xn)[i], TC), cols(i)]
        else:
            for d in range(1, C):
                rs1_s[d, l] = prod[rows(col_to(d), TC)].astype(BF16)
        own[l] = prod[rows(c, TC)]
        for copy in rs1_copies(l):
            copy.start()

    def rs_second(l):
        if square:
            arrived(rs1_r.at[:, l], rs1_in.at[l])
            for i in range(2):
                rs2_s[i, l] = (hold[i, l] + rs1_r[i, l, 1].astype(F32)).astype(BF16)
            for copy in rs2_copies(l):
                copy.start()

    def rs_finish(l):
        if square:
            for i in range(2):
                total = own[l, :, cols(i)] + rs1_r[i, l, 0].astype(F32) + rs2_r[i, l].astype(F32)
                ig[l, :, cols(i)] = total.astype(BF16)
        else:
            total = own[l]
            arrived(rs1_r.at[pl.ds(1, C - 1), l], rs1_in.at[l])
            for d in range(1, C):
                total = total + rs1_r[d, l].astype(F32)
            ig[l] = total.astype(BF16)

    def sq_copies():
        return [rcopy(sq_z.at[z], sq_z.at[z], sq_in.at[0], row=z_to(d)) for d in range(1, Z)]

    to_sib = [
        rcopy(sqm.at[pl.ds((1 - core) * H, H)], sq_sib, sib_in.at[0], row=sib),
        rcopy(sq_tot.at[core], sq_tot.at[core], sib_in.at[1], row=sib),
        rcopy(qs.at[1 - core], q_sib, sib_in.at[2], row=sib),
        rcopy(ims.at[1 - core], im_sib, sib_in.at[3], row=sib),
        rcopy(Qg.at[core], Qg.at[core], sib_in.at[4], row=sib),
        rcopy(im_fin.at[core], im_fin.at[core], sib_in.at[5], row=sib),
    ]

    def root_copies():
        return [rcopy(q_all.at[z], q_all.at[z], root_in.at[0], row=2 * root + core),
                rcopy(im_all.at[z], im_all.at[z], root_in.at[1], row=2 * root + core)]

    def out_ref(i):
        return Qg.at[core, c] if i == 0 else im_fin.at[core]

    def out_copies(i):
        ref = out_ref(i)
        return [rcopy(ref, ref, out_in.at[i], row=z_to(d)) for d in range(1, Z)]

    def gather_copies():
        mine = Qg.at[core, c]
        return [rcopy(mine, mine, col_in.at[0], col=col_to(d)) for d in range(1, C)]

    def start(copy):
        copy.start()

    def to_root():
        arrived(q_sib, sib_in.at[2])
        arrived(im_sib, sib_in.at[3])
        q_all[z] = qs[core] + q_sib[...]
        im_all[z] = (ims[core] + im_sib[...]).astype(BF16)

        @pl.when(z != root)
        def _():
            for copy in root_copies():
                copy.start()

    def at_root():
        arrived(q_all.at[pl.ds(0, Z - 1)], root_in.at[0])
        arrived(im_all.at[pl.ds(0, Z - 1)], root_in.at[1])
        q_sum, im_sum = q_all[0], im_all[0].astype(F32)
        for s in range(1, Z):
            q_sum = q_sum + q_all[s]
            im_sum = im_sum + im_all[s].astype(F32)
        Qg[core, c] = q_sum.astype(BF16)
        im_fin[core] = im_sum.astype(BF16)
        for copy in out_copies(0) + gather_copies():
            copy.start()

    def q_arrived():
        arrived(out_ref(0), out_in.at[0])
        for copy in gather_copies():
            copy.start()

    def dt_all_copies(l):
        mine = dt_all.at[l - (L - 2), r]
        return [rcopy(mine, mine, dt_last.at[l - (L - 2)], row=row_to(d)) for d in range(1, R)]

    def dt_own_copy(l, at):
        mine = dt_own.at[l, r]
        return rcopy(mine, mine, dt_in.at[0, l], row=2 * at + lax.rem(l, 2))

    def dt_own_each(l, act):
        for d in range(1, Z):
            act(dt_own_copy(l, lax.rem(z + d, Z)))

        @pl.when(jnp.logical_not(in_charge(l)))
        def _():
            act(dt_own_copy(l, z))

    def dt_tot_copy(l):
        return rcopy(dt_tot.at[l], dt_tot.at[l], dt_in.at[1, l], row=sib)

    def in_charge(l):
        return lax.rem(l, 2) == core

    def dots_out(l, part):
        @pl.when(l < L - 2)
        def _():
            dt_own[l, r] = part
            dt_own_each(l, start)

        @pl.when(l >= L - 2)
        def _():
            dt_all[l - (L - 2), r] = part
            for copy in dt_all_copies(l):
                copy.start()

    def dots_sum(l):
        @pl.when(in_charge(l))
        def _():
            arrived(dt_own.at[l, pl.ds(0, R - 1)], dt_in.at[0, l])
            total = dt_own[l, 0]
            for s in range(1, R):
                total = total + dt_own[l, s]
            dt_tot[l] = total
            dt_tot_copy(l).start()

    def q_copies(l):
        return [rcopy(q.at[l], q_recv.at[d, l], q_in.at[l], col=col_to(d)) for d in range(1, C)]

    def q1_copies(l):
        return [rcopy(q.at[l, i], q1_r.at[l, i], q1_in.at[l], col=to) for i, to in enumerate((xn, yn))]

    def q2_copies(l):
        return [rcopy(q2_s.at[l, i], q2_r.at[l, i], q2_in.at[0], col=to) for i, to in enumerate((yn, xn))]

    def cols(i):
        return slice(i * KS, (i + 1) * KS)

    loads[0].wait()
    loads[1].wait()

    @pl.loop(0, ahead)
    def _(l):
        g_own_each(l, start)

    @pl.loop(0, L)
    def _(l):
        for copy in a_copies(l):
            copy.start()

    if Z > 2:
        tell(2)
    for copy in loads[2:]:
        copy.wait()

    @pl.loop(0, L)
    def _(l):
        m = frozen[l].astype(F32) + mm(ain[l], aout[l], ((0,), (0,)))
        merged[l] = m
        sqm[l] = jnp.sum(m * m, axis=0, keepdims=True)

    to_sib[0].start()
    for hops in range(2, Z):
        hear(hops)
        if hops < Z - 1:
            tell(hops + 1)

    @pl.loop(0, L)
    def _(l):
        G[l, rows(r, TR)] = grads[l]
        A[l, rows(c, TC)] = acts[l]
        half, at = l // H, lax.rem(l, H)
        ims[half, at] = mm(ain[l], merged[l].astype(BF16), ((1,), (0,)))
        qs[half, at] = mm(ain[l], acts[l], ((1,), (1,)))

    to_sib[2].start()
    to_sib[3].start()
    for l in range(L):
        mag3[l] = mag[l:l + 1]

    def squares_out():
        arrived(sq_sib, sib_in.at[0])
        sq_z[z] = sqm[pl.ds(core * H, H)] + sq_sib[...]
        for copy in sq_copies():
            copy.start()

    def squares_sum():
        arrived(sq_z.at[pl.ds(0, Z - 1)], sq_in.at[0])
        total = sq_z[0]
        for s in range(1, Z):
            total = total + sq_z[s]
        sq_tot[core] = total
        to_sib[1].start()

    def scales():
        arrived(sq_tot.at[1 - core], sib_in.at[1])

        @pl.loop(0, L)
        def _(l):
            n = jnp.sqrt(sq_tot[l // H, lax.rem(l, H)] + 0.25)
            s = mag3[l] / n
            norms[l] = n
            scl[l] = s
            ws[l] = (merged[l] * s).astype(BF16)
            asc[l] = (aout[l].astype(F32) * s).astype(BF16)

    out = jnp.where(z < Z // 2, -1, 1)

    def relay(at, d, step):
        l = at - (d - 1)

        @pl.when(jnp.logical_and(l >= 0, l < L))
        def _():
            g_relay(l, d, step, start, True)

    def compute(l):
        back = jnp.where(middle, 3, 2)

        @pl.when(l >= back)
        def _():
            rs_second(l - back)

        arrived(G.at[l, pl.ds(0, Z * TR)], g_fw.at[l])
        a_ready(l)
        g = G[l]
        outer = mm(A[l], g, ((0,), (0,)))
        dots_out(l, jnp.sum(merged[l] * outer, axis=0, keepdims=True))

        @pl.when(jnp.logical_and(ends, l == L - 2))
        def _():
            relay(last - 1, Z - 2, out)

        low = outer.astype(BF16)
        prod_buf[...] = mm(g, ws[l], ((1,), (1,)))
        rs_first(l, prod_buf)

        @pl.when(jnp.logical_and(ends, l == L - 2))
        def _():
            relay(last, Z - 1, out)

        ing[l] = mm(asc[l], low, ((1,), (1,)))

    def correct(l, direct):
        if isinstance(l, int) and l >= L - 2:
            every = dt_all.at[l - (L - 2)]
            arrived(every.at[pl.ds(0, R - 1)], dt_last.at[l - (L - 2)])
            dots = every[0]
            for s in range(1, R):
                dots = dots + every[s]
        else:
            @pl.when(jnp.logical_not(in_charge(l)))
            def _():
                arrived(dt_tot.at[l], dt_in.at[1, l])

            dots = dt_tot[l]
        n = norms[l]
        mg3[l] = dots / n
        factor = -mag3[l] * dots / (n * n * n)
        cor[l] = factor
        adjusted = (merged[l] * factor).astype(BF16)
        part = ing[l] + mm(aout[l], adjusted, ((1,), (1,)))
        ing[l] = part
        for i in range(halves):
            q[l, i] = part[:, cols(i)].astype(BF16)
        for copy in q_copies(l) if direct else q1_copies(l):
            copy.start()

    def q_second(l):
        arrived(q1_r.at[l], q1_in.at[l])
        for i in range(2):
            total = ing[l, :, cols(i)] + q1_r[l, i].astype(F32)
            ing[l, :, cols(i)] = total
            q2_s[l, i] = total.astype(BF16)
        for copy in q2_copies(l):
            copy.start()

    def own_at(at):
        @pl.when(at + ahead < L)
        def _():
            g_own_each(at + ahead, start)

    def relays(at):
        own_at(at)

        @pl.when(at < Z - 2)
        def _():
            for d in range(1, Z):
                relay(at, d, -out)
                relay(at, d, out)

        @pl.when(at >= Z - 2)
        def _():
            for d in range(1, Z):
                relay(at, d, -out)
            for d in range(Z - 1, 0, -1):
                relay(at, d, out)

    squares_out()
    lead = 1

    @pl.when(middle)
    def _():
        for at in range(lead):
            relays(at)

    @pl.loop(0, last + 1)
    def _(at):
        late = jnp.logical_and(jnp.logical_not(middle), at >= Z - 2)

        @pl.when(jnp.logical_not(late))
        def _():
            relays(at + jnp.where(middle, lead, 0))

        @pl.when(jnp.logical_and(late, at < last))
        def _():
            own_at(at)
            relay(at, Z - 1, out)

        if square:
            for l in (2 * at - 1, 2 * at):
                @pl.when(jnp.logical_and(l >= 0, l < L))
                def _():
                    a_relay(l)

        @pl.when(at == max(Z - 3, 0))
        def _():
            squares_sum()

        @pl.when(at == Z - 2)
        def _():
            to_root()

        @pl.when(jnp.logical_and(at == jnp.where(middle, last, last - 1), z != root))
        def _():
            q_arrived()

        @pl.when(at == Z - 2)
        def _():
            scales()

        @pl.when(at >= Z - 2)
        def _():
            compute(at - (Z - 2))

        @pl.when(jnp.logical_and(late, at < last - 1))
        def _():
            for d in range(Z - 2, 0, -1):
                relay(at, d, out)

        @pl.when(jnp.logical_and(at == last - 4, z == root))
        def _():
            at_root()

        @pl.when(jnp.logical_and(ends, at >= last - 3))
        def _():
            dots_sum(at - (last - 3))

        @pl.when(jnp.logical_and(ends, at == last - 2))
        def _():
            correct(0, not square)

    @pl.loop(jnp.where(middle, 0, L - 2), L - 2)
    def _(l):
        dots_sum(l)

    @pl.loop(jnp.where(middle, 0, 1), L - 3)
    def _(l):
        correct(l, not square)

    @pl.when(z == root)
    def _():
        for copy in out_copies(1):
            copy.start()
        to_sib[5].start()

    arrived(Qg.at[core, pl.ds(0, C - 1)], col_in.at[0])
    to_sib[4].start()

    correct(L - 3, not square)

    arrived(Qg.at[1 - core], sib_in.at[4])

    @pl.loop(0, L)
    def _(l):
        half, at = l // H, lax.rem(l, H)
        for s in range(C):
            Qc[l, :, s * TC:(s + 1) * TC] = Qg[half, s, at]
        oug[l] = mm(Qc[l], G[l], ((1,), (0,))) * scl[l]

    @pl.when(middle)
    def _():
        rs_second(L - 3)

    rs_second(L - 2)

    correct(L - 2, True)

    correct(L - 1, True)

    rs_second(L - 1)

    if square:
        @pl.loop(0, L - 2)
        def _(l):
            q_second(l)

    @pl.when(z != root)
    def _():
        arrived(out_ref(1), out_in.at[1])
        to_sib[5].start()

    for l in range(L):
        mgrad[l:l + 1] = mg3[l]

    arrived(im_fin.at[1 - core], sib_in.at[5])

    @pl.loop(0, L)
    def _(l):
        oug[l] += im_fin[l // H, lax.rem(l, H)].astype(F32) * cor[l]

    def done(copy):
        copy.wait_send()

    @pl.loop(0, L)
    def _(l):
        g_own_each(l, done)
        for d in range(1, Z):
            g_relay(l, d, 1, done, False)
            g_relay(l, d, -1, done, False)
        for copy in a_copies(l):
            copy.wait_send()
        if square:
            for copy in a_passes(l):
                copy.wait_send()

    @pl.loop(0, L - 2)
    def _(l):
        dt_own_each(l, done)

        @pl.when(in_charge(l))
        def _():
            dt_tot_copy(l).wait_send()

    for copy in sq_copies() + to_sib + gather_copies() + dt_all_copies(L - 2) + dt_all_copies(L - 1):
        copy.wait_send()

    @pl.when(z == root)
    def _():
        for copy in out_copies(0) + out_copies(1):
            copy.wait_send()

    @pl.when(z != root)
    def _():
        for copy in root_copies():
            copy.wait_send()

    if square:
        arrived(rs2_r, rs2_in.at[0])

    @pl.loop(0, L)
    def _(l):
        rs_finish(l)

    if square:
        arrived(q2_r.at[pl.ds(0, L - 2)], q2_in.at[0])

        @pl.loop(0, L - 2)
        def _(l):
            for i in range(2):
                ing[l, :, cols(i)] += q2_r[l, i].astype(F32)

    @pl.loop(L - 2 if square else 0, L)
    def _(l):
        arrived(q_recv.at[pl.ds(1, C - 1), l], q_in.at[l])
        for i in range(halves):
            total = ing[l, :, cols(i)]
            for d in range(1, C):
                total = total + q_recv[d, l, i].astype(F32)
            ing[l, :, cols(i)] = total

    @pl.loop(0, L)
    def _(l):
        for copy in rs1_copies(l) + (rs2_copies(l) if square else []):
            copy.wait_send()

    @pl.loop(0, L - 2)
    def _(l):
        for copy in q1_copies(l) + q2_copies(l) if square else q_copies(l):
            copy.wait_send()

    for copy in q_copies(L - 2) + q_copies(L - 1):
        copy.wait_send()


def finish(ig, ing, oug, mgrad, ig_out, ing_out, oug_out, mgrad_out, sem):
    pairs = ((ig, ig_out), (ing, ing_out), (oug, oug_out), (mgrad, mgrad_out))
    copies = [pltpu.make_async_copy(a, b, sem.at[i]) for i, (a, b) in enumerate(pairs)]
    for copy in copies:
        copy.start()
    for copy in copies:
        copy.wait()


def body(R, C, acts, grads, frozen, ain, aout, mag):
    L, TR, W = grads.shape
    TC, KI = acts.shape[1:]
    RANK = ain.shape[1]
    V = pltpu.VMEM
    vm = pl.BlockSpec(memory_space=pltpu.VMEM)
    hbm = pl.BlockSpec(memory_space=pltpu.HBM)
    buffers = scratch(R, C, L, TR, W, TC, KI, RANK)
    ig, ing, oug, mgrad = pl.pallas_call(
        functools.partial(kernel, R, C),
        out_shape=(V((L, TC, KI), BF16), V((L, RANK, KI), F32), V((L, RANK, W), F32), V((L, W), F32)),
        in_specs=[hbm] * 6,
        out_specs=(vm,) * 4,
        scratch_shapes=[buffers[name] for name in NAMES],
        compiler_params=pltpu.CompilerParams(
            collective_id=0, has_side_effects=True, vmem_limit_bytes=60 * 1024 * 1024
        ),
    )(acts, grads, frozen, ain, aout, mag)
    return pl.pallas_call(
        finish,
        out_shape=tuple(jax.ShapeDtypeStruct(x.shape, x.dtype) for x in (ig, ing, oug, mgrad)),
        in_specs=[vm] * 4,
        out_specs=(hbm,) * 4,
        scratch_shapes=[pltpu.SemaphoreType.DMA((4,))],
        compiler_params=pltpu.CompilerParams(vmem_limit_bytes=1024 * 1024),
    )(ig, ing, oug, mgrad)


def solution(mesh):
    return jax.shard_map(
        functools.partial(body, mesh.shape["row"], mesh.shape["col"]),
        mesh=mesh,
        in_specs=(
            P(None, "col", "row"),
            P(None, "row", "col"),
            P(None, "row", "col"),
            P(None, None, "row"),
            P(None, None, "col"),
            P(None, "col"),
        ),
        out_specs=(
            P(None, "col", "row"),
            P(None, None, "row"),
            P(None, None, "col"),
            P(None, "col"),
        ),
        check_vma=False,
    )
```

```python
import functools

import jax
import jax.numpy as jnp
from jax import lax
from jax.experimental import pallas as pl
from jax.experimental.pallas import tpu as pltpu
from jax.sharding import PartitionSpec as P

MESH = pl.DeviceIdType.MESH
F32 = jnp.float32
BF16 = jnp.bfloat16


def mm(a, b, dims):
    return lax.dot_general(a, b, (dims, ((), ())), preferred_element_type=F32)


NAMES = (
    "acts", "grads", "frozen", "ain", "aout", "mag", "load", "G", "A", "merged", "ws", "asc", "sqm", "sq_sib", "sq_z",
    "sq_tot", "norms", "scl", "cor", "mag3", "mg3", "prod_buf", "qs", "q_sib", "q_all", "Qg", "Qc", "ims", "im_sib",
    "im_all", "im_fin", "dt_own", "dt_tot", "dt_all", "q", "q_recv", "q1_r", "q2_s", "q2_r", "own",
    "hold", "rs1_s", "rs1_r", "rs2_s", "rs2_r", "send", "g_in", "g_fw", "a_in", "rs1_in", "rs2_in", "sq_in", "dt_in",
    "dt_last", "root_in", "out_in", "col_in", "sib_in", "news", "q_in", "q1_in", "q2_in",
)


def scratch(R, C, L, TR, W, TC, KI, RANK):
    Z, T, H, KH = R // 2, TR * R, L // 2, KI // 2
    V, dma = pltpu.VMEM, pltpu.SemaphoreType.DMA
    wide = (2, L, 2, TC, KH) if C == 4 else (C, L, TC, KI)
    slim = (2, L, TC, KH) if C == 4 else (1, 1, 8, 128)
    pair = (L, 2, RANK, KH) if C == 4 else (L, 1, RANK, KI)
    return dict(
        acts=V((L, TC, KI), BF16), grads=V((L, TR, W), BF16), frozen=V((L, KI, W), BF16),
        ain=V((L, RANK, KI), BF16), aout=V((L, RANK, W), BF16), mag=V((L, W), F32), load=dma((6,)),
        G=V((L, T, W), BF16), A=V((L, T, KI), BF16), merged=V((L, KI, W), F32), ws=V((L, KI, W), BF16),
        asc=V((L, RANK, W), BF16),
        sqm=V((L, 1, W), F32), sq_sib=V((H, 1, W), F32), sq_z=V((Z, H, 1, W), F32), sq_tot=V((2, H, 1, W), F32),
        norms=V((L, 1, W), F32), scl=V((L, 1, W), F32), cor=V((L, 1, W), F32), mag3=V((L, 1, W), F32),
        mg3=V((L, 1, W), F32),
        prod_buf=V((T, KI), F32), qs=V((2, H, RANK, TC), F32), q_sib=V((H, RANK, TC), F32), q_all=V((Z, H, RANK, TC), BF16),
        Qg=V((2, C, H, RANK, TC), BF16), Qc=V((L, RANK, T), BF16),
        ims=V((2, H, RANK, W), F32), im_sib=V((H, RANK, W), F32), im_all=V((Z, H, RANK, W), BF16),
        im_fin=V((2, H, RANK, W), BF16),
        dt_own=V((L, R, 1, W), F32),
        dt_tot=V((L, 1, W), F32), dt_all=V((2, R, 1, W), F32), q=V(pair, BF16), q_recv=V((C,) + pair, BF16),
        q1_r=V(pair, BF16), q2_s=V(pair, BF16), q2_r=V(pair, BF16),
        own=V((L, TC, KI), F32), hold=V(slim, F32), rs1_s=V(wide, BF16), rs1_r=V(wide, BF16),
        rs2_s=V(slim, BF16), rs2_r=V(slim, BF16),
        send=dma((1,)), g_in=dma((L, Z - 1)), g_fw=dma((L,)), a_in=dma((L, 2)), rs1_in=dma((L,)), rs2_in=dma((1,)),
        sq_in=dma((1,)), dt_in=dma((2, L - 2)), dt_last=dma((2,)), root_in=dma((2,)), out_in=dma((2,)), col_in=dma((1,)),
        sib_in=dma((6,)), news=pltpu.SemaphoreType.REGULAR((2, max(Z - 2, 1))), q_in=dma((2 if C == 4 else L,)), q1_in=dma((L - 2,)), q2_in=dma((1,)),
    )


def kernel(R, C, *refs):
    acts_hbm, grads_hbm, frozen_hbm, ain_hbm, aout_hbm, mag_hbm, ig, ing, oug, mgrad = refs[:10]
    (acts, grads, frozen, ain, aout, mag, load, G, A, merged, ws, asc, sqm, sq_sib, sq_z, sq_tot, norms, scl, cor,
     mag3, mg3, prod_buf, qs, q_sib, q_all, Qg, Qc, ims, im_sib, im_all, im_fin, dt_own, dt_tot,
     dt_all, q, q_recv, q1_r, q2_s, q2_r, own, hold, rs1_s, rs1_r, rs2_s, rs2_r, send, g_in, g_fw, a_in, rs1_in,
     rs2_in, sq_in, dt_in, dt_last, root_in, out_in, col_in, sib_in, news, q_in, q1_in, q2_in) = refs[10:]
    pairs = ((grads_hbm, grads), (acts_hbm, acts), (frozen_hbm, frozen),
             (ain_hbm, ain), (aout_hbm, aout), (mag_hbm, mag))
    loads = [pltpu.make_async_copy(a, b, load.at[i]) for i, (a, b) in enumerate(pairs)]
    for copy in loads:
        copy.start()
    L, TR, W = grads.shape
    TC, KI = acts.shape[1:]
    Z, H, KH = R // 2, L // 2, KI // 2
    ahead = min(3, L)
    last = L + Z - 3
    r, c = lax.axis_index("row"), lax.axis_index("col")
    z, core = r // 2, lax.rem(r, 2)
    sib = 2 * z + 1 - core
    square = C == 4
    xn, yn = c + 1 - 2 * lax.rem(c, 2), lax.rem(c + 2, 4)
    dg = 3 - c
    root = Z // 2 - 1 + core
    middle = jnp.logical_and(z > 0, z < Z - 1)
    ends = jnp.logical_not(middle)
    halves = 2 if square else 1
    KS = KI // halves

    def row_to(d):
        return lax.rem(r + d, R)

    def row_from(d):
        return lax.rem(r + R - d, R)

    def col_to(d):
        return lax.rem(c + d, C)

    def col_from(d):
        return lax.rem(c + C - d, C)

    def z_to(d):
        return 2 * lax.rem(z + d, Z) + core

    def z_from(d):
        return lax.rem(z + Z - d, Z)

    def rows(at, size):
        return pl.ds(pl.multiple_of(at * size, size), size)

    def rcopy(src, dst, recv, **dev):
        return pltpu.make_async_remote_copy(
            src_ref=src, dst_ref=dst, send_sem=send.at[0], recv_sem=recv,
            device_id=dev, device_id_type=MESH,
        )

    def arrived(ref, recv):
        rcopy(ref, ref, recv, row=r).wait_recv()

    barrier = pltpu.get_barrier_semaphore()

    def greet(**dev):
        pl.semaphore_signal(barrier, inc=1, device_id=dev, device_id_type=MESH)

    greet(row=sib)
    for step in (1, -1):
        @pl.when(jnp.logical_and(z + step >= 0, z + step < Z))
        def _():
            greet(row=r + 2 * step)

    near = [xn, yn] if square else [col_to(d) for d in range(1, C)]
    for to in near:
        greet(col=to)
    pl.semaphore_wait(barrier, len(near) + jnp.where(middle, 3, 2))

    def tell(hops):
        for i, step in enumerate((1, -1)):
            of = z - step * (hops - 1)

            @pl.when((z + step >= 0) & (z + step < Z) & (of >= 0) & (of < Z))
            def _():
                pl.semaphore_signal(
                    news.at[i, hops - 2], inc=1, device_id={"row": r + 2 * step}, device_id_type=MESH
                )

    def hear(hops):
        for i, step in enumerate((1, -1)):
            of = z - step * hops

            @pl.when((of >= 0) & (of < Z))
            def _():
                pl.semaphore_wait(news.at[i, hops - 2], 1)

    def g_block(l, at, which):
        return G.at[l, rows(2 * at + which, TR)]

    def g_sem(l, at, to):
        return g_in.at[l, at - jnp.where(at > to, 1, 0)]

    def g_own(l, step):
        if step == 0:
            return rcopy(grads.at[l], g_block(l, z, core), g_fw.at[l], row=sib)
        return rcopy(grads.at[l], g_block(l, z, core), g_sem(l, z, z + step), row=r + 2 * step)

    def g_pass(l, at, step):
        block = g_block(l, at, core)
        if isinstance(step, int) and step == 0:
            return rcopy(block, block, g_fw.at[l], row=sib)
        return rcopy(block, block, g_sem(l, at, z + step), row=r + 2 * step)

    def g_own_each(l, act):
        @pl.when(z < Z - 1)
        def _():
            act(g_own(l, 1))

        @pl.when(z > 0)
        def _():
            act(g_own(l, -1))

        act(g_own(l, 0))

    def g_relay(l, d, step, act, arrive):
        at = z - step * d

        @pl.when(jnp.logical_and(at >= 0, at < Z))
        def _():
            if arrive:
                arrived(g_block(l, at, core), g_sem(l, at, z))

            @pl.when(jnp.logical_and(z + step >= 0, z + step < Z))
            def _():
                act(g_pass(l, at, step))

            act(g_pass(l, at, 0))

    def a_copies(l):
        mine = A.at[l, rows(c, TC)]
        if square:
            return [rcopy(acts.at[l], mine, a_in.at[l, 0], col=xn), rcopy(acts.at[l], mine, a_in.at[l, 0], col=yn)]
        return [rcopy(acts.at[l], mine, a_in.at[l, 0], col=col_to(d)) for d in range(1, C)]

    def a_half(l, of, part):
        size = TC // 2
        return A.at[l, rows(2 * of + part, size)]

    def a_passes(l):
        first, second = a_half(l, xn, 0), a_half(l, yn, 1)
        return [rcopy(first, first, a_in.at[l, 1], col=yn), rcopy(second, second, a_in.at[l, 1], col=xn)]

    def a_relay(l):
        arrived(A.at[l, pl.ds(0, 2 * TC)], a_in.at[l, 0])
        for copy in a_passes(l):
            copy.start()

    def a_ready(l):
        if square:
            arrived(A.at[l, rows(dg, TC)], a_in.at[l, 1])
        else:
            arrived(A.at[l, pl.ds(0, (C - 1) * TC)], a_in.at[l, 0])

    def rs1_copies(l):
        if square:
            return [rcopy(rs1_s.at[i, l], rs1_r.at[i, l], rs1_in.at[l], col=to) for i, to in enumerate((xn, yn))]
        return [rcopy(rs1_s.at[d, l], rs1_r.at[d, l], rs1_in.at[l], col=col_to(d)) for d in range(1, C)]

    def rs2_copies(l):
        return [rcopy(rs2_s.at[i, l], rs2_r.at[i, l], rs2_in.at[0], col=to) for i, to in enumerate((yn, xn))]

    def rs_first(l, prod):
        if square:
            for i, near in enumerate((xn, yn)):
                rs1_s[i, l, 0] = prod[rows(near, TC), cols(i)].astype(BF16)
                rs1_s[i, l, 1] = prod[rows(dg, TC), cols(i)].astype(BF16)
                hold[i, l] = prod[rows((yn, xn)[i], TC), cols(i)]
        else:
            for d in range(1, C):
                rs1_s[d, l] = prod[rows(col_to(d), TC)].astype(BF16)
        own[l] = prod[rows(c, TC)]
        for copy in rs1_copies(l):
            copy.start()

    def rs_second(l):
        if square:
            arrived(rs1_r.at[:, l], rs1_in.at[l])
            for i in range(2):
                rs2_s[i, l] = (hold[i, l] + rs1_r[i, l, 1].astype(F32)).astype(BF16)
            for copy in rs2_copies(l):
                copy.start()

    def rs_finish(l):
        if square:
            for i in range(2):
                total = own[l, :, cols(i)] + rs1_r[i, l, 0].astype(F32) + rs2_r[i, l].astype(F32)
                ig[l, :, cols(i)] = total.astype(BF16)
        else:
            total = own[l]
            arrived(rs1_r.at[pl.ds(1, C - 1), l], rs1_in.at[l])
            for d in range(1, C):
                total = total + rs1_r[d, l].astype(F32)
            ig[l] = total.astype(BF16)

    def sq_copies():
        return [rcopy(sq_z.at[z], sq_z.at[z], sq_in.at[0], row=z_to(d)) for d in range(1, Z)]

    to_sib = [
        rcopy(sqm.at[pl.ds((1 - core) * H, H)], sq_sib, sib_in.at[0], row=sib),
        rcopy(sq_tot.at[core], sq_tot.at[core], sib_in.at[1], row=sib),
        rcopy(qs.at[1 - core], q_sib, sib_in.at[2], row=sib),
        rcopy(ims.at[1 - core], im_sib, sib_in.at[3], row=sib),
        rcopy(Qg.at[core], Qg.at[core], sib_in.at[4], row=sib),
        rcopy(im_fin.at[core], im_fin.at[core], sib_in.at[5], row=sib),
    ]

    def root_copy(i):
        ref = (q_all, im_all)[i].at[z]
        return rcopy(ref, ref, root_in.at[i], row=2 * root + core)

    def out_ref(i):
        return Qg.at[core, c] if i == 0 else im_fin.at[core]

    def out_copies(i):
        ref = out_ref(i)
        return [rcopy(ref, ref, out_in.at[i], row=z_to(d)) for d in range(1, Z)]

    def gather_copies():
        mine = Qg.at[core, c]
        return [rcopy(mine, mine, col_in.at[0], col=col_to(d)) for d in range(1, C)]

    def start(copy):
        copy.start()

    def to_root(i):
        mine, theirs, every = (qs, q_sib, q_all) if i == 0 else (ims, im_sib, im_all)
        arrived(theirs, sib_in.at[2 + i])
        every[z] = (mine[core] + theirs[...]).astype(BF16)

        @pl.when(z != root)
        def _():
            root_copy(i).start()

    def at_root(i):
        every = (q_all, im_all)[i]
        arrived(every.at[pl.ds(0, Z - 1)], root_in.at[i])
        total = every[0].astype(F32)
        for s in range(1, Z):
            total = total + every[s].astype(F32)
        if i == 0:
            Qg[core, c] = total.astype(BF16)
        else:
            im_fin[core] = total.astype(BF16)
        for copy in out_copies(i) + (gather_copies() if i == 0 else [to_sib[5]]):
            copy.start()

    def q_arrived():
        arrived(out_ref(0), out_in.at[0])
        for copy in gather_copies():
            copy.start()

    def dt_all_copies(l):
        mine = dt_all.at[l - (L - 2), r]
        return [rcopy(mine, mine, dt_last.at[l - (L - 2)], row=row_to(d)) for d in range(1, R)]

    def dt_own_copy(l, at):
        mine = dt_own.at[l, r]
        return rcopy(mine, mine, dt_in.at[0, l], row=2 * at + lax.rem(l, 2))

    def dt_own_each(l, act):
        for d in range(1, Z):
            act(dt_own_copy(l, lax.rem(z + d, Z)))

        @pl.when(jnp.logical_not(in_charge(l)))
        def _():
            act(dt_own_copy(l, z))

    def dt_tot_copy(l):
        return rcopy(dt_tot.at[l], dt_tot.at[l], dt_in.at[1, l], row=sib)

    def in_charge(l):
        return lax.rem(l, 2) == core

    def dots_out(l, part):
        @pl.when(l < L - 2)
        def _():
            dt_own[l, r] = part
            dt_own_each(l, start)

        @pl.when(l >= L - 2)
        def _():
            dt_all[l - (L - 2), r] = part
            for copy in dt_all_copies(l):
                copy.start()

    def dots_sum(l):
        @pl.when(in_charge(l))
        def _():
            arrived(dt_own.at[l, pl.ds(0, R - 1)], dt_in.at[0, l])
            total = dt_own[l, 0]
            for s in range(1, R):
                total = total + dt_own[l, s]
            dt_tot[l] = total
            dt_tot_copy(l).start()

    def q_sem(l):
        return q_in.at[l - (L - 2) if square else l]

    def q_copies(l):
        return [rcopy(q.at[l], q_recv.at[d, l], q_sem(l), col=col_to(d)) for d in range(1, C)]

    def q1_copies(l):
        return [rcopy(q.at[l, i], q1_r.at[l, i], q1_in.at[l], col=to) for i, to in enumerate((xn, yn))]

    def q2_copies(l):
        return [rcopy(q2_s.at[l, i], q2_r.at[l, i], q2_in.at[0], col=to) for i, to in enumerate((yn, xn))]

    def cols(i):
        return slice(i * KS, (i + 1) * KS)

    loads[0].wait()
    loads[1].wait()

    @pl.loop(0, ahead)
    def _(l):
        g_own_each(l, start)

    @pl.loop(0, L)
    def _(l):
        for copy in a_copies(l):
            copy.start()

    if Z > 2:
        tell(2)
    for copy in loads[2:]:
        copy.wait()

    @pl.loop(0, L)
    def _(l):
        m = frozen[l].astype(F32) + mm(ain[l], aout[l], ((0,), (0,)))
        merged[l] = m
        sqm[l] = jnp.sum(m * m, axis=0, keepdims=True)

    to_sib[0].start()
    for hops in range(2, Z):
        hear(hops)
        if hops < Z - 1:
            tell(hops + 1)

    @pl.loop(0, L)
    def _(l):
        G[l, rows(r, TR)] = grads[l]
        A[l, rows(c, TC)] = acts[l]
        half, at = l // H, lax.rem(l, H)
        ims[half, at] = mm(ain[l], merged[l].astype(BF16), ((1,), (0,)))
        qs[half, at] = mm(ain[l], acts[l], ((1,), (1,)))

    to_sib[2].start()
    to_sib[3].start()
    for l in range(L):
        mag3[l] = mag[l:l + 1]

    def squares_out():
        arrived(sq_sib, sib_in.at[0])
        sq_z[z] = sqm[pl.ds(core * H, H)] + sq_sib[...]
        for copy in sq_copies():
            copy.start()

    def squares_sum():
        arrived(sq_z.at[pl.ds(0, Z - 1)], sq_in.at[0])
        total = sq_z[0]
        for s in range(1, Z):
            total = total + sq_z[s]
        sq_tot[core] = total
        to_sib[1].start()

    def scales():
        arrived(sq_tot.at[1 - core], sib_in.at[1])

        @pl.loop(0, L)
        def _(l):
            n = jnp.sqrt(sq_tot[l // H, lax.rem(l, H)] + 0.25)
            s = mag3[l] / n
            norms[l] = n
            scl[l] = s
            ws[l] = (merged[l] * s).astype(BF16)
            asc[l] = (aout[l].astype(F32) * s).astype(BF16)

    def correct(l, direct):
        if isinstance(l, int) and l >= L - 2:
            every = dt_all.at[l - (L - 2)]
            arrived(every.at[pl.ds(0, R - 1)], dt_last.at[l - (L - 2)])
            dots = every[0]
            for s in range(1, R):
                dots = dots + every[s]
        else:
            @pl.when(jnp.logical_not(in_charge(l)))
            def _():
                arrived(dt_tot.at[l], dt_in.at[1, l])

            dots = dt_tot[l]
        n = norms[l]
        mg3[l] = dots / n
        factor = -mag3[l] * dots / (n * n * n)
        cor[l] = factor
        adjusted = (merged[l] * factor).astype(BF16)
        part = ing[l] + mm(aout[l], adjusted, ((1,), (1,)))
        ing[l] = part
        for i in range(halves):
            q[l, i] = part[:, cols(i)].astype(BF16)
        for copy in q_copies(l) if direct else q1_copies(l):
            copy.start()

    def q_second(l):
        arrived(q1_r.at[l], q1_in.at[l])
        for i in range(2):
            total = ing[l, :, cols(i)] + q1_r[l, i].astype(F32)
            ing[l, :, cols(i)] = total
            q2_s[l, i] = total.astype(BF16)
        for copy in q2_copies(l):
            copy.start()

    out = jnp.where(z < Z // 2, -1, 1)

    def relay(at, d, step):
        l = at - (d - 1)

        @pl.when(jnp.logical_and(l >= 0, l < L))
        def _():
            g_relay(l, d, step, start, True)

    def compute(l):
        back = jnp.where(middle, 3, 2)

        @pl.when((l >= back) & (middle | (l < L - 1)))
        def _():
            rs_second(l - back)

        @pl.when(jnp.logical_and(ends, l == L - 1))
        def _():
            correct(1, not square)
            if square:
                q_second(0)

        arrived(G.at[l, pl.ds(0, Z * TR)], g_fw.at[l])
        a_ready(l)
        g = G[l]
        outer = mm(A[l], g, ((0,), (0,)))
        dots_out(l, jnp.sum(merged[l] * outer, axis=0, keepdims=True))

        @pl.when(ends & (l == L - 2) & (core == 0))
        def _():
            relay(last - 1, Z - 2, out)

        @pl.when(jnp.logical_and(ends, l == L - 1))
        def _():
            dots_sum(L - 3)

        low = outer.astype(BF16)
        prod_buf[...] = mm(g, ws[l], ((1,), (1,)))
        rs_first(l, prod_buf)

        @pl.when(ends & (l == L - 2) & (core == 0))
        def _():
            relay(last, Z - 1, out)

        ing[l] = mm(asc[l], low, ((1,), (1,)))

        @pl.when(jnp.logical_and(ends, l == L - 1))
        def _():
            rs_second(L - 3)

    def own_at(at):
        @pl.when(at + ahead < L)
        def _():
            g_own_each(at + ahead, start)

    def relays(at):
        own_at(at)

        @pl.when(at < Z - 2)
        def _():
            for d in range(1, Z):
                relay(at, d, -out)
                relay(at, d, out)

        @pl.when(at >= Z - 2)
        def _():
            for d in range(1, Z):
                relay(at, d, -out)
            for d in range(Z - 1, 0, -1):
                relay(at, d, out)

    squares_out()
    lead = 1

    @pl.when(middle)
    def _():
        for at in range(lead):
            relays(at)

    @pl.loop(0, last + 1)
    def _(at):
        late = jnp.logical_and(jnp.logical_not(middle), at >= Z - 2)

        @pl.when(jnp.logical_not(late))
        def _():
            relays(at + jnp.where(middle, lead, 0))

        @pl.when(jnp.logical_and(late, at < last))
        def _():
            own_at(at)
            relay(at, Z - 1, out)

        @pl.when(ends & (at == last - 1) & (core == 1))
        def _():
            relay(last - 1, Z - 2, out)
            relay(last, Z - 1, out)

        if square:
            for l in (2 * at - 1, 2 * at):
                @pl.when(jnp.logical_and(l >= 0, l < L))
                def _():
                    a_relay(l)

        @pl.when(at == max(Z - 3, 0))
        def _():
            squares_sum()

        @pl.when(at == Z - 2)
        def _():
            to_root(1)

        @pl.when(at == 0)
        def _():
            to_root(0)

        @pl.when(jnp.logical_and(at == jnp.where(middle, last, last - 2), z != root))
        def _():
            q_arrived()

        @pl.when(jnp.logical_and(at == Z - 2, z == root))
        def _():
            at_root(0)

        @pl.when(at == Z - 2)
        def _():
            scales()

        @pl.when(at >= Z - 2)
        def _():
            compute(at - (Z - 2))

        @pl.when(jnp.logical_and(late, at < last - 1))
        def _():
            for d in range(Z - 2, 0, -1):
                relay(at, d, out)

        @pl.when(ends & (at >= last - 3) & (at < last))
        def _():
            dots_sum(at - (last - 3))

        @pl.when(jnp.logical_and(ends, at == last - 2))
        def _():
            correct(0, not square)

    def low_rank(half):
        @pl.loop(0, H)
        def _(at):
            l = half * H + at
            for s in range(C):
                Qc[l, :, s * TC:(s + 1) * TC] = Qg[half, s, at]
            oug[l] = mm(Qc[l], G[l], ((1,), (0,))) * scl[l]

    @pl.loop(jnp.where(middle, 0, L - 2), L - 2)
    def _(l):
        dots_sum(l)

    @pl.loop(jnp.where(middle, 0, 2), L - 3)
    def _(l):
        correct(l, not square)

    @pl.when(z == root)
    def _():
        at_root(1)

    arrived(Qg.at[core, pl.ds(0, C - 1)], col_in.at[0])
    to_sib[4].start()

    correct(L - 3, not square)

    low_rank(core)

    @pl.when(middle)
    def _():
        rs_second(L - 3)

    rs_second(L - 2)

    correct(L - 2, True)

    if square:
        @pl.loop(jnp.where(middle, 0, 1), 2)
        def _(l):
            q_second(l)

    correct(L - 1, True)

    rs_second(L - 1)

    if square:
        @pl.loop(2, L - 2)
        def _(l):
            q_second(l)

    @pl.when(z != root)
    def _():
        arrived(out_ref(1), out_in.at[1])
        to_sib[5].start()

    for l in range(L):
        mgrad[l:l + 1] = mg3[l]

    arrived(Qg.at[1 - core], sib_in.at[4])
    low_rank(1 - core)

    arrived(im_fin.at[1 - core], sib_in.at[5])

    @pl.loop(0, L)
    def _(l):
        oug[l] += im_fin[l // H, lax.rem(l, H)].astype(F32) * cor[l]

    def done(copy):
        copy.wait_send()

    @pl.loop(0, L)
    def _(l):
        g_own_each(l, done)
        for d in range(1, Z):
            g_relay(l, d, 1, done, False)
            g_relay(l, d, -1, done, False)
        for copy in a_copies(l):
            copy.wait_send()
        if square:
            for copy in a_passes(l):
                copy.wait_send()

    @pl.loop(0, L - 2)
    def _(l):
        dt_own_each(l, done)

        @pl.when(in_charge(l))
        def _():
            dt_tot_copy(l).wait_send()

    for copy in sq_copies() + to_sib + gather_copies() + dt_all_copies(L - 2) + dt_all_copies(L - 1):
        copy.wait_send()

    @pl.when(z == root)
    def _():
        for copy in out_copies(0) + out_copies(1):
            copy.wait_send()

    @pl.when(z != root)
    def _():
        root_copy(0).wait_send()
        root_copy(1).wait_send()

    if square:
        arrived(rs2_r, rs2_in.at[0])

    @pl.loop(0, L)
    def _(l):
        rs_finish(l)

    if square:
        arrived(q2_r.at[pl.ds(0, L - 2)], q2_in.at[0])

        @pl.loop(0, L - 2)
        def _(l):
            for i in range(2):
                ing[l, :, cols(i)] += q2_r[l, i].astype(F32)

    @pl.loop(L - 2 if square else 0, L)
    def _(l):
        arrived(q_recv.at[pl.ds(1, C - 1), l], q_sem(l))
        for i in range(halves):
            total = ing[l, :, cols(i)]
            for d in range(1, C):
                total = total + q_recv[d, l, i].astype(F32)
            ing[l, :, cols(i)] = total

    @pl.loop(0, L)
    def _(l):
        for copy in rs1_copies(l) + (rs2_copies(l) if square else []):
            copy.wait_send()

    @pl.loop(0, L - 2)
    def _(l):
        for copy in q1_copies(l) + q2_copies(l) if square else q_copies(l):
            copy.wait_send()

    for copy in q_copies(L - 2) + q_copies(L - 1):
        copy.wait_send()


def finish(ig, ing, oug, mgrad, ig_out, ing_out, oug_out, mgrad_out, sem):
    pairs = ((ig, ig_out), (ing, ing_out), (oug, oug_out), (mgrad, mgrad_out))
    copies = [pltpu.make_async_copy(a, b, sem.at[i]) for i, (a, b) in enumerate(pairs)]
    for copy in copies:
        copy.start()
    for copy in copies:
        copy.wait()


def body(R, C, acts, grads, frozen, ain, aout, mag):
    L, TR, W = grads.shape
    TC, KI = acts.shape[1:]
    RANK = ain.shape[1]
    V = pltpu.VMEM
    vm = pl.BlockSpec(memory_space=pltpu.VMEM)
    hbm = pl.BlockSpec(memory_space=pltpu.HBM)
    buffers = scratch(R, C, L, TR, W, TC, KI, RANK)
    ig, ing, oug, mgrad = pl.pallas_call(
        functools.partial(kernel, R, C),
        out_shape=(V((L, TC, KI), BF16), V((L, RANK, KI), F32), V((L, RANK, W), F32), V((L, W), F32)),
        in_specs=[hbm] * 6,
        out_specs=(vm,) * 4,
        scratch_shapes=[buffers[name] for name in NAMES],
        compiler_params=pltpu.CompilerParams(
            collective_id=0, has_side_effects=True, vmem_limit_bytes=60 * 1024 * 1024
        ),
    )(acts, grads, frozen, ain, aout, mag)
    return pl.pallas_call(
        finish,
        out_shape=tuple(jax.ShapeDtypeStruct(x.shape, x.dtype) for x in (ig, ing, oug, mgrad)),
        in_specs=[vm] * 4,
        out_specs=(hbm,) * 4,
        scratch_shapes=[pltpu.SemaphoreType.DMA((4,))],
        compiler_params=pltpu.CompilerParams(vmem_limit_bytes=1024 * 1024),
    )(ig, ing, oug, mgrad)


def solution(mesh):
    return jax.shard_map(
        functools.partial(body, mesh.shape["row"], mesh.shape["col"]),
        mesh=mesh,
        in_specs=(
            P(None, "col", "row"),
            P(None, "row", "col"),
            P(None, "row", "col"),
            P(None, None, "row"),
            P(None, None, "col"),
            P(None, "col"),
        ),
        out_specs=(
            P(None, "col", "row"),
            P(None, None, "row"),
            P(None, None, "col"),
            P(None, "col"),
        ),
        check_vma=False,
    )
```

```python
import functools

import jax
import jax.numpy as jnp
from jax import lax
from jax.experimental import pallas as pl
from jax.experimental.pallas import tpu as pltpu
from jax.sharding import PartitionSpec as P

MESH = pl.DeviceIdType.MESH
F32 = jnp.float32
BF16 = jnp.bfloat16


def mm(a, b, dims):
    return lax.dot_general(a, b, (dims, ((), ())), preferred_element_type=F32)


NAMES = (
    "acts", "grads", "frozen", "ain", "aout", "mag", "load", "G", "A", "merged", "ws", "asc", "sqm", "sq_sib", "sq_z",
    "sq_tot", "norms", "scl", "cor", "mag3", "mg3", "prod_buf", "qs", "q_sib", "q_all", "Qg", "Qc", "ims", "im_sib",
    "im_all", "im_fin", "dt_own", "dt_tot", "dt_all", "q", "q_recv", "q1_r", "q2_s", "q2_r", "own",
    "hold", "rs1_s", "rs1_r", "rs2_s", "rs2_r", "send", "g_in", "g_fw", "a_in", "rs1_in", "rs2_in", "sq_in", "dt_in",
    "dt_last", "root_in", "out_in", "col_in", "sib_in", "news", "q_in", "q1_in", "q2_in",
)


def scratch(R, C, L, TR, W, TC, KI, RANK):
    Z, T, H, KH = R // 2, TR * R, L // 2, KI // 2
    V, dma = pltpu.VMEM, pltpu.SemaphoreType.DMA
    wide = (2, L, 2, TC, KH) if C == 4 else (C, L, TC, KI)
    slim = (2, L, TC, KH) if C == 4 else (1, 1, 8, 128)
    pair = (L, 2, RANK, KH) if C == 4 else (L, 1, RANK, KI)
    return dict(
        acts=V((L, TC, KI), BF16), grads=V((L, TR, W), BF16), frozen=V((L, KI, W), BF16),
        ain=V((L, RANK, KI), BF16), aout=V((L, RANK, W), BF16), mag=V((L, W), F32), load=dma((6,)),
        G=V((L, T, W), BF16), A=V((L, T, KI), BF16), merged=V((L, KI, W), F32), ws=V((L, KI, W), BF16),
        asc=V((L, RANK, W), BF16),
        sqm=V((L, 1, W), F32), sq_sib=V((H, 1, W), F32), sq_z=V((Z, H, 1, W), F32), sq_tot=V((2, H, 1, W), F32),
        norms=V((L, 1, W), F32), scl=V((L, 1, W), F32), cor=V((L, 1, W), F32), mag3=V((L, 1, W), F32),
        mg3=V((L, 1, W), F32),
        prod_buf=V((T, KI), F32), qs=V((2, H, RANK, TC), F32), q_sib=V((H, RANK, TC), F32), q_all=V((Z, H, RANK, TC), BF16),
        Qg=V((2, C, H, RANK, TC), BF16), Qc=V((L, RANK, T), BF16),
        ims=V((2, H, RANK, W), F32), im_sib=V((H, RANK, W), F32), im_all=V((Z, H, RANK, W), BF16),
        im_fin=V((2, H, RANK, W), BF16),
        dt_own=V((L, R, 1, W), F32),
        dt_tot=V((L, 1, W), F32), dt_all=V((2, R, 1, W), F32), q=V(pair, BF16), q_recv=V((C,) + pair, BF16),
        q1_r=V(pair, BF16), q2_s=V(pair, BF16), q2_r=V(pair, BF16),
        own=V((L, TC, KI), F32), hold=V(slim, F32), rs1_s=V(wide, BF16), rs1_r=V(wide, BF16),
        rs2_s=V(slim, BF16), rs2_r=V(slim, BF16),
        send=dma((1,)), g_in=dma((L, Z - 1)), g_fw=dma((L + 1,)), a_in=dma((L, 2)), rs1_in=dma((L,)), rs2_in=dma((2,)),
        sq_in=dma((1,)), dt_in=dma((2, L - 2)), dt_last=dma((2,)), root_in=dma((2,)), out_in=dma((2,)), col_in=dma((1,)),
        sib_in=dma((6,)), news=pltpu.SemaphoreType.REGULAR((2, max(Z - 2, 1))), q_in=dma((2 if C == 4 else L,)), q1_in=dma((L - 2,)), q2_in=dma((2,)),
    )


def kernel(R, C, *refs):
    acts_hbm, grads_hbm, frozen_hbm, ain_hbm, aout_hbm, mag_hbm, ig, ing, oug, mgrad = refs[:10]
    (acts, grads, frozen, ain, aout, mag, load, G, A, merged, ws, asc, sqm, sq_sib, sq_z, sq_tot, norms, scl, cor,
     mag3, mg3, prod_buf, qs, q_sib, q_all, Qg, Qc, ims, im_sib, im_all, im_fin, dt_own, dt_tot,
     dt_all, q, q_recv, q1_r, q2_s, q2_r, own, hold, rs1_s, rs1_r, rs2_s, rs2_r, send, g_in, g_fw, a_in, rs1_in,
     rs2_in, sq_in, dt_in, dt_last, root_in, out_in, col_in, sib_in, news, q_in, q1_in, q2_in) = refs[10:]
    pairs = ((grads_hbm, grads), (acts_hbm, acts), (frozen_hbm, frozen),
             (ain_hbm, ain), (aout_hbm, aout), (mag_hbm, mag))
    loads = [pltpu.make_async_copy(a, b, load.at[i]) for i, (a, b) in enumerate(pairs)]
    for copy in loads:
        copy.start()
    L, TR, W = grads.shape
    TC, KI = acts.shape[1:]
    Z, H, KH = R // 2, L // 2, KI // 2
    ahead = min(3, L)
    last = L + Z - 3
    r, c = lax.axis_index("row"), lax.axis_index("col")
    z, core = r // 2, lax.rem(r, 2)
    sib = 2 * z + 1 - core
    square = C == 4
    xn, yn = c + 1 - 2 * lax.rem(c, 2), lax.rem(c + 2, 4)
    dg = 3 - c
    root = Z // 2 - 1 + core
    middle = jnp.logical_and(z > 0, z < Z - 1)
    ends = jnp.logical_not(middle)
    halves = 2 if square else 1
    split = square and 2 * TR == TC
    far = jnp.where(z < Z // 2, Z - 1, 0)
    KS = KI // halves

    def row_to(d):
        return lax.rem(r + d, R)

    def row_from(d):
        return lax.rem(r + R - d, R)

    def col_to(d):
        return lax.rem(c + d, C)

    def col_from(d):
        return lax.rem(c + C - d, C)

    def z_to(d):
        return 2 * lax.rem(z + d, Z) + core

    def z_from(d):
        return lax.rem(z + Z - d, Z)

    def rows(at, size):
        return pl.ds(pl.multiple_of(at * size, size), size)

    def rcopy(src, dst, recv, **dev):
        return pltpu.make_async_remote_copy(
            src_ref=src, dst_ref=dst, send_sem=send.at[0], recv_sem=recv,
            device_id=dev, device_id_type=MESH,
        )

    def arrived(ref, recv):
        rcopy(ref, ref, recv, row=r).wait_recv()

    barrier = pltpu.get_barrier_semaphore()

    def greet(**dev):
        pl.semaphore_signal(barrier, inc=1, device_id=dev, device_id_type=MESH)

    greet(row=sib)
    for step in (1, -1):
        @pl.when(jnp.logical_and(z + step >= 0, z + step < Z))
        def _():
            greet(row=r + 2 * step)

    near = [xn, yn] if square else [col_to(d) for d in range(1, C)]
    for to in near:
        greet(col=to)
    pl.semaphore_wait(barrier, len(near) + jnp.where(middle, 3, 2))

    def tell(hops):
        for i, step in enumerate((1, -1)):
            of = z - step * (hops - 1)

            @pl.when((z + step >= 0) & (z + step < Z) & (of >= 0) & (of < Z))
            def _():
                pl.semaphore_signal(
                    news.at[i, hops - 2], inc=1, device_id={"row": r + 2 * step}, device_id_type=MESH
                )

    def hear(hops):
        for i, step in enumerate((1, -1)):
            of = z - step * hops

            @pl.when((of >= 0) & (of < Z))
            def _():
                pl.semaphore_wait(news.at[i, hops - 2], 1)

    def g_block(l, at, which):
        return G.at[l, rows(2 * at + which, TR)]

    def g_sem(l, at, to):
        return g_in.at[l, at - jnp.where(at > to, 1, 0)]

    def over(l, at):
        return jnp.where(ends & (l == L - 2) & (at == far), L, l) if split else l

    def g_own(l, step):
        if step == 0:
            return rcopy(grads.at[l], g_block(l, z, core), g_fw.at[l], row=sib)
        return rcopy(grads.at[l], g_block(l, z, core), g_sem(l, z, z + step), row=r + 2 * step)

    def g_pass(l, at, step):
        block = g_block(l, at, core)
        if isinstance(step, int) and step == 0:
            return rcopy(block, block, g_fw.at[over(l, at)], row=sib)
        return rcopy(block, block, g_sem(l, at, z + step), row=r + 2 * step)

    def g_own_each(l, act):
        @pl.when(z < Z - 1)
        def _():
            act(g_own(l, 1))

        @pl.when(z > 0)
        def _():
            act(g_own(l, -1))

        act(g_own(l, 0))

    def g_relay(l, d, step, act, arrive):
        at = z - step * d

        @pl.when(jnp.logical_and(at >= 0, at < Z))
        def _():
            if arrive:
                arrived(g_block(l, at, core), g_sem(l, at, z))

            @pl.when(jnp.logical_and(z + step >= 0, z + step < Z))
            def _():
                act(g_pass(l, at, step))

            act(g_pass(l, at, 0))

    def a_copies(l):
        mine = A.at[l, rows(c, TC)]
        if square:
            return [rcopy(acts.at[l], mine, a_in.at[l, 0], col=xn), rcopy(acts.at[l], mine, a_in.at[l, 0], col=yn)]
        return [rcopy(acts.at[l], mine, a_in.at[l, 0], col=col_to(d)) for d in range(1, C)]

    def a_half(l, of, part):
        size = TC // 2
        return A.at[l, rows(2 * of + part, size)]

    def a_passes(l):
        first, second = a_half(l, xn, 0), a_half(l, yn, 1)
        return [rcopy(first, first, a_in.at[l, 1], col=yn), rcopy(second, second, a_in.at[l, 1], col=xn)]

    def a_relay(l):
        arrived(A.at[l, pl.ds(0, 2 * TC)], a_in.at[l, 0])
        for copy in a_passes(l):
            copy.start()

    def a_ready(l):
        if square:
            arrived(A.at[l, rows(dg, TC)], a_in.at[l, 1])
        else:
            arrived(A.at[l, pl.ds(0, (C - 1) * TC)], a_in.at[l, 0])

    def rs1_copies(l):
        if square:
            return [rcopy(rs1_s.at[i, l], rs1_r.at[i, l], rs1_in.at[l], col=to) for i, to in enumerate((xn, yn))]
        return [rcopy(rs1_s.at[d, l], rs1_r.at[d, l], rs1_in.at[l], col=col_to(d)) for d in range(1, C)]

    def rs2_copies(l):
        return [rcopy(rs2_s.at[i, l], rs2_r.at[i, l], rs2_in.at[l // (L - 1)], col=to) for i, to in enumerate((yn, xn))]

    def rs_keep(l, prod):
        for i in range(2):
            hold[i, l] = prod[rows((yn, xn)[i], TC), cols(i)]
        own[l] = prod[rows(c, TC)]

    def rs_parts(l, late):
        for i, near in enumerate((xn, yn)):
            for which, block in enumerate((near, dg)):
                @pl.when((block == far) if late else (block != far))
                def _():
                    part, there = rs1_s.at[i, l, which], rs1_r.at[i, l, which]
                    rs1_s[i, l, which] = prod_buf[rows(block, TC), cols(i)].astype(BF16)
                    rcopy(part, there, rs1_in.at[l], col=near).start()

    def rs_first(l, prod):
        if square:
            for i, near in enumerate((xn, yn)):
                rs1_s[i, l, 0] = prod[rows(near, TC), cols(i)].astype(BF16)
                rs1_s[i, l, 1] = prod[rows(dg, TC), cols(i)].astype(BF16)
                hold[i, l] = prod[rows((yn, xn)[i], TC), cols(i)]
        else:
            for d in range(1, C):
                rs1_s[d, l] = prod[rows(col_to(d), TC)].astype(BF16)
        own[l] = prod[rows(c, TC)]
        for copy in rs1_copies(l):
            copy.start()

    def rs_second(l):
        if square:
            arrived(rs1_r.at[:, l], rs1_in.at[l])
            for i in range(2):
                rs2_s[i, l] = (hold[i, l] + rs1_r[i, l, 1].astype(F32)).astype(BF16)
            for copy in rs2_copies(l):
                copy.start()

    def rs_finish(l):
        if square:
            for i in range(2):
                total = own[l, :, cols(i)] + rs1_r[i, l, 0].astype(F32) + rs2_r[i, l].astype(F32)
                ig[l, :, cols(i)] = total.astype(BF16)
        else:
            total = own[l]
            arrived(rs1_r.at[pl.ds(1, C - 1), l], rs1_in.at[l])
            for d in range(1, C):
                total = total + rs1_r[d, l].astype(F32)
            ig[l] = total.astype(BF16)

    def sq_copies():
        return [rcopy(sq_z.at[z], sq_z.at[z], sq_in.at[0], row=z_to(d)) for d in range(1, Z)]

    to_sib = [
        rcopy(sqm.at[pl.ds((1 - core) * H, H)], sq_sib, sib_in.at[0], row=sib),
        rcopy(sq_tot.at[core], sq_tot.at[core], sib_in.at[1], row=sib),
        rcopy(qs.at[1 - core], q_sib, sib_in.at[2], row=sib),
        rcopy(ims.at[1 - core], im_sib, sib_in.at[3], row=sib),
        rcopy(Qg.at[core], Qg.at[core], sib_in.at[4], row=sib),
        rcopy(im_fin.at[core], im_fin.at[core], sib_in.at[5], row=sib),
    ]

    def root_copy(i):
        ref = (q_all, im_all)[i].at[z]
        return rcopy(ref, ref, root_in.at[i], row=2 * root + core)

    def out_ref(i):
        return Qg.at[core, c] if i == 0 else im_fin.at[core]

    def out_copies(i):
        ref = out_ref(i)
        return [rcopy(ref, ref, out_in.at[i], row=z_to(d)) for d in range(1, Z)]

    def gather_copies():
        mine = Qg.at[core, c]
        return [rcopy(mine, mine, col_in.at[0], col=col_to(d)) for d in range(1, C)]

    def start(copy):
        copy.start()

    def to_root(i):
        mine, theirs, every = (qs, q_sib, q_all) if i == 0 else (ims, im_sib, im_all)
        arrived(theirs, sib_in.at[2 + i])
        every[z] = (mine[core] + theirs[...]).astype(BF16)

        @pl.when(z != root)
        def _():
            root_copy(i).start()

    def at_root(i):
        every = (q_all, im_all)[i]
        arrived(every.at[pl.ds(0, Z - 1)], root_in.at[i])
        total = every[0].astype(F32)
        for s in range(1, Z):
            total = total + every[s].astype(F32)
        if i == 0:
            Qg[core, c] = total.astype(BF16)
        else:
            im_fin[core] = total.astype(BF16)
        for copy in out_copies(i) + (gather_copies() if i == 0 else [to_sib[5]]):
            copy.start()

    def q_arrived():
        arrived(out_ref(0), out_in.at[0])
        for copy in gather_copies():
            copy.start()

    def dt_all_copies(l):
        mine = dt_all.at[l - (L - 2), r]
        return [rcopy(mine, mine, dt_last.at[l - (L - 2)], row=row_to(d)) for d in range(1, R)]

    def dt_own_copy(l, at):
        mine = dt_own.at[l, r]
        return rcopy(mine, mine, dt_in.at[0, l], row=2 * at + lax.rem(l, 2))

    def dt_own_each(l, act):
        for d in range(1, Z):
            act(dt_own_copy(l, lax.rem(z + d, Z)))

        @pl.when(jnp.logical_not(in_charge(l)))
        def _():
            act(dt_own_copy(l, z))

    def dt_tot_copy(l):
        return rcopy(dt_tot.at[l], dt_tot.at[l], dt_in.at[1, l], row=sib)

    def in_charge(l):
        return lax.rem(l, 2) == core

    def dots_out(l, part):
        @pl.when(l < L - 2)
        def _():
            dt_own[l, r] = part
            dt_own_each(l, start)

        @pl.when(l >= L - 2)
        def _():
            dt_all[l - (L - 2), r] = part
            for copy in dt_all_copies(l):
                copy.start()

    def dots_sum(l):
        @pl.when(in_charge(l))
        def _():
            arrived(dt_own.at[l, pl.ds(0, R - 1)], dt_in.at[0, l])
            total = dt_own[l, 0]
            for s in range(1, R):
                total = total + dt_own[l, s]
            dt_tot[l] = total
            dt_tot_copy(l).start()

    def q_sem(l):
        return q_in.at[l - (L - 2) if square else l]

    def q_copies(l):
        return [rcopy(q.at[l], q_recv.at[d, l], q_sem(l), col=col_to(d)) for d in range(1, C)]

    def q1_copies(l):
        return [rcopy(q.at[l, i], q1_r.at[l, i], q1_in.at[l], col=to) for i, to in enumerate((xn, yn))]

    def q2_copies(l):
        return [rcopy(q2_s.at[l, i], q2_r.at[l, i], q2_in.at[l // (L - 3)], col=to) for i, to in enumerate((yn, xn))]

    def cols(i):
        return slice(i * KS, (i + 1) * KS)

    loads[0].wait()
    loads[1].wait()

    @pl.loop(0, ahead)
    def _(l):
        g_own_each(l, start)

    @pl.loop(0, L)
    def _(l):
        for copy in a_copies(l):
            copy.start()

    if Z > 2:
        tell(2)
    for copy in loads[2:]:
        copy.wait()

    @pl.loop(0, L)
    def _(l):
        m = frozen[l].astype(F32) + mm(ain[l], aout[l], ((0,), (0,)))
        merged[l] = m
        sqm[l] = jnp.sum(m * m, axis=0, keepdims=True)

    to_sib[0].start()
    for hops in range(2, Z):
        hear(hops)
        if hops < Z - 1:
            tell(hops + 1)

    @pl.loop(0, L)
    def _(l):
        G[l, rows(r, TR)] = grads[l]
        A[l, rows(c, TC)] = acts[l]
        half, at = l // H, lax.rem(l, H)
        ims[half, at] = mm(ain[l], merged[l].astype(BF16), ((1,), (0,)))
        qs[half, at] = mm(ain[l], acts[l], ((1,), (1,)))

    to_sib[2].start()
    to_sib[3].start()
    for l in range(L):
        mag3[l] = mag[l:l + 1]

    def squares_out():
        arrived(sq_sib, sib_in.at[0])
        sq_z[z] = sqm[pl.ds(core * H, H)] + sq_sib[...]
        for copy in sq_copies():
            copy.start()

    def squares_sum():
        arrived(sq_z.at[pl.ds(0, Z - 1)], sq_in.at[0])
        total = sq_z[0]
        for s in range(1, Z):
            total = total + sq_z[s]
        sq_tot[core] = total
        to_sib[1].start()

    def scales():
        arrived(sq_tot.at[1 - core], sib_in.at[1])

        @pl.loop(0, L)
        def _(l):
            n = jnp.sqrt(sq_tot[l // H, lax.rem(l, H)] + 0.25)
            s = mag3[l] / n
            norms[l] = n
            scl[l] = s
            ws[l] = (merged[l] * s).astype(BF16)
            asc[l] = (aout[l].astype(F32) * s).astype(BF16)

    def correct(l, direct):
        if isinstance(l, int) and l >= L - 2:
            every = dt_all.at[l - (L - 2)]
            arrived(every.at[pl.ds(0, R - 1)], dt_last.at[l - (L - 2)])
            dots = every[0]
            for s in range(1, R):
                dots = dots + every[s]
        else:
            @pl.when(jnp.logical_not(in_charge(l)))
            def _():
                arrived(dt_tot.at[l], dt_in.at[1, l])

            dots = dt_tot[l]
        n = norms[l]
        mg3[l] = dots / n
        factor = -mag3[l] * dots / (n * n * n)
        cor[l] = factor
        adjusted = (merged[l] * factor).astype(BF16)
        part = ing[l] + mm(aout[l], adjusted, ((1,), (1,)))
        ing[l] = part
        for i in range(halves):
            q[l, i] = part[:, cols(i)].astype(BF16)
        for copy in q_copies(l) if direct else q1_copies(l):
            copy.start()

    def q_second(l):
        arrived(q1_r.at[l], q1_in.at[l])
        for i in range(2):
            total = ing[l, :, cols(i)] + q1_r[l, i].astype(F32)
            ing[l, :, cols(i)] = total
            q2_s[l, i] = total.astype(BF16)
        for copy in q2_copies(l):
            copy.start()

    out = jnp.where(z < Z // 2, -1, 1)

    def relay(at, d, step):
        l = at - (d - 1)

        @pl.when(jnp.logical_and(l >= 0, l < L))
        def _():
            g_relay(l, d, step, start, True)

    def compute(l):
        back = jnp.where(middle, 3, 2)

        @pl.when((l >= back) & (middle | (l < L - 1)))
        def _():
            rs_second(l - back)

        if split:
            @pl.when(jnp.logical_or(middle, l != L - 2))
            def _():
                arrived(G.at[l, pl.ds(0, Z * TR)], g_fw.at[l])

            @pl.when(jnp.logical_and(ends, l == L - 2))
            def _():
                arrived(G.at[l, pl.ds(0, (Z - 1) * TR)], g_fw.at[l])
                near_rows = pl.ds(pl.multiple_of(jnp.where(far == 0, TC, 0), TC), (Z - 1) * TC)
                prod_buf[near_rows] = mm(G[l, near_rows], ws[l], ((1,), (1,)))
                rs_parts(l, False)
                arrived(G.at[l, pl.ds(0, TR)], g_fw.at[L])
        else:
            arrived(G.at[l, pl.ds(0, Z * TR)], g_fw.at[l])
        a_ready(l)
        g = G[l]
        outer = mm(A[l], g, ((0,), (0,)))
        dots_out(l, jnp.sum(merged[l] * outer, axis=0, keepdims=True))

        @pl.when(ends & (l == L - 2) & (core == 0))
        def _():
            relay(last - 1, Z - 2, out)

        @pl.when(jnp.logical_and(ends, l == L - 2))
        def _():
            dots_sum(L - 4)
            correct(1, not square)

        @pl.when(jnp.logical_and(ends, l == L - 1))
        def _():
            dots_sum(L - 3)

        low = outer.astype(BF16)
        if split:
            @pl.when(jnp.logical_or(middle, l != L - 2))
            def _():
                prod_buf[...] = mm(G[l], ws[l], ((1,), (1,)))
                rs_first(l, prod_buf)

            @pl.when(jnp.logical_and(ends, l == L - 2))
            def _():
                prod_buf[rows(far, TC)] = mm(G[l, rows(far, TC)], ws[l], ((1,), (1,)))
                rs_parts(l, True)
                rs_keep(l, prod_buf)
        else:
            prod_buf[...] = mm(g, ws[l], ((1,), (1,)))
            rs_first(l, prod_buf)

        @pl.when(ends & (l == L - 2) & (core == 0))
        def _():
            relay(last, Z - 1, out)

        ing[l] = mm(asc[l], low, ((1,), (1,)))

        @pl.when(jnp.logical_and(ends, l == L - 1))
        def _():
            rs_second(L - 3)

    def own_at(at):
        @pl.when(at + ahead < L)
        def _():
            g_own_each(at + ahead, start)

    def relays(at):
        own_at(at)

        @pl.when(at < Z - 2)
        def _():
            for d in range(1, Z):
                relay(at, d, -out)
                relay(at, d, out)

        @pl.when(at >= Z - 2)
        def _():
            for d in range(1, Z):
                relay(at, d, -out)
            for d in range(Z - 1, 0, -1):
                relay(at, d, out)

    squares_out()
    lead = 1

    @pl.when(middle)
    def _():
        for at in range(lead):
            relays(at)

    @pl.loop(0, last + 1)
    def _(at):
        late = jnp.logical_and(jnp.logical_not(middle), at >= Z - 2)

        @pl.when(jnp.logical_not(late))
        def _():
            relays(at + jnp.where(middle, lead, 0))

        @pl.when(jnp.logical_and(late, at < last))
        def _():
            own_at(at)
            relay(at, Z - 1, out)

        @pl.when(ends & (at == last - 1) & (core == 1))
        def _():
            relay(last - 1, Z - 2, out)
            relay(last, Z - 1, out)

        if square:
            for l in (2 * at - 1, 2 * at):
                @pl.when(jnp.logical_and(l >= 0, l < L))
                def _():
                    a_relay(l)

        @pl.when(at == max(Z - 3, 0))
        def _():
            squares_sum()

        @pl.when(at == Z - 2)
        def _():
            to_root(1)

        @pl.when(at == 0)
        def _():
            to_root(0)

        @pl.when(jnp.logical_and(at == jnp.where(middle, last, last - 2), z != root))
        def _():
            q_arrived()

        @pl.when(jnp.logical_and(at == Z - 2, z == root))
        def _():
            at_root(0)

        @pl.when(at == Z - 2)
        def _():
            scales()

        @pl.when(at >= Z - 2)
        def _():
            compute(at - (Z - 2))

        @pl.when(jnp.logical_and(late, at < last - 1))
        def _():
            for d in range(Z - 2, 0, -1):
                relay(at, d, out)

        @pl.when(ends & (at >= last - 3) & (at < last - 1))
        def _():
            dots_sum(at - (last - 3))

        @pl.when(jnp.logical_and(ends, at == last - 2))
        def _():
            correct(0, not square)

    def low_rank(half):
        @pl.loop(0, H)
        def _(at):
            l = half * H + at
            for s in range(C):
                Qc[l, :, s * TC:(s + 1) * TC] = Qg[half, s, at]
            oug[l] = mm(Qc[l], G[l], ((1,), (0,))) * scl[l]

    @pl.loop(jnp.where(middle, 0, L - 2), L - 2)
    def _(l):
        dots_sum(l)

    @pl.loop(jnp.where(middle, 0, 2), L - 3)
    def _(l):
        correct(l, not square)

    @pl.when(z == root)
    def _():
        at_root(1)

    arrived(Qg.at[core, pl.ds(0, C - 1)], col_in.at[0])
    to_sib[4].start()

    correct(L - 3, not square)

    low_rank(core)

    @pl.when(middle)
    def _():
        rs_second(L - 3)

    rs_second(L - 2)

    correct(L - 2, True)

    if square:
        q_second(0)

    correct(L - 1, True)

    rs_second(L - 1)

    if square:
        @pl.loop(1, L - 2)
        def _(l):
            q_second(l)

    @pl.when(z != root)
    def _():
        arrived(out_ref(1), out_in.at[1])
        to_sib[5].start()

    for l in range(L):
        mgrad[l:l + 1] = mg3[l]

    arrived(Qg.at[1 - core], sib_in.at[4])
    low_rank(1 - core)

    arrived(im_fin.at[1 - core], sib_in.at[5])

    @pl.loop(0, L)
    def _(l):
        oug[l] += im_fin[l // H, lax.rem(l, H)].astype(F32) * cor[l]

    def done(copy):
        copy.wait_send()

    @pl.loop(0, L)
    def _(l):
        g_own_each(l, done)
        for d in range(1, Z):
            g_relay(l, d, 1, done, False)
            g_relay(l, d, -1, done, False)
        for copy in a_copies(l):
            copy.wait_send()
        if square:
            for copy in a_passes(l):
                copy.wait_send()

    @pl.loop(0, L - 2)
    def _(l):
        dt_own_each(l, done)

        @pl.when(in_charge(l))
        def _():
            dt_tot_copy(l).wait_send()

    for copy in sq_copies() + to_sib + gather_copies() + dt_all_copies(L - 2) + dt_all_copies(L - 1):
        copy.wait_send()

    @pl.when(z == root)
    def _():
        for copy in out_copies(0) + out_copies(1):
            copy.wait_send()

    @pl.when(z != root)
    def _():
        root_copy(0).wait_send()
        root_copy(1).wait_send()

    def q_finish(l):
        arrived(q_recv.at[pl.ds(1, C - 1), l], q_sem(l))
        for i in range(halves):
            total = ing[l, :, cols(i)]
            for d in range(1, C):
                total = total + q_recv[d, l, i].astype(F32)
            ing[l, :, cols(i)] = total

    def q2_finish(l):
        for i in range(2):
            ing[l, :, cols(i)] += q2_r[l, i].astype(F32)

    if square:
        arrived(rs2_r.at[:, pl.ds(0, L - 1)], rs2_in.at[0])

    @pl.loop(0, L - 1)
    def _(l):
        rs_finish(l)

    if square:
        arrived(q2_r.at[pl.ds(0, L - 3)], q2_in.at[0])

        @pl.loop(0, L - 3)
        def _(l):
            q2_finish(l)

        q_finish(L - 2)
    else:
        @pl.loop(0, L - 1)
        def _(l):
            q_finish(l)

    if square:
        arrived(rs2_r.at[:, L - 1], rs2_in.at[1])
    rs_finish(L - 1)

    q_finish(L - 1)
    if square:
        arrived(q2_r.at[L - 3], q2_in.at[1])
        q2_finish(L - 3)

    @pl.loop(0, L)
    def _(l):
        for copy in rs1_copies(l) + (rs2_copies(l) if square else []):
            copy.wait_send()

    @pl.loop(0, L - 2)
    def _(l):
        for copy in q1_copies(l) + q2_copies(l) if square else q_copies(l):
            copy.wait_send()

    for copy in q_copies(L - 2) + q_copies(L - 1):
        copy.wait_send()


def finish(ig, ing, oug, mgrad, ig_out, ing_out, oug_out, mgrad_out, sem):
    pairs = ((ig, ig_out), (ing, ing_out), (oug, oug_out), (mgrad, mgrad_out))
    copies = [pltpu.make_async_copy(a, b, sem.at[i]) for i, (a, b) in enumerate(pairs)]
    for copy in copies:
        copy.start()
    for copy in copies:
        copy.wait()


def body(R, C, acts, grads, frozen, ain, aout, mag):
    L, TR, W = grads.shape
    TC, KI = acts.shape[1:]
    RANK = ain.shape[1]
    V = pltpu.VMEM
    vm = pl.BlockSpec(memory_space=pltpu.VMEM)
    hbm = pl.BlockSpec(memory_space=pltpu.HBM)
    buffers = scratch(R, C, L, TR, W, TC, KI, RANK)
    ig, ing, oug, mgrad = pl.pallas_call(
        functools.partial(kernel, R, C),
        out_shape=(V((L, TC, KI), BF16), V((L, RANK, KI), F32), V((L, RANK, W), F32), V((L, W), F32)),
        in_specs=[hbm] * 6,
        out_specs=(vm,) * 4,
        scratch_shapes=[buffers[name] for name in NAMES],
        compiler_params=pltpu.CompilerParams(
            collective_id=0, has_side_effects=True, vmem_limit_bytes=60 * 1024 * 1024
        ),
    )(acts, grads, frozen, ain, aout, mag)
    return pl.pallas_call(
        finish,
        out_shape=tuple(jax.ShapeDtypeStruct(x.shape, x.dtype) for x in (ig, ing, oug, mgrad)),
        in_specs=[vm] * 4,
        out_specs=(hbm,) * 4,
        scratch_shapes=[pltpu.SemaphoreType.DMA((4,))],
        compiler_params=pltpu.CompilerParams(vmem_limit_bytes=1024 * 1024),
    )(ig, ing, oug, mgrad)


def solution(mesh):
    return jax.shard_map(
        functools.partial(body, mesh.shape["row"], mesh.shape["col"]),
        mesh=mesh,
        in_specs=(
            P(None, "col", "row"),
            P(None, "row", "col"),
            P(None, "row", "col"),
            P(None, None, "row"),
            P(None, None, "col"),
            P(None, "col"),
        ),
        out_specs=(
            P(None, "col", "row"),
            P(None, None, "row"),
            P(None, None, "col"),
            P(None, "col"),
        ),
        check_vma=False,
    )
```

```python
import functools

import jax
import jax.numpy as jnp
from jax import lax
from jax.experimental import pallas as pl
from jax.experimental.pallas import tpu as pltpu
from jax.sharding import PartitionSpec as P

MESH = pl.DeviceIdType.MESH
F32 = jnp.float32
BF16 = jnp.bfloat16


def mm(a, b, dims):
    return lax.dot_general(a, b, (dims, ((), ())), preferred_element_type=F32)


NAMES = (
    "acts", "grads", "frozen", "ain", "aout", "mag", "load", "G", "A", "AT", "merged", "ws", "asc", "sqm", "sq_sib", "sq_z",
    "sq_tot", "norms", "scl", "cor", "mag3", "mg3", "prod_buf", "qs", "q_sib", "q_all", "Qg", "Qc", "ims", "im_sib",
    "im_all", "im_fin", "dt_own", "dt_tot", "dt_all", "q", "q_recv", "q1_r", "q2_s", "q2_r", "own",
    "hold", "rs1_s", "rs1_r", "rs2_s", "rs2_r", "send", "g_in", "g_fw", "a_in", "rs1_in", "rs2_in", "sq_in", "dt_in",
    "dt_last", "root_in", "out_in", "col_in", "sib_in", "news", "q_in", "q1_in", "q2_in",
)


def scratch(R, C, L, TR, W, TC, KI, RANK):
    Z, T, H, KH = R // 2, TR * R, L // 2, KI // 2
    V, dma = pltpu.VMEM, pltpu.SemaphoreType.DMA
    wide = (2, L, 2, TC, KH) if C == 4 else (C, L, TC, KI)
    slim = (2, L, TC, KH) if C == 4 else (1, 1, 8, 128)
    pair = (L, 2, RANK, KH) if C == 4 else (L, 1, RANK, KI)
    return dict(
        acts=V((L, TC, KI), BF16), grads=V((L, TR, W), BF16), frozen=V((L, KI, W), BF16),
        ain=V((L, RANK, KI), BF16), aout=V((L, RANK, W), BF16), mag=V((L, W), F32), load=dma((6,)),
        G=V((L, T, W), BF16), A=V((L, T, KI), BF16), AT=V((L, KI, T), BF16), merged=V((L, KI, W), F32), ws=V((L, KI, W), BF16),
        asc=V((L, RANK, W), BF16),
        sqm=V((L, 1, W), F32), sq_sib=V((H, 1, W), F32), sq_z=V((Z, H, 1, W), F32), sq_tot=V((2, H, 1, W), F32),
        norms=V((L, 1, W), F32), scl=V((L, 1, W), F32), cor=V((L, 1, W), F32), mag3=V((L, 1, W), F32),
        mg3=V((L, 1, W), F32),
        prod_buf=V((T, KI), F32), qs=V((2, H, RANK, TC), F32), q_sib=V((H, RANK, TC), F32), q_all=V((Z, H, RANK, TC), BF16),
        Qg=V((2, C, H, RANK, TC), BF16), Qc=V((L, RANK, T), BF16),
        ims=V((2, H, RANK, W), F32), im_sib=V((H, RANK, W), F32), im_all=V((Z, H, RANK, W), BF16),
        im_fin=V((2, H, RANK, W), BF16),
        dt_own=V((L, R, 1, W), F32),
        dt_tot=V((L, 1, W), F32), dt_all=V((2, R, 1, W), F32), q=V(pair, BF16), q_recv=V((C,) + pair, BF16),
        q1_r=V(pair, BF16), q2_s=V(pair, BF16), q2_r=V(pair, BF16),
        own=V((L, TC, KI), F32), hold=V(slim, F32), rs1_s=V(wide, BF16), rs1_r=V(wide, BF16),
        rs2_s=V(slim, BF16), rs2_r=V(slim, BF16),
        send=dma((1,)), g_in=dma((L, Z - 1)), g_fw=dma((L + 1,)), a_in=dma((L, 2)), rs1_in=dma((L,)), rs2_in=dma((2,)),
        sq_in=dma((1,)), dt_in=dma((2, L - 2)), dt_last=dma((2,)), root_in=dma((2,)), out_in=dma((2,)), col_in=dma((1,)),
        sib_in=dma((6,)), news=pltpu.SemaphoreType.REGULAR((2, max(Z - 2, 1))), q_in=dma((2 if C == 4 else L,)), q1_in=dma((L - 2,)), q2_in=dma((2,)),
    )


def kernel(R, C, *refs):
    acts_hbm, grads_hbm, frozen_hbm, ain_hbm, aout_hbm, mag_hbm, ig, ing, oug, mgrad = refs[:10]
    (acts, grads, frozen, ain, aout, mag, load, G, A, AT, merged, ws, asc, sqm, sq_sib, sq_z, sq_tot, norms, scl, cor,
     mag3, mg3, prod_buf, qs, q_sib, q_all, Qg, Qc, ims, im_sib, im_all, im_fin, dt_own, dt_tot,
     dt_all, q, q_recv, q1_r, q2_s, q2_r, own, hold, rs1_s, rs1_r, rs2_s, rs2_r, send, g_in, g_fw, a_in, rs1_in,
     rs2_in, sq_in, dt_in, dt_last, root_in, out_in, col_in, sib_in, news, q_in, q1_in, q2_in) = refs[10:]
    pairs = ((grads_hbm, grads), (acts_hbm, acts), (frozen_hbm, frozen),
             (ain_hbm, ain), (aout_hbm, aout), (mag_hbm, mag))
    loads = [pltpu.make_async_copy(a, b, load.at[i]) for i, (a, b) in enumerate(pairs)]
    for copy in loads:
        copy.start()
    L, TR, W = grads.shape
    TC, KI = acts.shape[1:]
    Z, H, KH = R // 2, L // 2, KI // 2
    ahead = min(3, L)
    last = L + Z - 3
    r, c = lax.axis_index("row"), lax.axis_index("col")
    z, core = r // 2, lax.rem(r, 2)
    sib = 2 * z + 1 - core
    square = C == 4
    xn, yn = c + 1 - 2 * lax.rem(c, 2), lax.rem(c + 2, 4)
    dg = 3 - c
    root = Z // 2 - 1 + core
    middle = jnp.logical_and(z > 0, z < Z - 1)
    ends = jnp.logical_not(middle)
    halves = 2 if square else 1
    split = square and 2 * TR == TC
    far = jnp.where(z < Z // 2, Z - 1, 0)
    KS = KI // halves

    def row_to(d):
        return lax.rem(r + d, R)

    def row_from(d):
        return lax.rem(r + R - d, R)

    def col_to(d):
        return lax.rem(c + d, C)

    def col_from(d):
        return lax.rem(c + C - d, C)

    def z_to(d):
        return 2 * lax.rem(z + d, Z) + core

    def z_from(d):
        return lax.rem(z + Z - d, Z)

    def rows(at, size):
        return pl.ds(pl.multiple_of(at * size, size), size)

    def rcopy(src, dst, recv, **dev):
        return pltpu.make_async_remote_copy(
            src_ref=src, dst_ref=dst, send_sem=send.at[0], recv_sem=recv,
            device_id=dev, device_id_type=MESH,
        )

    def arrived(ref, recv):
        rcopy(ref, ref, recv, row=r).wait_recv()

    barrier = pltpu.get_barrier_semaphore()

    def greet(**dev):
        pl.semaphore_signal(barrier, inc=1, device_id=dev, device_id_type=MESH)

    greet(row=sib)
    for step in (1, -1):
        @pl.when(jnp.logical_and(z + step >= 0, z + step < Z))
        def _():
            greet(row=r + 2 * step)

    near = [xn, yn] if square else [col_to(d) for d in range(1, C)]
    for to in near:
        greet(col=to)
    pl.semaphore_wait(barrier, len(near) + jnp.where(middle, 3, 2))

    def tell(hops):
        for i, step in enumerate((1, -1)):
            of = z - step * (hops - 1)

            @pl.when((z + step >= 0) & (z + step < Z) & (of >= 0) & (of < Z))
            def _():
                pl.semaphore_signal(
                    news.at[i, hops - 2], inc=1, device_id={"row": r + 2 * step}, device_id_type=MESH
                )

    def hear(hops):
        for i, step in enumerate((1, -1)):
            of = z - step * hops

            @pl.when((of >= 0) & (of < Z))
            def _():
                pl.semaphore_wait(news.at[i, hops - 2], 1)

    def g_block(l, at, which):
        return G.at[l, rows(2 * at + which, TR)]

    def g_sem(l, at, to):
        return g_in.at[l, at - jnp.where(at > to, 1, 0)]

    def over(l, at):
        return jnp.where(ends & (l == L - 2) & (at == far), L, l) if split else l

    def g_own(l, step):
        if step == 0:
            return rcopy(grads.at[l], g_block(l, z, core), g_fw.at[l], row=sib)
        return rcopy(grads.at[l], g_block(l, z, core), g_sem(l, z, z + step), row=r + 2 * step)

    def g_pass(l, at, step):
        block = g_block(l, at, core)
        if isinstance(step, int) and step == 0:
            return rcopy(block, block, g_fw.at[over(l, at)], row=sib)
        return rcopy(block, block, g_sem(l, at, z + step), row=r + 2 * step)

    def g_own_each(l, act):
        @pl.when(z < Z - 1)
        def _():
            act(g_own(l, 1))

        @pl.when(z > 0)
        def _():
            act(g_own(l, -1))

        act(g_own(l, 0))

    def g_relay(l, d, step, act, arrive):
        at = z - step * d

        @pl.when(jnp.logical_and(at >= 0, at < Z))
        def _():
            if arrive:
                arrived(g_block(l, at, core), g_sem(l, at, z))

            @pl.when(jnp.logical_and(z + step >= 0, z + step < Z))
            def _():
                act(g_pass(l, at, step))

            act(g_pass(l, at, 0))

    def a_copies(l):
        mine = A.at[l, rows(c, TC)]
        if square:
            return [rcopy(acts.at[l], mine, a_in.at[l, 0], col=xn), rcopy(acts.at[l], mine, a_in.at[l, 0], col=yn)]
        return [rcopy(acts.at[l], mine, a_in.at[l, 0], col=col_to(d)) for d in range(1, C)]

    def a_half(l, of, part):
        size = TC // 2
        return A.at[l, rows(2 * of + part, size)]

    def a_passes(l):
        first, second = a_half(l, xn, 0), a_half(l, yn, 1)
        return [rcopy(first, first, a_in.at[l, 1], col=yn), rcopy(second, second, a_in.at[l, 1], col=xn)]

    def a_relay(l):
        arrived(A.at[l, pl.ds(0, 2 * TC)], a_in.at[l, 0])
        for copy in a_passes(l):
            copy.start()

    def a_ready(l):
        if square:
            arrived(A.at[l, rows(dg, TC)], a_in.at[l, 1])
        else:
            arrived(A.at[l, pl.ds(0, (C - 1) * TC)], a_in.at[l, 0])

    def rs1_copies(l):
        if square:
            return [rcopy(rs1_s.at[i, l], rs1_r.at[i, l], rs1_in.at[l], col=to) for i, to in enumerate((xn, yn))]
        return [rcopy(rs1_s.at[d, l], rs1_r.at[d, l], rs1_in.at[l], col=col_to(d)) for d in range(1, C)]

    def rs2_copies(l):
        return [rcopy(rs2_s.at[i, l], rs2_r.at[i, l], rs2_in.at[l // (L - 1)], col=to) for i, to in enumerate((yn, xn))]

    def rs_keep(l, prod):
        for i in range(2):
            hold[i, l] = prod[rows((yn, xn)[i], TC), cols(i)]
        own[l] = prod[rows(c, TC)]

    def rs_parts(l, late):
        for i, near in enumerate((xn, yn)):
            for which, block in enumerate((near, dg)):
                @pl.when((block == far) if late else (block != far))
                def _():
                    part, there = rs1_s.at[i, l, which], rs1_r.at[i, l, which]
                    rs1_s[i, l, which] = prod_buf[rows(block, TC), cols(i)].astype(BF16)
                    rcopy(part, there, rs1_in.at[l], col=near).start()

    def rs_first(l, prod):
        if square:
            for i, near in enumerate((xn, yn)):
                rs1_s[i, l, 0] = prod[rows(near, TC), cols(i)].astype(BF16)
                rs1_s[i, l, 1] = prod[rows(dg, TC), cols(i)].astype(BF16)
                hold[i, l] = prod[rows((yn, xn)[i], TC), cols(i)]
        else:
            for d in range(1, C):
                rs1_s[d, l] = prod[rows(col_to(d), TC)].astype(BF16)
        own[l] = prod[rows(c, TC)]
        for copy in rs1_copies(l):
            copy.start()

    def rs_second(l):
        if square:
            arrived(rs1_r.at[:, l], rs1_in.at[l])
            for i in range(2):
                rs2_s[i, l] = (hold[i, l] + rs1_r[i, l, 1].astype(F32)).astype(BF16)
            for copy in rs2_copies(l):
                copy.start()

    def rs_finish(l):
        if square:
            for i in range(2):
                total = own[l, :, cols(i)] + rs1_r[i, l, 0].astype(F32) + rs2_r[i, l].astype(F32)
                ig[l, :, cols(i)] = total.astype(BF16)
        else:
            total = own[l]
            arrived(rs1_r.at[pl.ds(1, C - 1), l], rs1_in.at[l])
            for d in range(1, C):
                total = total + rs1_r[d, l].astype(F32)
            ig[l] = total.astype(BF16)

    def sq_copies():
        return [rcopy(sq_z.at[z], sq_z.at[z], sq_in.at[0], row=z_to(d)) for d in range(1, Z)]

    to_sib = [
        rcopy(sqm.at[pl.ds((1 - core) * H, H)], sq_sib, sib_in.at[0], row=sib),
        rcopy(sq_tot.at[core], sq_tot.at[core], sib_in.at[1], row=sib),
        rcopy(qs.at[1 - core], q_sib, sib_in.at[2], row=sib),
        rcopy(ims.at[1 - core], im_sib, sib_in.at[3], row=sib),
        rcopy(Qg.at[core], Qg.at[core], sib_in.at[4], row=sib),
        rcopy(im_fin.at[core], im_fin.at[core], sib_in.at[5], row=sib),
    ]

    def root_copy(i):
        ref = (q_all, im_all)[i].at[z]
        return rcopy(ref, ref, root_in.at[i], row=2 * root + core)

    def out_ref(i):
        return Qg.at[core, c] if i == 0 else im_fin.at[core]

    def out_copies(i):
        ref = out_ref(i)
        return [rcopy(ref, ref, out_in.at[i], row=z_to(d)) for d in range(1, Z)]

    def gather_copies():
        mine = Qg.at[core, c]
        return [rcopy(mine, mine, col_in.at[0], col=col_to(d)) for d in range(1, C)]

    def start(copy):
        copy.start()

    def to_root(i):
        mine, theirs, every = (qs, q_sib, q_all) if i == 0 else (ims, im_sib, im_all)
        arrived(theirs, sib_in.at[2 + i])
        every[z] = (mine[core] + theirs[...]).astype(BF16)

        @pl.when(z != root)
        def _():
            root_copy(i).start()

    def at_root(i):
        every = (q_all, im_all)[i]
        arrived(every.at[pl.ds(0, Z - 1)], root_in.at[i])
        total = every[0].astype(F32)
        for s in range(1, Z):
            total = total + every[s].astype(F32)
        if i == 0:
            Qg[core, c] = total.astype(BF16)
        else:
            im_fin[core] = total.astype(BF16)
        for copy in out_copies(i) + (gather_copies() if i == 0 else [to_sib[5]]):
            copy.start()

    def q_arrived():
        arrived(out_ref(0), out_in.at[0])
        for copy in gather_copies():
            copy.start()

    def dt_all_copies(l):
        mine = dt_all.at[l - (L - 2), r]
        return [rcopy(mine, mine, dt_last.at[l - (L - 2)], row=row_to(d)) for d in range(1, R)]

    def dt_own_copy(l, at):
        mine = dt_own.at[l, r]
        return rcopy(mine, mine, dt_in.at[0, l], row=2 * at + lax.rem(l, 2))

    def dt_own_each(l, act):
        for d in range(1, Z):
            act(dt_own_copy(l, lax.rem(z + d, Z)))

        @pl.when(jnp.logical_not(in_charge(l)))
        def _():
            act(dt_own_copy(l, z))

    def dt_tot_copy(l):
        return rcopy(dt_tot.at[l], dt_tot.at[l], dt_in.at[1, l], row=sib)

    def in_charge(l):
        return lax.rem(l, 2) == core

    def dots_out(l, part):
        @pl.when(l < L - 2)
        def _():
            dt_own[l, r] = part
            dt_own_each(l, start)

        @pl.when(l >= L - 2)
        def _():
            dt_all[l - (L - 2), r] = part
            for copy in dt_all_copies(l):
                copy.start()

    def dots_sum(l):
        @pl.when(in_charge(l))
        def _():
            arrived(dt_own.at[l, pl.ds(0, R - 1)], dt_in.at[0, l])
            total = dt_own[l, 0]
            for s in range(1, R):
                total = total + dt_own[l, s]
            dt_tot[l] = total
            dt_tot_copy(l).start()

    def q_sem(l):
        return q_in.at[l - (L - 2) if square else l]

    def q_copies(l):
        return [rcopy(q.at[l], q_recv.at[d, l], q_sem(l), col=col_to(d)) for d in range(1, C)]

    def q1_copies(l):
        return [rcopy(q.at[l, i], q1_r.at[l, i], q1_in.at[l], col=to) for i, to in enumerate((xn, yn))]

    def q2_copies(l):
        return [rcopy(q2_s.at[l, i], q2_r.at[l, i], q2_in.at[l // (L - 3)], col=to) for i, to in enumerate((yn, xn))]

    def cols(i):
        return slice(i * KS, (i + 1) * KS)

    loads[0].wait()
    loads[1].wait()

    @pl.loop(0, ahead)
    def _(l):
        g_own_each(l, start)

    @pl.loop(0, L)
    def _(l):
        for copy in a_copies(l):
            copy.start()

    if Z > 2:
        tell(2)
    for copy in loads[2:]:
        copy.wait()

    @pl.loop(0, L)
    def _(l):
        m = frozen[l].astype(F32) + mm(ain[l], aout[l], ((0,), (0,)))
        merged[l] = m
        sqm[l] = jnp.sum(m * m, axis=0, keepdims=True)

    to_sib[0].start()
    for hops in range(2, Z):
        hear(hops)
        if hops < Z - 1:
            tell(hops + 1)

    @pl.loop(0, L)
    def _(l):
        G[l, rows(r, TR)] = grads[l]
        A[l, rows(c, TC)] = acts[l]
        half, at = l // H, lax.rem(l, H)
        ims[half, at] = mm(ain[l], merged[l].astype(BF16), ((1,), (0,)))
        qs[half, at] = mm(ain[l], acts[l], ((1,), (1,)))

    to_sib[2].start()
    to_sib[3].start()
    for l in range(L):
        mag3[l] = mag[l:l + 1]

    def squares_out():
        arrived(sq_sib, sib_in.at[0])
        sq_z[z] = sqm[pl.ds(core * H, H)] + sq_sib[...]
        for copy in sq_copies():
            copy.start()

    def squares_sum():
        arrived(sq_z.at[pl.ds(0, Z - 1)], sq_in.at[0])
        total = sq_z[0]
        for s in range(1, Z):
            total = total + sq_z[s]
        sq_tot[core] = total
        to_sib[1].start()

    def scales():
        arrived(sq_tot.at[1 - core], sib_in.at[1])

        @pl.loop(0, L)
        def _(l):
            n = jnp.sqrt(sq_tot[l // H, lax.rem(l, H)] + 0.25)
            s = mag3[l] / n
            norms[l] = n
            scl[l] = s
            ws[l] = (merged[l] * s).astype(BF16)
            asc[l] = (aout[l].astype(F32) * s).astype(BF16)

    def correct(l, direct):
        if isinstance(l, int) and l >= L - 2:
            every = dt_all.at[l - (L - 2)]
            arrived(every.at[pl.ds(0, R - 1)], dt_last.at[l - (L - 2)])
            dots = every[0]
            for s in range(1, R):
                dots = dots + every[s]
        else:
            @pl.when(jnp.logical_not(in_charge(l)))
            def _():
                arrived(dt_tot.at[l], dt_in.at[1, l])

            dots = dt_tot[l]
        n = norms[l]
        mg3[l] = dots / n
        factor = -mag3[l] * dots / (n * n * n)
        cor[l] = factor
        adjusted = (merged[l] * factor).astype(BF16)
        part = ing[l] + mm(aout[l], adjusted, ((1,), (1,)))
        ing[l] = part
        for i in range(halves):
            q[l, i] = part[:, cols(i)].astype(BF16)
        for copy in q_copies(l) if direct else q1_copies(l):
            copy.start()

    def q_second(l):
        arrived(q1_r.at[l], q1_in.at[l])
        for i in range(2):
            total = ing[l, :, cols(i)] + q1_r[l, i].astype(F32)
            ing[l, :, cols(i)] = total
            q2_s[l, i] = total.astype(BF16)
        for copy in q2_copies(l):
            copy.start()

    out = jnp.where(z < Z // 2, -1, 1)

    def relay(at, d, step):
        l = at - (d - 1)

        @pl.when(jnp.logical_and(l >= 0, l < L))
        def _():
            g_relay(l, d, step, start, True)

    def turn(l):
        a_ready(l)
        AT[l] = A[l].T

    def compute(l):
        @pl.when(l < L - 1)
        def _():
            turn(l + 1)

        back = jnp.where(middle, 3, 2)

        @pl.when((l >= back) & (middle | (l < L - 1)))
        def _():
            rs_second(l - back)

        if split:
            @pl.when(jnp.logical_or(middle, l != L - 2))
            def _():
                arrived(G.at[l, pl.ds(0, Z * TR)], g_fw.at[l])

            @pl.when(jnp.logical_and(ends, l == L - 2))
            def _():
                arrived(G.at[l, pl.ds(0, (Z - 1) * TR)], g_fw.at[l])
                near_rows = pl.ds(pl.multiple_of(jnp.where(far == 0, TC, 0), TC), (Z - 1) * TC)
                prod_buf[near_rows] = mm(G[l, near_rows], ws[l], ((1,), (1,)))
                rs_parts(l, False)
                arrived(G.at[l, pl.ds(0, TR)], g_fw.at[L])
        else:
            arrived(G.at[l, pl.ds(0, Z * TR)], g_fw.at[l])
        g = G[l]
        outer = mm(AT[l], g, ((1,), (0,)))
        dots_out(l, jnp.sum(merged[l] * outer, axis=0, keepdims=True))

        @pl.when(ends & (l == L - 2) & (core == 0))
        def _():
            relay(last - 1, Z - 2, out)

        @pl.when(jnp.logical_and(ends, l == L - 2))
        def _():
            dots_sum(L - 4)
            correct(1, not square)

        @pl.when(jnp.logical_and(ends, l == L - 1))
        def _():
            dots_sum(L - 3)

        low = outer.astype(BF16)
        if split:
            @pl.when(jnp.logical_or(middle, l != L - 2))
            def _():
                prod_buf[...] = mm(G[l], ws[l], ((1,), (1,)))
                rs_first(l, prod_buf)

            @pl.when(jnp.logical_and(ends, l == L - 2))
            def _():
                prod_buf[rows(far, TC)] = mm(G[l, rows(far, TC)], ws[l], ((1,), (1,)))
                rs_parts(l, True)
                rs_keep(l, prod_buf)
        else:
            prod_buf[...] = mm(g, ws[l], ((1,), (1,)))
            rs_first(l, prod_buf)

        @pl.when(ends & (l == L - 2) & (core == 0))
        def _():
            relay(last, Z - 1, out)

        @pl.when(jnp.logical_and(ends, l == L - 1))
        def _():
            rs_second(L - 3)

        ing[l] = mm(asc[l], low, ((1,), (1,)))

    def own_at(at):
        @pl.when(at + ahead < L)
        def _():
            g_own_each(at + ahead, start)

    def relays(at):
        own_at(at)

        @pl.when(at < Z - 2)
        def _():
            for d in range(1, Z):
                relay(at, d, -out)
                relay(at, d, out)

        @pl.when(at >= Z - 2)
        def _():
            for d in range(1, Z):
                relay(at, d, -out)
            for d in range(Z - 1, 0, -1):
                relay(at, d, out)

    squares_out()
    lead = 1

    @pl.when(middle)
    def _():
        for at in range(lead):
            relays(at)

    @pl.loop(0, last + 1)
    def _(at):
        late = jnp.logical_and(jnp.logical_not(middle), at >= Z - 2)

        @pl.when(jnp.logical_not(late))
        def _():
            relays(at + jnp.where(middle, lead, 0))

        @pl.when(jnp.logical_and(late, at < last))
        def _():
            own_at(at)
            relay(at, Z - 1, out)

        @pl.when(ends & (at == last - 1) & (core == 1))
        def _():
            relay(last - 1, Z - 2, out)
            relay(last, Z - 1, out)

        if square:
            for l in (2 * at - 1, 2 * at):
                @pl.when(jnp.logical_and(l >= 0, l < L))
                def _():
                    a_relay(l)

        @pl.when(at == max(Z - 3, 0))
        def _():
            squares_sum()

        @pl.when(at == Z - 2)
        def _():
            to_root(1)

        @pl.when(at == 0)
        def _():
            to_root(0)

        @pl.when(jnp.logical_and(at == jnp.where(middle, last, last - 2), z != root))
        def _():
            q_arrived()

        @pl.when(jnp.logical_and(at == Z - 2, z == root))
        def _():
            at_root(0)

        @pl.when(at == Z - 2)
        def _():
            scales()
            turn(0)

        @pl.when(at >= Z - 2)
        def _():
            compute(at - (Z - 2))

        @pl.when(jnp.logical_and(late, at < last - 1))
        def _():
            for d in range(Z - 2, 0, -1):
                relay(at, d, out)

        @pl.when(ends & (at >= last - 3) & (at < last - 1))
        def _():
            dots_sum(at - (last - 3))

        @pl.when(jnp.logical_and(ends, at == last - 2))
        def _():
            correct(0, not square)

    def low_rank(half):
        @pl.loop(0, H)
        def _(at):
            l = half * H + at
            for s in range(C):
                Qc[l, :, s * TC:(s + 1) * TC] = Qg[half, s, at]
            oug[l] = mm(Qc[l], G[l], ((1,), (0,))) * scl[l]

    @pl.loop(jnp.where(middle, 0, L - 2), L - 2)
    def _(l):
        dots_sum(l)

    @pl.loop(jnp.where(middle, 0, 2), L - 3)
    def _(l):
        correct(l, not square)

    @pl.when(z == root)
    def _():
        at_root(1)

    arrived(Qg.at[core, pl.ds(0, C - 1)], col_in.at[0])
    to_sib[4].start()

    correct(L - 3, not square)

    low_rank(core)

    @pl.when(middle)
    def _():
        rs_second(L - 3)

    rs_second(L - 2)

    correct(L - 2, True)

    if square:
        q_second(0)

    correct(L - 1, True)

    rs_second(L - 1)

    if square:
        @pl.loop(1, L - 2)
        def _(l):
            q_second(l)

    @pl.when(z != root)
    def _():
        arrived(out_ref(1), out_in.at[1])
        to_sib[5].start()

    for l in range(L):
        mgrad[l:l + 1] = mg3[l]

    arrived(Qg.at[1 - core], sib_in.at[4])
    low_rank(1 - core)

    arrived(im_fin.at[1 - core], sib_in.at[5])

    @pl.loop(0, L)
    def _(l):
        oug[l] += im_fin[l // H, lax.rem(l, H)].astype(F32) * cor[l]

    def done(copy):
        copy.wait_send()

    @pl.loop(0, L)
    def _(l):
        g_own_each(l, done)
        for d in range(1, Z):
            g_relay(l, d, 1, done, False)
            g_relay(l, d, -1, done, False)
        for copy in a_copies(l):
            copy.wait_send()
        if square:
            for copy in a_passes(l):
                copy.wait_send()

    @pl.loop(0, L - 2)
    def _(l):
        dt_own_each(l, done)

        @pl.when(in_charge(l))
        def _():
            dt_tot_copy(l).wait_send()

    for copy in sq_copies() + to_sib + gather_copies() + dt_all_copies(L - 2) + dt_all_copies(L - 1):
        copy.wait_send()

    @pl.when(z == root)
    def _():
        for copy in out_copies(0) + out_copies(1):
            copy.wait_send()

    @pl.when(z != root)
    def _():
        root_copy(0).wait_send()
        root_copy(1).wait_send()

    def q_finish(l):
        arrived(q_recv.at[pl.ds(1, C - 1), l], q_sem(l))
        for i in range(halves):
            total = ing[l, :, cols(i)]
            for d in range(1, C):
                total = total + q_recv[d, l, i].astype(F32)
            ing[l, :, cols(i)] = total

    def q2_finish(l):
        for i in range(2):
            ing[l, :, cols(i)] += q2_r[l, i].astype(F32)

    if square:
        arrived(rs2_r.at[:, pl.ds(0, L - 1)], rs2_in.at[0])

    @pl.loop(0, L - 1)
    def _(l):
        rs_finish(l)

    if square:
        arrived(q2_r.at[pl.ds(0, L - 3)], q2_in.at[0])

        @pl.loop(0, L - 3)
        def _(l):
            q2_finish(l)

        q_finish(L - 2)
    else:
        @pl.loop(0, L - 1)
        def _(l):
            q_finish(l)

    if square:
        arrived(rs2_r.at[:, L - 1], rs2_in.at[1])
    rs_finish(L - 1)

    q_finish(L - 1)
    if square:
        arrived(q2_r.at[L - 3], q2_in.at[1])
        q2_finish(L - 3)

    @pl.loop(0, L)
    def _(l):
        for copy in rs1_copies(l) + (rs2_copies(l) if square else []):
            copy.wait_send()

    @pl.loop(0, L - 2)
    def _(l):
        for copy in q1_copies(l) + q2_copies(l) if square else q_copies(l):
            copy.wait_send()

    for copy in q_copies(L - 2) + q_copies(L - 1):
        copy.wait_send()


def finish(ig, ing, oug, mgrad, ig_out, ing_out, oug_out, mgrad_out, sem):
    pairs = ((ig, ig_out), (ing, ing_out), (oug, oug_out), (mgrad, mgrad_out))
    copies = [pltpu.make_async_copy(a, b, sem.at[i]) for i, (a, b) in enumerate(pairs)]
    for copy in copies:
        copy.start()
    for copy in copies:
        copy.wait()


def body(R, C, acts, grads, frozen, ain, aout, mag):
    L, TR, W = grads.shape
    TC, KI = acts.shape[1:]
    RANK = ain.shape[1]
    V = pltpu.VMEM
    vm = pl.BlockSpec(memory_space=pltpu.VMEM)
    hbm = pl.BlockSpec(memory_space=pltpu.HBM)
    buffers = scratch(R, C, L, TR, W, TC, KI, RANK)
    ig, ing, oug, mgrad = pl.pallas_call(
        functools.partial(kernel, R, C),
        out_shape=(V((L, TC, KI), BF16), V((L, RANK, KI), F32), V((L, RANK, W), F32), V((L, W), F32)),
        in_specs=[hbm] * 6,
        out_specs=(vm,) * 4,
        scratch_shapes=[buffers[name] for name in NAMES],
        compiler_params=pltpu.CompilerParams(
            collective_id=0, has_side_effects=True, vmem_limit_bytes=60 * 1024 * 1024
        ),
    )(acts, grads, frozen, ain, aout, mag)
    return pl.pallas_call(
        finish,
        out_shape=tuple(jax.ShapeDtypeStruct(x.shape, x.dtype) for x in (ig, ing, oug, mgrad)),
        in_specs=[vm] * 4,
        out_specs=(hbm,) * 4,
        scratch_shapes=[pltpu.SemaphoreType.DMA((4,))],
        compiler_params=pltpu.CompilerParams(vmem_limit_bytes=1024 * 1024),
    )(ig, ing, oug, mgrad)


def solution(mesh):
    return jax.shard_map(
        functools.partial(body, mesh.shape["row"], mesh.shape["col"]),
        mesh=mesh,
        in_specs=(
            P(None, "col", "row"),
            P(None, "row", "col"),
            P(None, "row", "col"),
            P(None, None, "row"),
            P(None, None, "col"),
            P(None, "col"),
        ),
        out_specs=(
            P(None, "col", "row"),
            P(None, None, "row"),
            P(None, None, "col"),
            P(None, "col"),
        ),
        check_vma=False,
    )
```

```python
import functools

import jax
import jax.numpy as jnp
from jax import lax
from jax.experimental import pallas as pl
from jax.experimental.pallas import tpu as pltpu
from jax.sharding import PartitionSpec as P

MESH = pl.DeviceIdType.MESH
F32 = jnp.float32
BF16 = jnp.bfloat16


def mm(a, b, dims):
    return lax.dot_general(a, b, (dims, ((), ())), preferred_element_type=F32)


NAMES = (
    "acts", "grads", "frozen", "ain", "aout", "mag", "load", "G", "A", "AT", "merged", "ws", "asc", "sqm", "sq_sib", "sq_z",
    "sq_tot", "norms", "scl", "cor", "mag3", "mg3", "prod_buf", "qs", "q_sib", "q_all", "Qg", "Qc", "ims", "im_sib",
    "im_all", "im_fin", "dt_own", "dt_tot", "dt_all", "q", "q_recv", "q1_r", "q2_s", "q2_r", "own",
    "hold", "rs1_s", "rs1_r", "rs2_s", "rs2_r", "send", "g_in", "g_fw", "a_in", "rs1_in", "rs2_in", "sq_in", "dt_in",
    "dt_last", "root_in", "out_in", "col_in", "sib_in", "news", "q_in", "q1_in", "q2_in",
)


def scratch(R, C, L, TR, W, TC, KI, RANK):
    Z, T, H, KH = R // 2, TR * R, L // 2, KI // 2
    V, dma = pltpu.VMEM, pltpu.SemaphoreType.DMA
    wide = (2, L, 2, TC, KH) if C == 4 else (C, L, TC, KI)
    slim = (2, L, TC, KH) if C == 4 else (1, 1, 8, 128)
    pair = (L, 2, RANK, KH) if C == 4 else (L, 1, RANK, KI)
    return dict(
        acts=V((L, TC, KI), BF16), grads=V((L, TR, W), BF16), frozen=V((L, KI, W), BF16),
        ain=V((L, RANK, KI), BF16), aout=V((L, RANK, W), BF16), mag=V((L, W), F32), load=dma((6,)),
        G=V((L, T, W), BF16), A=V((L, T, KI), BF16), AT=V((L, KI, T), BF16), merged=V((L, KI, W), F32), ws=V((L, KI, W), BF16),
        asc=V((L, RANK, W), BF16),
        sqm=V((L, 1, W), F32), sq_sib=V((H, 1, W), F32), sq_z=V((Z, H, 1, W), F32), sq_tot=V((2, H, 1, W), F32),
        norms=V((L, 1, W), F32), scl=V((L, 1, W), F32), cor=V((L, 1, W), F32), mag3=V((L, 1, W), F32),
        mg3=V((L, 1, W), F32),
        prod_buf=V((T, KI), F32), qs=V((2, H, RANK, TC), F32), q_sib=V((H, RANK, TC), F32), q_all=V((Z, H, RANK, TC), BF16),
        Qg=V((2, C, H, RANK, TC), BF16), Qc=V((L, RANK, T), BF16),
        ims=V((2, H, RANK, W), F32), im_sib=V((H, RANK, W), F32), im_all=V((Z, H, RANK, W), BF16),
        im_fin=V((2, H, RANK, W), BF16),
        dt_own=V((L, R, 1, W), F32),
        dt_tot=V((L, 1, W), F32), dt_all=V((2, R, 1, W), F32), q=V(pair, BF16), q_recv=V((C,) + pair, BF16),
        q1_r=V(pair, BF16), q2_s=V(pair, BF16), q2_r=V(pair, BF16),
        own=V((L, TC, KI), F32), hold=V(slim, F32), rs1_s=V(wide, BF16), rs1_r=V(wide, BF16),
        rs2_s=V(slim, BF16), rs2_r=V(slim, BF16),
        send=dma((1,)), g_in=dma((L, Z - 1)), g_fw=dma((L + 1,)), a_in=dma((L, 2)), rs1_in=dma((L,)), rs2_in=dma((2,)),
        sq_in=dma((1,)), dt_in=dma((2, L - 2)), dt_last=dma((2,)), root_in=dma((2,)), out_in=dma((2,)), col_in=dma((1,)),
        sib_in=dma((6,)), news=pltpu.SemaphoreType.REGULAR((2, max(Z - 2, 1))), q_in=dma((2 if C == 4 else L,)), q1_in=dma((L - 2,)), q2_in=dma((2,)),
    )


def kernel(R, C, *refs):
    acts_hbm, grads_hbm, frozen_hbm, ain_hbm, aout_hbm, mag_hbm, ig, ing, oug, mgrad = refs[:10]
    (acts, grads, frozen, ain, aout, mag, load, G, A, AT, merged, ws, asc, sqm, sq_sib, sq_z, sq_tot, norms, scl, cor,
     mag3, mg3, prod_buf, qs, q_sib, q_all, Qg, Qc, ims, im_sib, im_all, im_fin, dt_own, dt_tot,
     dt_all, q, q_recv, q1_r, q2_s, q2_r, own, hold, rs1_s, rs1_r, rs2_s, rs2_r, send, g_in, g_fw, a_in, rs1_in,
     rs2_in, sq_in, dt_in, dt_last, root_in, out_in, col_in, sib_in, news, q_in, q1_in, q2_in) = refs[10:]
    pairs = ((grads_hbm, grads), (acts_hbm, acts), (frozen_hbm, frozen),
             (ain_hbm, ain), (aout_hbm, aout), (mag_hbm, mag))
    loads = [pltpu.make_async_copy(a, b, load.at[i]) for i, (a, b) in enumerate(pairs)]
    for copy in loads:
        copy.start()
    L, TR, W = grads.shape
    TC, KI = acts.shape[1:]
    Z, H, KH = R // 2, L // 2, KI // 2
    ahead = min(3, L)
    last = L + Z - 3
    r, c = lax.axis_index("row"), lax.axis_index("col")
    z, core = r // 2, lax.rem(r, 2)
    sib = 2 * z + 1 - core
    square = C == 4
    xn, yn = c + 1 - 2 * lax.rem(c, 2), lax.rem(c + 2, 4)
    dg = 3 - c
    root = Z // 2 - 1 + core
    middle = jnp.logical_and(z > 0, z < Z - 1)
    ends = jnp.logical_not(middle)
    halves = 2 if square else 1
    split = square and 2 * TR == TC
    far = jnp.where(z < Z // 2, Z - 1, 0)
    KS = KI // halves

    def row_to(d):
        return lax.rem(r + d, R)

    def row_from(d):
        return lax.rem(r + R - d, R)

    def col_to(d):
        return lax.rem(c + d, C)

    def col_from(d):
        return lax.rem(c + C - d, C)

    def z_to(d):
        return 2 * lax.rem(z + d, Z) + core

    def z_from(d):
        return lax.rem(z + Z - d, Z)

    def rows(at, size):
        return pl.ds(pl.multiple_of(at * size, size), size)

    def rcopy(src, dst, recv, **dev):
        return pltpu.make_async_remote_copy(
            src_ref=src, dst_ref=dst, send_sem=send.at[0], recv_sem=recv,
            device_id=dev, device_id_type=MESH,
        )

    def arrived(ref, recv):
        rcopy(ref, ref, recv, row=r).wait_recv()

    barrier = pltpu.get_barrier_semaphore()

    def greet(**dev):
        pl.semaphore_signal(barrier, inc=1, device_id=dev, device_id_type=MESH)

    greet(row=sib)
    for step in (1, -1):
        @pl.when(jnp.logical_and(z + step >= 0, z + step < Z))
        def _():
            greet(row=r + 2 * step)

    near = [xn, yn] if square else [col_to(d) for d in range(1, C)]
    for to in near:
        greet(col=to)
    pl.semaphore_wait(barrier, len(near) + jnp.where(middle, 3, 2))

    def tell(hops):
        for i, step in enumerate((1, -1)):
            of = z - step * (hops - 1)

            @pl.when((z + step >= 0) & (z + step < Z) & (of >= 0) & (of < Z))
            def _():
                pl.semaphore_signal(
                    news.at[i, hops - 2], inc=1, device_id={"row": r + 2 * step}, device_id_type=MESH
                )

    def hear(hops):
        for i, step in enumerate((1, -1)):
            of = z - step * hops

            @pl.when((of >= 0) & (of < Z))
            def _():
                pl.semaphore_wait(news.at[i, hops - 2], 1)

    def g_block(l, at, which):
        return G.at[l, rows(2 * at + which, TR)]

    def g_sem(l, at, to):
        return g_in.at[l, at - jnp.where(at > to, 1, 0)]

    def over(l, at):
        return jnp.where(ends & (l == L - 2) & (at == far), L, l) if split else l

    def g_own(l, step):
        if step == 0:
            return rcopy(grads.at[l], g_block(l, z, core), g_fw.at[l], row=sib)
        return rcopy(grads.at[l], g_block(l, z, core), g_sem(l, z, z + step), row=r + 2 * step)

    def g_pass(l, at, step):
        block = g_block(l, at, core)
        if isinstance(step, int) and step == 0:
            return rcopy(block, block, g_fw.at[over(l, at)], row=sib)
        return rcopy(block, block, g_sem(l, at, z + step), row=r + 2 * step)

    def g_own_each(l, act):
        @pl.when(z < Z - 1)
        def _():
            act(g_own(l, 1))

        @pl.when(z > 0)
        def _():
            act(g_own(l, -1))

        act(g_own(l, 0))

    def g_relay(l, d, step, act, arrive):
        at = z - step * d

        @pl.when(jnp.logical_and(at >= 0, at < Z))
        def _():
            if arrive:
                arrived(g_block(l, at, core), g_sem(l, at, z))

            @pl.when(jnp.logical_and(z + step >= 0, z + step < Z))
            def _():
                act(g_pass(l, at, step))

            act(g_pass(l, at, 0))

    def a_copies(l):
        mine = A.at[l, rows(c, TC)]
        if square:
            return [rcopy(acts.at[l], mine, a_in.at[l, 0], col=xn), rcopy(acts.at[l], mine, a_in.at[l, 0], col=yn)]
        return [rcopy(acts.at[l], mine, a_in.at[l, 0], col=col_to(d)) for d in range(1, C)]

    def a_half(l, of, part):
        size = TC // 2
        return A.at[l, rows(2 * of + part, size)]

    def a_passes(l):
        first, second = a_half(l, xn, 0), a_half(l, yn, 1)
        return [rcopy(first, first, a_in.at[l, 1], col=yn), rcopy(second, second, a_in.at[l, 1], col=xn)]

    def a_relay(l):
        arrived(A.at[l, pl.ds(0, 2 * TC)], a_in.at[l, 0])
        for copy in a_passes(l):
            copy.start()

    def a_ready(l):
        if square:
            arrived(A.at[l, rows(dg, TC)], a_in.at[l, 1])
        else:
            arrived(A.at[l, pl.ds(0, (C - 1) * TC)], a_in.at[l, 0])

    def rs1_copies(l):
        if square:
            return [rcopy(rs1_s.at[i, l], rs1_r.at[i, l], rs1_in.at[l], col=to) for i, to in enumerate((xn, yn))]
        return [rcopy(rs1_s.at[d, l], rs1_r.at[d, l], rs1_in.at[l], col=col_to(d)) for d in range(1, C)]

    def rs2_copies(l):
        return [rcopy(rs2_s.at[i, l], rs2_r.at[i, l], rs2_in.at[l // (L - 1)], col=to) for i, to in enumerate((yn, xn))]

    def rs_keep(l, prod):
        for i in range(2):
            hold[i, l] = prod[rows((yn, xn)[i], TC), cols(i)]
        own[l] = prod[rows(c, TC)]

    def rs_parts(l, late):
        for i, near in enumerate((xn, yn)):
            for which, block in enumerate((near, dg)):
                @pl.when((block == far) if late else (block != far))
                def _():
                    part, there = rs1_s.at[i, l, which], rs1_r.at[i, l, which]
                    rs1_s[i, l, which] = prod_buf[rows(block, TC), cols(i)].astype(BF16)
                    rcopy(part, there, rs1_in.at[l], col=near).start()

    def rs_first(l, prod):
        if square:
            for i, near in enumerate((xn, yn)):
                rs1_s[i, l, 0] = prod[rows(near, TC), cols(i)].astype(BF16)
                rs1_s[i, l, 1] = prod[rows(dg, TC), cols(i)].astype(BF16)
                hold[i, l] = prod[rows((yn, xn)[i], TC), cols(i)]
        else:
            for d in range(1, C):
                rs1_s[d, l] = prod[rows(col_to(d), TC)].astype(BF16)
        own[l] = prod[rows(c, TC)]
        for copy in rs1_copies(l):
            copy.start()

    def rs_second(l):
        if square:
            arrived(rs1_r.at[:, l], rs1_in.at[l])
            for i in range(2):
                rs2_s[i, l] = (hold[i, l] + rs1_r[i, l, 1].astype(F32)).astype(BF16)
            for copy in rs2_copies(l):
                copy.start()

    def rs_finish(l):
        if square:
            for i in range(2):
                total = own[l, :, cols(i)] + rs1_r[i, l, 0].astype(F32) + rs2_r[i, l].astype(F32)
                ig[l, :, cols(i)] = total.astype(BF16)
        else:
            total = own[l]
            arrived(rs1_r.at[pl.ds(1, C - 1), l], rs1_in.at[l])
            for d in range(1, C):
                total = total + rs1_r[d, l].astype(F32)
            ig[l] = total.astype(BF16)

    def sq_copies():
        return [rcopy(sq_z.at[z], sq_z.at[z], sq_in.at[0], row=z_to(d)) for d in range(1, Z)]

    to_sib = [
        rcopy(sqm.at[pl.ds((1 - core) * H, H)], sq_sib, sib_in.at[0], row=sib),
        rcopy(sq_tot.at[core], sq_tot.at[core], sib_in.at[1], row=sib),
        rcopy(qs.at[1 - core], q_sib, sib_in.at[2], row=sib),
        rcopy(ims.at[1 - core], im_sib, sib_in.at[3], row=sib),
        rcopy(Qg.at[core], Qg.at[core], sib_in.at[4], row=sib),
        rcopy(im_fin.at[core], im_fin.at[core], sib_in.at[5], row=sib),
    ]

    def root_copy(i):
        ref = (q_all, im_all)[i].at[z]
        return rcopy(ref, ref, root_in.at[i], row=2 * root + core)

    def out_ref(i):
        return Qg.at[core, c] if i == 0 else im_fin.at[core]

    def out_copies(i):
        ref = out_ref(i)
        return [rcopy(ref, ref, out_in.at[i], row=z_to(d)) for d in range(1, Z)]

    def gather_copies():
        mine = Qg.at[core, c]
        return [rcopy(mine, mine, col_in.at[0], col=col_to(d)) for d in range(1, C)]

    def start(copy):
        copy.start()

    def to_root(i):
        mine, theirs, every = (qs, q_sib, q_all) if i == 0 else (ims, im_sib, im_all)
        arrived(theirs, sib_in.at[2 + i])
        every[z] = (mine[core] + theirs[...]).astype(BF16)

        @pl.when(z != root)
        def _():
            root_copy(i).start()

    def at_root(i):
        every = (q_all, im_all)[i]
        arrived(every.at[pl.ds(0, Z - 1)], root_in.at[i])
        total = every[0].astype(F32)
        for s in range(1, Z):
            total = total + every[s].astype(F32)
        if i == 0:
            Qg[core, c] = total.astype(BF16)
        else:
            im_fin[core] = total.astype(BF16)
        for copy in out_copies(i) + (gather_copies() if i == 0 else [to_sib[5]]):
            copy.start()

    def q_arrived():
        arrived(out_ref(0), out_in.at[0])
        for copy in gather_copies():
            copy.start()

    def dt_all_copies(l):
        mine = dt_all.at[l - (L - 2), r]
        return [rcopy(mine, mine, dt_last.at[l - (L - 2)], row=row_to(d)) for d in range(1, R)]

    def dt_own_copy(l, at):
        mine = dt_own.at[l, r]
        return rcopy(mine, mine, dt_in.at[0, l], row=2 * at + lax.rem(l, 2))

    def dt_own_each(l, act):
        for d in range(1, Z):
            act(dt_own_copy(l, lax.rem(z + d, Z)))

        @pl.when(jnp.logical_not(in_charge(l)))
        def _():
            act(dt_own_copy(l, z))

    def dt_tot_copy(l):
        return rcopy(dt_tot.at[l], dt_tot.at[l], dt_in.at[1, l], row=sib)

    def in_charge(l):
        return lax.rem(l, 2) == core

    def dots_out(l, part):
        @pl.when(l < L - 2)
        def _():
            dt_own[l, r] = part
            dt_own_each(l, start)

        @pl.when(l >= L - 2)
        def _():
            dt_all[l - (L - 2), r] = part
            for copy in dt_all_copies(l):
                copy.start()

    def dots_sum(l):
        @pl.when(in_charge(l))
        def _():
            arrived(dt_own.at[l, pl.ds(0, R - 1)], dt_in.at[0, l])
            total = dt_own[l, 0]
            for s in range(1, R):
                total = total + dt_own[l, s]
            dt_tot[l] = total
            dt_tot_copy(l).start()

    def q_sem(l):
        return q_in.at[l - (L - 2) if square else l]

    def q_copies(l):
        return [rcopy(q.at[l], q_recv.at[d, l], q_sem(l), col=col_to(d)) for d in range(1, C)]

    def q1_copies(l):
        return [rcopy(q.at[l, i], q1_r.at[l, i], q1_in.at[l], col=to) for i, to in enumerate((xn, yn))]

    def q2_copies(l):
        return [rcopy(q2_s.at[l, i], q2_r.at[l, i], q2_in.at[l // (L - 3)], col=to) for i, to in enumerate((yn, xn))]

    def cols(i):
        return slice(i * KS, (i + 1) * KS)

    loads[0].wait()
    loads[1].wait()

    @pl.loop(0, ahead)
    def _(l):
        g_own_each(l, start)

    @pl.loop(0, L)
    def _(l):
        for copy in a_copies(l):
            copy.start()

    if Z > 2:
        tell(2)
    for copy in loads[2:]:
        copy.wait()

    @pl.loop(0, L)
    def _(l):
        m = frozen[l].astype(F32) + mm(ain[l], aout[l], ((0,), (0,)))
        merged[l] = m
        sqm[l] = jnp.sum(m * m, axis=0, keepdims=True)

    to_sib[0].start()
    for hops in range(2, Z):
        hear(hops)
        if hops < Z - 1:
            tell(hops + 1)

    @pl.loop(0, L)
    def _(l):
        G[l, rows(r, TR)] = grads[l]
        A[l, rows(c, TC)] = acts[l]
        half, at = l // H, lax.rem(l, H)
        ims[half, at] = mm(ain[l], merged[l].astype(BF16), ((1,), (0,)))
        qs[half, at] = mm(ain[l], acts[l], ((1,), (1,)))

    to_sib[2].start()
    to_sib[3].start()
    for l in range(L):
        mag3[l] = mag[l:l + 1]

    def squares_out():
        arrived(sq_sib, sib_in.at[0])
        sq_z[z] = sqm[pl.ds(core * H, H)] + sq_sib[...]
        for copy in sq_copies():
            copy.start()

    def squares_sum():
        arrived(sq_z.at[pl.ds(0, Z - 1)], sq_in.at[0])
        total = sq_z[0]
        for s in range(1, Z):
            total = total + sq_z[s]
        sq_tot[core] = total
        to_sib[1].start()

    def scales():
        arrived(sq_tot.at[1 - core], sib_in.at[1])

        @pl.loop(0, L)
        def _(l):
            n = jnp.sqrt(sq_tot[l // H, lax.rem(l, H)] + 0.25)
            s = mag3[l] / n
            norms[l] = n
            scl[l] = s
            ws[l] = (merged[l] * s).astype(BF16)
            asc[l] = (aout[l].astype(F32) * s).astype(BF16)

    def correct(l, direct):
        if isinstance(l, int) and l >= L - 2:
            every = dt_all.at[l - (L - 2)]
            arrived(every.at[pl.ds(0, R - 1)], dt_last.at[l - (L - 2)])
            dots = every[0]
            for s in range(1, R):
                dots = dots + every[s]
        else:
            @pl.when(jnp.logical_not(in_charge(l)))
            def _():
                arrived(dt_tot.at[l], dt_in.at[1, l])

            dots = dt_tot[l]
        n = norms[l]
        mg3[l] = dots / n
        factor = -mag3[l] * dots / (n * n * n)
        cor[l] = factor
        adjusted = (merged[l] * factor).astype(BF16)
        part = ing[l] + mm(aout[l], adjusted, ((1,), (1,)))
        ing[l] = part
        for i in range(halves):
            q[l, i] = part[:, cols(i)].astype(BF16)
        for copy in q_copies(l) if direct else q1_copies(l):
            copy.start()

    def q_second(l):
        arrived(q1_r.at[l], q1_in.at[l])
        for i in range(2):
            total = ing[l, :, cols(i)] + q1_r[l, i].astype(F32)
            ing[l, :, cols(i)] = total
            q2_s[l, i] = total.astype(BF16)
        for copy in q2_copies(l):
            copy.start()

    out = jnp.where(z < Z // 2, -1, 1)

    def relay(at, d, step):
        l = at - (d - 1)

        @pl.when(jnp.logical_and(l >= 0, l < L))
        def _():
            g_relay(l, d, step, start, True)

    def turn(l):
        a_ready(l)
        AT[l] = A[l].T

    def compute(l):
        @pl.when(l < L - 1)
        def _():
            turn(l + 1)

        back = jnp.where(middle, 3, 2)

        @pl.when((l >= back) & (middle | (l < L - 1)))
        def _():
            rs_second(l - back)

        if split:
            @pl.when(jnp.logical_or(middle, l != L - 2))
            def _():
                arrived(G.at[l, pl.ds(0, Z * TR)], g_fw.at[l])

            @pl.when(jnp.logical_and(ends, l == L - 2))
            def _():
                arrived(G.at[l, pl.ds(0, (Z - 1) * TR)], g_fw.at[l])
                near_rows = pl.ds(pl.multiple_of(jnp.where(far == 0, TC, 0), TC), (Z - 1) * TC)
                prod_buf[near_rows] = mm(G[l, near_rows], ws[l], ((1,), (1,)))
                rs_parts(l, False)
                arrived(G.at[l, pl.ds(0, TR)], g_fw.at[L])
        else:
            arrived(G.at[l, pl.ds(0, Z * TR)], g_fw.at[l])
        g = G[l]
        outer = mm(AT[l], g, ((1,), (0,)))
        dots_out(l, jnp.sum(merged[l] * outer, axis=0, keepdims=True))

        @pl.when(ends & (l == L - 2) & (core == 0))
        def _():
            relay(last - 1, Z - 2, out)

        @pl.when(jnp.logical_and(ends, l == L - 2))
        def _():
            dots_sum(L - 4)
            correct(1, not square)

        @pl.when(jnp.logical_and(ends, l == L - 1))
        def _():
            dots_sum(L - 3)

        low = outer.astype(BF16)
        if split:
            @pl.when(jnp.logical_or(middle, l != L - 2))
            def _():
                prod_buf[...] = mm(G[l], ws[l], ((1,), (1,)))
                rs_first(l, prod_buf)

            @pl.when(jnp.logical_and(ends, l == L - 2))
            def _():
                prod_buf[rows(far, TC)] = mm(G[l, rows(far, TC)], ws[l], ((1,), (1,)))
                rs_parts(l, True)
                rs_keep(l, prod_buf)
        else:
            prod_buf[...] = mm(g, ws[l], ((1,), (1,)))
            rs_first(l, prod_buf)

        @pl.when(ends & (l == L - 2) & (core == 0))
        def _():
            relay(last, Z - 1, out)

        @pl.when(jnp.logical_and(ends, l == L - 1))
        def _():
            rs_second(L - 3)

        ing[l] = mm(asc[l], low, ((1,), (1,)))

    def own_at(at):
        @pl.when(at + ahead < L)
        def _():
            g_own_each(at + ahead, start)

    def relays(at):
        own_at(at)

        @pl.when(at < Z - 2)
        def _():
            for d in range(1, Z):
                relay(at, d, -out)
                relay(at, d, out)

        @pl.when(at >= Z - 2)
        def _():
            for d in range(1, Z):
                relay(at, d, -out)
            for d in range(Z - 1, 0, -1):
                relay(at, d, out)

    squares_out()
    lead = 1

    @pl.when(middle)
    def _():
        for at in range(lead):
            relays(at)

    @pl.loop(0, last + 1)
    def _(at):
        late = jnp.logical_and(jnp.logical_not(middle), at >= Z - 2)

        @pl.when(jnp.logical_not(late))
        def _():
            relays(at + jnp.where(middle, lead, 0))

        @pl.when(jnp.logical_and(late, at < last))
        def _():
            own_at(at)
            relay(at, Z - 1, out)

        @pl.when(ends & (at == last - 1) & (core == 1))
        def _():
            relay(last - 1, Z - 2, out)
            relay(last, Z - 1, out)

        if square:
            for l in (2 * at - 1, 2 * at):
                @pl.when(jnp.logical_and(l >= 0, l < L))
                def _():
                    a_relay(l)

        @pl.when(at == max(Z - 3, 0))
        def _():
            squares_sum()

        @pl.when(at == Z - 2)
        def _():
            to_root(1)

        @pl.when(at == 0)
        def _():
            to_root(0)

        @pl.when(jnp.logical_and(at == jnp.where(middle, last, last - 2), z != root))
        def _():
            q_arrived()

        @pl.when(jnp.logical_and(at == Z - 2, z == root))
        def _():
            at_root(0)

        @pl.when(at == Z - 2)
        def _():
            scales()
            turn(0)

        @pl.when(at >= Z - 2)
        def _():
            compute(at - (Z - 2))

        @pl.when(jnp.logical_and(late, at < last - 1))
        def _():
            for d in range(Z - 2, 0, -1):
                relay(at, d, out)

        @pl.when(ends & (at >= last - 3) & (at < last - 1))
        def _():
            dots_sum(at - (last - 3))

        @pl.when(jnp.logical_and(ends, at == last - 2))
        def _():
            correct(0, not square)

    def low_rank(half):
        @pl.loop(0, H)
        def _(at):
            l = half * H + at
            for s in range(C):
                Qc[l, :, s * TC:(s + 1) * TC] = Qg[half, s, at]
            oug[l] = mm(Qc[l], G[l], ((1,), (0,))) * scl[l]

    @pl.loop(jnp.where(middle, 0, L - 2), L - 2)
    def _(l):
        dots_sum(l)

    @pl.loop(jnp.where(middle, 0, 2), L - 3)
    def _(l):
        correct(l, not square)

    @pl.when(z == root)
    def _():
        at_root(1)

    arrived(Qg.at[core, pl.ds(0, C - 1)], col_in.at[0])
    to_sib[4].start()

    low_rank(core)

    correct(L - 3, not square)

    @pl.when(middle)
    def _():
        rs_second(L - 3)

    rs_second(L - 2)

    correct(L - 2, True)

    if square:
        q_second(0)

    correct(L - 1, True)

    rs_second(L - 1)

    if square:
        @pl.loop(1, L - 2)
        def _(l):
            q_second(l)

    @pl.when(z != root)
    def _():
        arrived(out_ref(1), out_in.at[1])
        to_sib[5].start()

    for l in range(L):
        mgrad[l:l + 1] = mg3[l]

    arrived(Qg.at[1 - core], sib_in.at[4])
    low_rank(1 - core)

    arrived(im_fin.at[1 - core], sib_in.at[5])

    @pl.loop(0, L)
    def _(l):
        oug[l] += im_fin[l // H, lax.rem(l, H)].astype(F32) * cor[l]

    def done(copy):
        copy.wait_send()

    @pl.loop(0, L)
    def _(l):
        g_own_each(l, done)
        for d in range(1, Z):
            g_relay(l, d, 1, done, False)
            g_relay(l, d, -1, done, False)
        for copy in a_copies(l):
            copy.wait_send()
        if square:
            for copy in a_passes(l):
                copy.wait_send()

    @pl.loop(0, L - 2)
    def _(l):
        dt_own_each(l, done)

        @pl.when(in_charge(l))
        def _():
            dt_tot_copy(l).wait_send()

    for copy in sq_copies() + to_sib + gather_copies() + dt_all_copies(L - 2) + dt_all_copies(L - 1):
        copy.wait_send()

    @pl.when(z == root)
    def _():
        for copy in out_copies(0) + out_copies(1):
            copy.wait_send()

    @pl.when(z != root)
    def _():
        root_copy(0).wait_send()
        root_copy(1).wait_send()

    def q_finish(l):
        arrived(q_recv.at[pl.ds(1, C - 1), l], q_sem(l))
        for i in range(halves):
            total = ing[l, :, cols(i)]
            for d in range(1, C):
                total = total + q_recv[d, l, i].astype(F32)
            ing[l, :, cols(i)] = total

    def q2_finish(l):
        for i in range(2):
            ing[l, :, cols(i)] += q2_r[l, i].astype(F32)

    if square:
        arrived(rs2_r.at[:, pl.ds(0, L - 1)], rs2_in.at[0])

    @pl.loop(0, L - 1)
    def _(l):
        rs_finish(l)

    if square:
        arrived(q2_r.at[pl.ds(0, L - 3)], q2_in.at[0])

        @pl.loop(0, L - 3)
        def _(l):
            q2_finish(l)

        q_finish(L - 2)
    else:
        @pl.loop(0, L - 1)
        def _(l):
            q_finish(l)

    if square:
        arrived(rs2_r.at[:, L - 1], rs2_in.at[1])
    rs_finish(L - 1)

    q_finish(L - 1)
    if square:
        arrived(q2_r.at[L - 3], q2_in.at[1])
        q2_finish(L - 3)

    @pl.loop(0, L)
    def _(l):
        for copy in rs1_copies(l) + (rs2_copies(l) if square else []):
            copy.wait_send()

    @pl.loop(0, L - 2)
    def _(l):
        for copy in q1_copies(l) + q2_copies(l) if square else q_copies(l):
            copy.wait_send()

    for copy in q_copies(L - 2) + q_copies(L - 1):
        copy.wait_send()


def finish(ig, ing, oug, mgrad, ig_out, ing_out, oug_out, mgrad_out, sem):
    pairs = ((ig, ig_out), (ing, ing_out), (oug, oug_out), (mgrad, mgrad_out))
    copies = [pltpu.make_async_copy(a, b, sem.at[i]) for i, (a, b) in enumerate(pairs)]
    for copy in copies:
        copy.start()
    for copy in copies:
        copy.wait()


def body(R, C, acts, grads, frozen, ain, aout, mag):
    L, TR, W = grads.shape
    TC, KI = acts.shape[1:]
    RANK = ain.shape[1]
    V = pltpu.VMEM
    vm = pl.BlockSpec(memory_space=pltpu.VMEM)
    hbm = pl.BlockSpec(memory_space=pltpu.HBM)
    buffers = scratch(R, C, L, TR, W, TC, KI, RANK)
    ig, ing, oug, mgrad = pl.pallas_call(
        functools.partial(kernel, R, C),
        out_shape=(V((L, TC, KI), BF16), V((L, RANK, KI), F32), V((L, RANK, W), F32), V((L, W), F32)),
        in_specs=[hbm] * 6,
        out_specs=(vm,) * 4,
        scratch_shapes=[buffers[name] for name in NAMES],
        compiler_params=pltpu.CompilerParams(
            collective_id=0, has_side_effects=True, vmem_limit_bytes=60 * 1024 * 1024
        ),
    )(acts, grads, frozen, ain, aout, mag)
    return pl.pallas_call(
        finish,
        out_shape=tuple(jax.ShapeDtypeStruct(x.shape, x.dtype) for x in (ig, ing, oug, mgrad)),
        in_specs=[vm] * 4,
        out_specs=(hbm,) * 4,
        scratch_shapes=[pltpu.SemaphoreType.DMA((4,))],
        compiler_params=pltpu.CompilerParams(vmem_limit_bytes=1024 * 1024),
    )(ig, ing, oug, mgrad)


def solution(mesh):
    return jax.shard_map(
        functools.partial(body, mesh.shape["row"], mesh.shape["col"]),
        mesh=mesh,
        in_specs=(
            P(None, "col", "row"),
            P(None, "row", "col"),
            P(None, "row", "col"),
            P(None, None, "row"),
            P(None, None, "col"),
            P(None, "col"),
        ),
        out_specs=(
            P(None, "col", "row"),
            P(None, None, "row"),
            P(None, None, "col"),
            P(None, "col"),
        ),
        check_vma=False,
    )
```
